128 devices in a mesh: data: 1, expert: 128 (over z, y, x, core).
Axes of the slice: x: 4, y: 4, z: 4, core: 2. Of those that a mesh axis runs over, the one named last changes fastest.
Arguments:
- tokens: bfloat16 [4096, 2048], P(('data', 'expert'))
- w_router: bfloat16 [2048, 128], replicated
- routes: int32 [4096, 8], P(('data', 'expert'))
- w_gate: bfloat16 [128, 2048, 768], P('expert')
- w_up: bfloat16 [128, 2048, 768], P('expert')
- w_down: bfloat16 [128, 768, 2048], P('expert')
Outputs:
- output: bfloat16 [4096, 2048], P(('data', 'expert'))
All inputs are finite; a program needn't handle non-finite values.
Results may differ from the reference program's by a relative error of at most 0.00817875.
Values are sent between devices in bfloat16 or wider.
A program may use at most 1 GiB of HBM per device.

```python
import jax
import jax.numpy as jnp
from jax import lax

D = 2048
FF = 768
EXPERTS = 128
TOP = 8
TOKENS = 32
GROUP = 128

HOT_COUNT = max(1, EXPERTS // 16)
CAP = 4 * TOKENS * TOP // EXPERTS


def draw_routing(key):
    pair_count = TOKENS * TOP
    cold_count = EXPERTS - HOT_COUNT
    cold_pairs = pair_count - HOT_COUNT * CAP
    cold_base = cold_pairs // cold_count
    cold_extra = cold_pairs - cold_base * cold_count
    key_label, key_dev = jax.random.split(key)
    labels = jax.random.permutation(key_label, EXPERTS).astype(jnp.int32)

    def one_device(dev_key):
        key_a, key_b, key_c = jax.random.split(dev_key, 3)
        jitter = jax.random.randint(key_a, (cold_count,), 0, cold_base // 2 + 1, dtype=jnp.int32)
        mixing = jax.random.permutation(key_b, cold_count)
        cold_counts = cold_base + (jnp.arange(cold_count) < cold_extra).astype(jnp.int32) + jitter - jitter[mixing]
        counts = jnp.concatenate([jnp.full((HOT_COUNT,), CAP, jnp.int32), cold_counts.astype(jnp.int32)])
        run_ends = jnp.cumsum(counts)
        position = jnp.searchsorted(run_ends, jnp.arange(pair_count, dtype=jnp.int32), side='right')
        slot_table = labels[position].reshape(TOP, TOKENS).T
        tok_order = jax.random.permutation(key_c, TOKENS)
        return slot_table[tok_order]

    dev_keys = jax.random.split(key_dev, GROUP)
    return jax.vmap(one_device)(dev_keys).reshape(GROUP * TOKENS, TOP).astype(jnp.int32)


def setup_inputs(seed: int = 0, part: int = 0) -> dict:
    key_part = jax.random.fold_in(jax.random.key(seed), part)
    key_x, key_route = jax.random.split(key_part)
    key_r, key_1, key_3, key_2 = jax.random.split(jax.random.key(seed + 1), 4)
    tokens = jax.random.normal(key_x, (GROUP * TOKENS, D), jnp.float32).astype(jnp.bfloat16)
    w_router = (jax.random.normal(key_r, (D, EXPERTS), jnp.float32) * (1.5 * D ** -0.5)).astype(jnp.bfloat16)
    routes = draw_routing(key_route)
    w_gate = (jax.random.normal(key_1, (EXPERTS, D, FF), jnp.float32) * D ** -0.5).astype(jnp.bfloat16)
    w_up = (jax.random.normal(key_3, (EXPERTS, D, FF), jnp.float32) * D ** -0.5).astype(jnp.bfloat16)
    w_down = (jax.random.normal(key_2, (EXPERTS, FF, D), jnp.float32) * FF ** -0.5).astype(jnp.bfloat16)
    return {'tokens': tokens, 'w_router': w_router, 'routes': routes, 'w_gate': w_gate, 'w_up': w_up, 'w_down': w_down}


def reference(tokens, w_router, routes, w_gate, w_up, w_down):
    row_count = tokens.shape[0]
    cap_all = GROUP * CAP
    logits = jnp.dot(tokens, w_router, preferred_element_type=jnp.float32)
    gate_vals = jax.nn.softmax(jnp.take_along_axis(logits, routes, axis=1), axis=-1)
    flat_ids = routes.reshape(-1)
    flat_gates = gate_vals.reshape(-1)
    pair_tok = jnp.arange(row_count * TOP, dtype=jnp.int32) // TOP

    def expert_step(y_acc, inputs):
        expert_id, gate_w, up_w, down_w = inputs
        hit_mask = flat_ids == expert_id
        slot_pos = jnp.where(hit_mask, jnp.cumsum(hit_mask.astype(jnp.int32)) - 1, cap_all)
        slot_tok = jnp.full((cap_all,), row_count, jnp.int32).at[slot_pos].set(pair_tok, mode='drop')
        slot_gate = jnp.zeros((cap_all,), jnp.float32).at[slot_pos].set(flat_gates, mode='drop')
        rows_in = jnp.take(tokens, slot_tok, axis=0, mode='fill', fill_value=0)
        hidden = jax.nn.silu(jnp.dot(rows_in, gate_w, preferred_element_type=jnp.float32)) * jnp.dot(rows_in, up_w, preferred_element_type=jnp.float32)
        expert_out = jnp.dot(hidden.astype(jnp.bfloat16), down_w, preferred_element_type=jnp.float32).astype(jnp.bfloat16)
        weighted = expert_out.astype(jnp.float32) * slot_gate[:, None]
        y_acc = y_acc + jax.ops.segment_sum(weighted, slot_tok, num_segments=row_count)
        return y_acc, None

    expert_ids = jnp.arange(EXPERTS, dtype=jnp.int32)
    total, _ = lax.scan(expert_step, jnp.zeros((row_count, D), jnp.float32), (expert_ids, w_gate, w_up, w_down))
    return total.astype(jnp.bfloat16)
```

```python
import functools

import jax
import jax.numpy as jnp
from jax import lax
from jax.experimental import pallas as pl
from jax.experimental.pallas import tpu as pltpu
from jax.sharding import PartitionSpec as P

F32 = jnp.float32
BF16 = jnp.bfloat16
CAP = 8


def _iota(shape, dim):
    return lax.broadcasted_iota(jnp.int32, shape, dim)


def prep_kernel(x_ref, wr_ref, r_ref, tab_ref, aux_ref):
    tok, experts = x_ref.shape[0], wr_ref.shape[1]
    logits = jnp.dot(x_ref[...], wr_ref[...], preferred_element_type=F32)
    routes = r_ref[...]
    lane = _iota((tok, experts), 1)
    hit = jnp.zeros((tok, experts), F32)
    for j in range(routes.shape[1]):
        hit += (routes[:, j:j + 1] == lane).astype(F32)
    on = hit > 0.5
    masked = jnp.where(on, logits, -jnp.inf)
    top = jnp.max(masked, axis=1, keepdims=True)
    e = jnp.where(on, jnp.exp(jnp.where(on, logits, top) - top), 0.0)
    gate = e / jnp.sum(e, axis=1, keepdims=True)
    below = (_iota((tok, tok), 1) < _iota((tok, tok), 0)).astype(BF16)
    rank = jnp.dot(below, hit.astype(BF16), preferred_element_type=F32)
    rank = jnp.where(on, rank, -1.0)
    row = _iota((tok, experts), 0).astype(F32)
    rows = []
    for r in range(CAP):
        rows.append(jnp.sum(jnp.where(rank == r, row + 1.0, 0.0), axis=0, keepdims=True) - 1.0)
    tab_ref[...] = jnp.concatenate(rows, axis=0)
    g1 = gate.astype(BF16)
    rest = gate - g1.astype(F32)
    g2 = rest.astype(BF16)
    g3 = (rest - g2.astype(F32)).astype(BF16)
    aux_ref[...] = jnp.concatenate([g1, g2, g3, rank.astype(BF16)], axis=0)


def ffn_kernel(tab_ref, x_ref, wg_ref, wu_ref, wd_ref, o_ref, rows_ref):
    me = lax.axis_index('expert')
    n_rows = tab_ref.shape[0]
    tab = tab_ref[...]
    col = jnp.sum(jnp.where(_iota(tab.shape, 1) == me, tab, 0.0), axis=1, keepdims=True)
    for g in range(n_rows // 64):
        c = col[g * 64:(g + 1) * 64]
        src = (_iota((64, 1), 0) // CAP * 32).astype(F32)
        want = jnp.where(c >= 0.0, c + src, -1.0)
        pick = (want == _iota((64, 256), 1).astype(F32)).astype(BF16)
        rows_ref[g * 64:(g + 1) * 64] = jnp.dot(pick, x_ref[g * 256:(g + 1) * 256], preferred_element_type=F32).astype(BF16)
    rows = rows_ref[...]
    a = jnp.dot(rows, wg_ref[...], preferred_element_type=F32)
    b = jnp.dot(rows, wu_ref[...], preferred_element_type=F32)
    h = (a * jax.nn.sigmoid(a) * b).astype(BF16)
    o_ref[...] = jnp.dot(h, wd_ref[...], preferred_element_type=F32).astype(BF16)


def combine_kernel(aux_ref, back_ref, y_ref, gate_ref):
    tok = y_ref.shape[0]
    experts = aux_ref.shape[1]
    slots = back_ref.shape[0]

    @pl.when(pl.program_id(0) == 0)
    def _():
        spread = (_iota((experts, slots), 1) // CAP == _iota((experts, slots), 0)).astype(BF16)
        wide = jnp.dot(aux_ref[...], spread, preferred_element_type=F32)
        here = wide[3 * tok:] == (_iota((tok, slots), 1) % CAP).astype(F32)
        for p in range(3):
            gate_ref[p * tok:(p + 1) * tok] = jnp.where(here, wide[p * tok:(p + 1) * tok], 0.0).astype(BF16)

    y = jnp.dot(gate_ref[...], back_ref[...], preferred_element_type=F32)
    y_ref[...] = (y[:tok] + y[tok:2 * tok] + y[2 * tok:]).astype(BF16)


def solution(mesh):
    row_spec = P(('data', 'expert'), None)
    expert_spec = P('expert', None, None)
    vmem = pl.BlockSpec(memory_space=pltpu.VMEM)

    def device_step(tokens, w_router, routes, w_gate, w_up, w_down):
        tok, width = tokens.shape
        experts = w_router.shape[1]
        ff = w_gate.shape[2]
        slots = experts * CAP
        tab, aux = pl.pallas_call(
            prep_kernel,
            out_shape=(jax.ShapeDtypeStruct((CAP, experts), F32), jax.ShapeDtypeStruct((4 * tok, experts), BF16)),
            in_specs=[vmem] * 3, out_specs=(vmem, vmem), name='prep',
        )(tokens, w_router, routes)
        all_x = lax.all_gather(tokens, 'expert', axis=0, tiled=True)
        all_tab = lax.all_gather(tab, 'expert', axis=0, tiled=True)
        steps = 4
        m, k = slots // steps, experts * tok // steps
        out = pl.pallas_call(
            ffn_kernel,
            grid=(steps,),
            out_shape=jax.ShapeDtypeStruct((slots, width), BF16),
            in_specs=[
                pl.BlockSpec((m, experts), lambda i: (i, 0)),
                pl.BlockSpec((k, width), lambda i: (i, 0)),
                pl.BlockSpec((None, width, ff), lambda i: (0, 0, 0), pipeline_mode=pl.Buffered(1)),
                pl.BlockSpec((None, width, ff), lambda i: (0, 0, 0), pipeline_mode=pl.Buffered(1)),
                pl.BlockSpec((None, ff, width), lambda i: (0, 0, 0), pipeline_mode=pl.Buffered(1)),
            ],
            out_specs=pl.BlockSpec((m, width), lambda i: (i, 0)),
            scratch_shapes=[pltpu.VMEM((m, width), BF16)],
            name='ffn',
        )(all_tab, all_x, w_gate, w_up, w_down)
        back = lax.all_to_all(out.reshape(experts, CAP, width), 'expert', 0, 0, tiled=True).reshape(slots, width)
        nt = 512
        return pl.pallas_call(
            combine_kernel,
            grid=(width // nt,),
            out_shape=jax.ShapeDtypeStruct((tok, width), BF16),
            in_specs=[pl.BlockSpec((4 * tok, experts), lambda i: (0, 0)), pl.BlockSpec((slots, nt), lambda i: (0, i))],
            out_specs=pl.BlockSpec((tok, nt), lambda i: (0, i)),
            scratch_shapes=[pltpu.VMEM((3 * tok, slots), BF16)],
            name='combine',
        )(aux, back)

    return jax.shard_map(device_step, mesh=mesh, in_specs=(row_spec, P(None, None), row_spec, expert_spec, expert_spec, expert_spec), out_specs=row_spec, check_vma=False)
```

```python
import functools

import jax
import jax.numpy as jnp
from jax import lax
from jax.experimental import pallas as pl
from jax.experimental.pallas import tpu as pltpu
from jax.sharding import PartitionSpec as P

F32 = jnp.float32
BF16 = jnp.bfloat16
CAP = 8
ORDERS = ((2, 1, 0), (1, 0, 2), (0, 2, 1))


def _iota(shape, dim):
    return lax.broadcasted_iota(jnp.int32, shape, dim)


def prep_kernel(x_ref, wr_ref, r_ref, tab_ref):
    tok, experts = x_ref.shape[0], wr_ref.shape[1]
    logits = jnp.dot(x_ref[...], wr_ref[...], preferred_element_type=F32)
    routes = r_ref[...]
    lane = _iota((tok, experts), 1)
    hit = jnp.zeros((tok, experts), F32)
    for j in range(routes.shape[1]):
        hit += (routes[:, j:j + 1] == lane).astype(F32)
    on = hit > 0.5
    masked = jnp.where(on, logits, -jnp.inf)
    top = jnp.max(masked, axis=1, keepdims=True)
    e = jnp.where(on, jnp.exp(jnp.where(on, logits, top) - top), 0.0)
    gate = e / jnp.sum(e, axis=1, keepdims=True)
    below = (_iota((tok, tok), 1) < _iota((tok, tok), 0)).astype(BF16)
    rank = jnp.dot(below, hit.astype(BF16), preferred_element_type=F32)
    rank = jnp.where(on, rank, -1.0)
    row = _iota((tok, experts), 0).astype(F32)
    toks, gates = [], []
    for r in range(CAP):
        at = rank == r
        toks.append(jnp.sum(jnp.where(at, row + 1.0, 0.0), axis=0, keepdims=True) - 1.0)
        gates.append(jnp.sum(jnp.where(at, gate, 0.0), axis=0, keepdims=True))
    tab_ref[...] = jnp.concatenate(toks + gates, axis=0)


def moe_kernel(n, parts, x_ref, tab_ref, wg_hbm, wu_hbm, wd_hbm, y_ref, wg, wu, wd, rbuf, obuf, *rest):
    np_ = len(parts)
    tbuf, xbuf, sbuf, cbuf, bbuf, pbuf, abuf = [rest[i * np_:(i + 1) * np_] for i in range(7)]
    (w_sem, ta_s, ta_r, tb_s, tb_r, xa_s, xa_r, xb_s, xb_r, c_s, c_r, rc_s, rc_r, rb_s, rb_r, ra_s, ra_r) = rest[7 * np_:]
    tok = x_ref.shape[0]
    experts = tab_ref.shape[1]
    me = lax.axis_index('expert')
    strides = (2 * n * n, 2 * n, 2)
    pos = tuple(lax.rem(me // s, n) for s in strides)
    core = lax.rem(me, 2)

    def moved(axis, d, flip=0):
        other = me + (lax.rem(pos[axis] + d, n) - pos[axis]) * strides[axis]
        return other + (1 - 2 * core) if flip else other

    def put(src, dst, send, recv, device):
        pltpu.make_async_remote_copy(src_ref=src, dst_ref=dst, send_sem=send, recv_sem=recv,
                                     device_id={'expert': device}, device_id_type=pl.DeviceIdType.MESH).start()

    def drain(ref, sem):
        pltpu.make_async_copy(ref, ref, sem).wait()

    loads = [pltpu.make_async_copy(src, dst, w_sem.at[i]) for i, (src, dst) in enumerate(((wg_hbm.at[0], wg), (wu_hbm.at[0], wu), (wd_hbm.at[0], wd)))]
    for load in loads:
        load.start()

    barrier = pltpu.get_barrier_semaphore()
    peers = [moved(axis, d, flip) for axis in range(3) for d in range(1, n) for flip in (0, 1)] + [moved(0, 0, 1)]
    for peer in peers:
        pl.semaphore_signal(barrier, inc=1, device_id={'expert': peer}, device_id_type=pl.DeviceIdType.MESH)
    pl.semaphore_wait(barrier, len(peers))

    def canon(ref, p, a, b, k, c):
        axes = ORDERS[p]
        index = [None] * 3
        index[axes[0]], index[axes[1]], index[axes[2]] = a, b, k
        off, w = parts[p]
        return ref.at[index[0], index[1], index[2], c, :, pl.ds(off, w)]

    every = pl.ds(0, n)
    at = [tuple(pos[axis] for axis in ORDERS[p]) for p in range(np_)]

    for p in range(np_):
        a, b, _ = at[p]
        for d in range(1, n):
            put(tab_ref, tbuf[p].at[b, a], ta_s.at[p], ta_r.at[p], moved(ORDERS[p][0], d))
    for d in range(1, n):
        for p in range(np_):
            a, b, _ = at[p]
            off, w = parts[p]
            put(x_ref.at[:, pl.ds(off, w)], xbuf[p].at[b, a], xa_s.at[p], xa_r.at[p, d - 1], moved(ORDERS[p][0], d))
    for d in range(1, n):
        for p in range(np_):
            a, b, _ = at[p]
            off, w = parts[p]
            put(x_ref.at[:, pl.ds(off, w)], xbuf[p].at[b, a], xb_s.at[p], xb_r.at[p, d - 1], moved(ORDERS[p][1], d))
    for p in range(np_):
        a, b, _ = at[p]
        off, w = parts[p]
        xbuf[p][b, a] = x_ref[:, off:off + w]
        tbuf[p][b, a] = tab_ref[...]
    for p in range(np_):
        a, b, _ = at[p]
        drain(tbuf[p].at[0, pl.ds(0, n - 1)], ta_r.at[p])
        for d in range(1, n):
            put(tbuf[p].at[b], tbuf[p].at[b], tb_s.at[p], tb_r.at[p], moved(ORDERS[p][1], d))
    for da in range(1, n):
        for p in range(np_):
            a, b, _ = at[p]
            src = lax.rem(a + n - da, n)
            drain(xbuf[p].at[0, 0], xa_r.at[p, da - 1])
            for d in range(1, n):
                put(xbuf[p].at[b, src], xbuf[p].at[b, src], xb_s.at[p], xb_r.at[p, d - 1], moved(ORDERS[p][1], d))
    for db in range(n):
        for p in range(np_):
            a, b, k = at[p]
            axis_c = ORDERS[p][2]
            off, w = parts[p]
            bb = lax.rem(b + n - db, n)
            if db == 1:
                drain(tbuf[p].at[pl.ds(0, n - 1)], tb_r.at[p])
            if db:
                drain(xbuf[p].at[0], xb_r.at[p, db - 1])
            table = tbuf[p][bb][:, :CAP].reshape(n * CAP, experts)
            shift = (_iota((n * CAP, 1), 0) // CAP * tok).astype(F32)
            lane = _iota((n * CAP, experts), 1)
            token = _iota((n * CAP, n * tok), 1).astype(F32)
            picks = []
            for dk in range(n):
                for flip in range(2):
                    col = jnp.sum(jnp.where(lane == moved(axis_c, dk, flip), table, 0.0), axis=1, keepdims=True)
                    want = jnp.where(col >= 0.0, col + shift, -1.0)
                    picks.append((want == token).astype(F32))
            pick = jnp.concatenate(picks, axis=0).astype(BF16)
            rows = jnp.dot(pick, xbuf[p][bb].reshape(n * tok, w), preferred_element_type=F32).astype(BF16)
            rows = rows.reshape(2 * n, n, CAP, w)
            sbuf[p][db] = rows
            index = [None] * 3
            index[ORDERS[p][0]], index[ORDERS[p][1]], index[axis_c] = slice(None), bb, k
            rbuf[index[0], index[1], index[2], core, :, off:off + w] = rows[0]
            for q in range(1, 2 * n):
                put(sbuf[p].at[db, q], canon(rbuf, p, every, bb, k, core), c_s.at[p], c_r.at[p], moved(axis_c, q // 2, q % 2))

    for load in loads:
        load.wait()
    for p in range(np_):
        drain(sbuf[p].at[:, pl.ds(0, 2 * n - 1)], c_r.at[p])

    def expert(i, carry):
        rows = rbuf[i].reshape(n * n * 2 * CAP, x_ref.shape[1])
        g = jnp.dot(rows, wg[...], preferred_element_type=F32)
        u = jnp.dot(rows, wu[...], preferred_element_type=F32)
        h = (g * jax.nn.sigmoid(g) * u).astype(BF16)
        o = jnp.dot(h, wd[...], preferred_element_type=F32).astype(BF16)
        obuf[i] = o.reshape(n, n, 2, CAP, x_ref.shape[1])
        return carry

    lax.fori_loop(0, n, expert, 0)

    for db in range(n):
        for p in range(np_):
            a, b, k = at[p]
            axis_c = ORDERS[p][2]
            off, w = parts[p]
            bb = lax.rem(b + db, n)
            mine = k * 2 + core
            for q in range(1, 2 * n):
                dk, flip = q // 2, q % 2
                there = lax.rem(k + dk, n)
                c = 1 - core if flip else core
                put(canon(obuf, p, every, bb, there, c), cbuf[p].at[bb, :, mine], rc_s.at[p], rc_r.at[p, (n - db) % n], moved(axis_c, dk, flip))
            index = [None] * 3
            index[ORDERS[p][0]], index[ORDERS[p][1]], index[axis_c] = slice(None), bb, k
            cbuf[p][bb, :, mine] = obuf[index[0], index[1], index[2], core, :, off:off + w]
    for db in list(range(1, n)) + [0]:
        for p in range(np_):
            a, b, _ = at[p]
            bb = lax.rem(b + db, n)
            drain(cbuf[p].at[0, :, pl.ds(0, 2 * n - 1)], rc_r.at[p, (n - db) % n])
            if db:
                put(cbuf[p].at[bb], bbuf[p].at[:, b], rb_s.at[p], rb_r.at[p], moved(ORDERS[p][1], db))
            else:
                bbuf[p][:, b] = cbuf[p][b]
    cols = n * 2 * n * CAP
    for p in range(np_):
        a, b, k = at[p]
        axis_a, axis_b, axis_c = ORDERS[p]
        off, w = parts[p]
        drain(cbuf[p].at[pl.ds(0, n - 1)], rb_r.at[p])
        slot = _iota((experts, cols), 1)
        ident = (slot // (2 * n * CAP) * strides[axis_b] + lax.rem(slot // (2 * CAP), n) * strides[axis_c]
                 + lax.rem(slot // CAP, 2) + a * strides[axis_a])
        spread = (ident == _iota((experts, cols), 0)).astype(BF16)
        keep = _iota((CAP, cols), 0) == lax.rem(_iota((CAP, cols), 1), CAP)
        for da in list(range(1, n)) + [0]:
            aa = lax.rem(a + da, n)
            tg = tbuf[p][b, aa]
            gate = tg[CAP:]
            g1 = gate.astype(BF16).astype(F32)
            g2 = (gate - g1).astype(BF16).astype(F32)
            g3 = gate - g1 - g2
            wide = jnp.dot(jnp.concatenate([tg[:CAP], g1, g2, g3], axis=0).astype(BF16), spread, preferred_element_type=F32)
            line = [jnp.sum(jnp.where(keep, wide[i * CAP:(i + 1) * CAP], 0.0), axis=0, keepdims=True) for i in range(4)]
            here = line[0] == _iota((tok, cols), 0).astype(F32)
            mix = jnp.concatenate([jnp.where(here, line[i], 0.0) for i in (1, 2, 3)], axis=0).astype(BF16)
            part = jnp.dot(mix, bbuf[p][aa].reshape(cols, w), preferred_element_type=F32)
            part = part[:tok] + part[tok:2 * tok] + part[2 * tok:]
            if da:
                pbuf[p][da - 1] = part
                put(pbuf[p].at[da - 1], abuf[p].at[a], ra_s.at[p], ra_r.at[p], moved(axis_a, da))
            else:
                abuf[p][a] = part
    for p in range(np_):
        off, w = parts[p]
        drain(pbuf[p], ra_r.at[p])
        total = abuf[p][0]
        for i in range(1, n):
            total += abuf[p][i]
        y_ref[:, off:off + w] = total.astype(BF16)
    for p in range(np_):
        drain(tbuf[p].at[0, pl.ds(0, n - 1)], ta_s.at[p])
        drain(tbuf[p].at[pl.ds(0, n - 1)], tb_s.at[p])
        drain(xbuf[p].at[0, pl.ds(0, n - 1)], xa_s.at[p])
        drain(xbuf[p].at[pl.ds(0, n - 1)], xb_s.at[p])
        drain(sbuf[p].at[:, pl.ds(0, 2 * n - 1)], c_s.at[p])
        drain(cbuf[p].at[:, :, pl.ds(0, 2 * n - 1)], rc_s.at[p])
        drain(cbuf[p].at[pl.ds(0, n - 1)], rb_s.at[p])
        drain(pbuf[p], ra_s.at[p])


def build(mesh, n, parts):
    row_spec = P(('data', 'expert'), None)
    expert_spec = P('expert', None, None)
    vmem = pl.BlockSpec(memory_space=pltpu.VMEM)
    hbm = pl.BlockSpec(memory_space=pl.ANY)

    def device_step(tokens, w_router, routes, w_gate, w_up, w_down):
        tok, width = tokens.shape
        experts = w_router.shape[1]
        ff = w_gate.shape[2]
        tab = pl.pallas_call(
            prep_kernel, out_shape=jax.ShapeDtypeStruct((2 * CAP, experts), F32),
            in_specs=[vmem] * 3, out_specs=vmem, name='prep',
        )(tokens, w_router, routes)
        dma = pltpu.SemaphoreType.DMA
        np_ = len(parts)
        return pl.pallas_call(
            functools.partial(moe_kernel, n, parts),
            out_shape=jax.ShapeDtypeStruct((tok, width), BF16),
            in_specs=[vmem, vmem, hbm, hbm, hbm], out_specs=vmem,
            scratch_shapes=[
                pltpu.VMEM((width, ff), BF16), pltpu.VMEM((width, ff), BF16), pltpu.VMEM((ff, width), BF16),
                pltpu.VMEM((n, n, n, 2, CAP, width), BF16), pltpu.VMEM((n, n, n, 2, CAP, width), BF16),
                *[pltpu.VMEM((n, n, 2 * CAP, experts), F32) for _ in parts],
                *[pltpu.VMEM((n, n, tok, w), BF16) for _, w in parts],
                *[pltpu.VMEM((n, 2 * n, n, CAP, w), BF16) for _, w in parts],
                *[pltpu.VMEM((n, n, 2 * n, CAP, w), BF16) for _, w in parts],
                *[pltpu.VMEM((n, n, 2 * n, CAP, w), BF16) for _, w in parts],
                *[pltpu.VMEM((n - 1, tok, w), F32) for _, w in parts],
                *[pltpu.VMEM((n, tok, w), F32) for _, w in parts],
                dma((3,)), dma((np_,)), dma((np_,)), dma((np_,)), dma((np_,)),
                dma((np_,)), dma((np_, n - 1)), dma((np_,)), dma((np_, n - 1)), dma((np_,)), dma((np_,)),
                dma((np_,)), dma((np_, n)), dma((np_,)), dma((np_,)), dma((np_,)), dma((np_,)),
            ],
            compiler_params=pltpu.CompilerParams(collective_id=0, has_side_effects=True, vmem_limit_bytes=60 * 1024 * 1024),
            name='moe',
        )(tokens, tab, w_gate, w_up, w_down)

    return jax.shard_map(device_step, mesh=mesh, in_specs=(row_spec, P(None, None), row_spec, expert_spec, expert_spec, expert_spec), out_specs=row_spec, check_vma=False)


def solution(mesh):
    return build(mesh, 4, ((0, 768), (768, 640), (1408, 640)))
```

```python
import functools

import jax
import jax.numpy as jnp
from jax import lax
from jax.experimental import pallas as pl
from jax.experimental.pallas import tpu as pltpu
from jax.sharding import PartitionSpec as P

F32 = jnp.float32
BF16 = jnp.bfloat16
CAP = 8


def _iota(shape, dim):
    return lax.broadcasted_iota(jnp.int32, shape, dim)


def _places(r):
    return (2 - r) % 3, (1 - r) % 3, (-r) % 3


def routing_table(x, wr, routes_t):
    tok, experts = x.shape[0], wr.shape[1]
    top_k = routes_t.shape[0]
    logits = jnp.dot(x, wr, preferred_element_type=F32)
    eye = (_iota((top_k, top_k), 0) == _iota((top_k, top_k), 1)).astype(BF16)
    routes = lax.dot_general(routes_t.astype(F32).astype(BF16), eye, (((0,), (0,)), ((), ())), preferred_element_type=F32)
    lane = _iota((tok, experts), 1).astype(F32)
    hit = jnp.zeros((tok, experts), F32)
    for j in range(top_k):
        hit += (routes[:, j:j + 1] == lane).astype(F32)
    on = hit > 0.5
    top = jnp.max(jnp.where(on, logits, -jnp.inf), axis=1, keepdims=True)
    e = jnp.where(on, jnp.exp(jnp.where(on, logits, top) - top), 0.0)
    gate = e / jnp.sum(e, axis=1, keepdims=True)
    below = (_iota((tok, tok), 1) < _iota((tok, tok), 0)).astype(BF16)
    rank = jnp.dot(below, hit.astype(BF16), preferred_element_type=F32)
    rank = jnp.where(on, rank, -1.0)
    row = _iota((tok, experts), 0).astype(F32)
    toks, gates = [], []
    for r in range(CAP):
        at = rank == r
        toks.append(jnp.sum(jnp.where(at, row + 1.0, 0.0), axis=0, keepdims=True) - 1.0)
        gates.append(jnp.sum(jnp.where(at, gate, 0.0), axis=0, keepdims=True))
    return jnp.concatenate(toks + gates, axis=0)


def moe_kernel(n, parts, x_ref, wr_ref, rt_ref, wg_hbm, wu_hbm, wd_hbm, y_ref, wg, wu, wd, rbuf, obuf, tab_ref, *rest):
    np_ = len(parts)
    tbuf, xbuf, sbuf, cbuf, bbuf, pbuf, abuf, mixbuf = [rest[i * np_:(i + 1) * np_] for i in range(8)]
    (w_sem, ta_s, ta_r, tb_s, tb_r, xa_s, xa_r, xb_s, xb_r, c_s, c_r, rc_s, rc_r, rb_s, rb_r, ra_s, ra_r) = rest[8 * np_:]
    tok, width = x_ref.shape
    experts = tab_ref.shape[1]
    me = lax.axis_index('expert')
    strides = (2 * n * n, 2 * n, 2)
    pos = tuple(lax.rem(me // s, n) for s in strides)
    core = lax.rem(me, 2)
    mod = lambda v: lax.rem(v, n)

    def order(p, cc):
        r0, r1 = _places(p % 3), _places((p + 1) % 3)
        return [(pos[i] + cc * (pos[j] - pos[i]), strides[i] + cc * (strides[j] - strides[i])) for i, j in zip(r0, r1)]

    mine = [order(p, core) for p in range(np_)]
    theirs = [order(p, 1 - core) for p in range(np_)]

    def moved(axis, d, flip=0):
        where, stride = axis
        other = me + (mod(where + d) - where) * stride
        return other + (1 - 2 * core) if flip else other

    def put(src, dst, send, recv, device):
        pltpu.make_async_remote_copy(src_ref=src, dst_ref=dst, send_sem=send, recv_sem=recv,
                                     device_id={'expert': device}, device_id_type=pl.DeviceIdType.MESH).start()

    def drain(ref, sem):
        pltpu.make_async_copy(ref, ref, sem).wait()

    def canon(p, cc, a, b, k):
        r0, r1 = _places(p % 3), _places((p + 1) % 3)
        v = (a, b, k)
        return [v[r0.index(j)] + cc * (v[r1.index(j)] - v[r0.index(j)]) for j in (0, 1)]

    loads = [pltpu.make_async_copy(src, dst, w_sem.at[i]) for i, (src, dst) in enumerate(((wg_hbm.at[0], wg), (wu_hbm.at[0], wu), (wd_hbm.at[0], wd)))]
    for load in loads:
        load.start()

    barrier = pltpu.get_barrier_semaphore()
    peers = [moved((pos[j], strides[j]), d, flip) for j in range(3) for d in range(1, n) for flip in (0, 1)] + [me + 1 - 2 * core]
    for peer in peers:
        pl.semaphore_signal(barrier, inc=1, device_id={'expert': peer}, device_id_type=pl.DeviceIdType.MESH)
    pl.semaphore_wait(barrier, len(peers))

    for axis, send, recv in ((0, xa_s, xa_r), (1, xb_s, xb_r)):
        for d in range(1, n):
            for p, (off, w) in enumerate(parts):
                (a, _), (b, _), _ = mine[p]
                put(x_ref.at[:, pl.ds(off, w)], xbuf[p].at[b, a], send.at[p], recv.at[p, d - 1], moved(mine[p][axis], d))
    tab_ref[...] = routing_table(x_ref[...], wr_ref[...], rt_ref[...])
    for p, (off, w) in enumerate(parts):
        (a, _), (b, _), _ = mine[p]
        xbuf[p][b, a] = x_ref[:, off:off + w]
        tbuf[p][b, a] = tab_ref[...]
    for p in range(np_):
        (a, _), (b, _), _ = mine[p]
        for d in range(1, n):
            put(tab_ref, tbuf[p].at[b, a], ta_s.at[p], ta_r.at[p], moved(mine[p][0], d))
    for da in range(1, n):
        for p in range(np_):
            (a, _), (b, _), _ = mine[p]
            src = mod(a + n - da)
            drain(xbuf[p].at[0, 0], xa_r.at[p, da - 1])
            for d in range(1, n):
                put(xbuf[p].at[b, src], xbuf[p].at[b, src], xb_s.at[p], xb_r.at[p, d - 1], moved(mine[p][1], d))
    for p in range(np_):
        b = mine[p][1][0]
        drain(tbuf[p].at[0, pl.ds(0, n - 1)], ta_r.at[p])
        for d in range(1, n):
            put(tbuf[p].at[b], tbuf[p].at[b], tb_s.at[p], tb_r.at[p], moved(mine[p][1], d))

    def select(p, db):
        off, w = parts[p]
        (a, _), (b, _), (k, _) = mine[p]
        bb = mod(b + n - db)
        table = tbuf[p][bb][:, :CAP].reshape(n * CAP, experts)
        shift = (_iota((n * CAP, 1), 0) // CAP * tok).astype(F32)
        lane = _iota((n * CAP, experts), 1)
        token = _iota((n * CAP, n * tok), 1).astype(F32)
        picks = []
        for q in range(2 * n):
            col = jnp.sum(jnp.where(lane == moved(mine[p][2], q // 2, q % 2), table, 0.0), axis=1, keepdims=True)
            want = jnp.where(col >= 0.0, col + shift, -1.0)
            picks.append((want == token).astype(F32))
        pick = jnp.concatenate(picks, axis=0).astype(BF16)
        rows = jnp.dot(pick, xbuf[p][bb].reshape(n * tok, w), preferred_element_type=F32).astype(BF16)
        sbuf[p][db] = rows.reshape(2 * n, n, CAP, w)

    def send_rows(p, db, i):
        off, w = parts[p]
        (a, _), (b, _), (k, _) = mine[p]
        bb = mod(b + n - db)
        aa = mod(i + 2 * n - bb - k)
        z, y = canon(p, core, aa, bb, k)
        for q in range(1, 2 * n):
            put(sbuf[p].at[db, q, aa], rbuf.at[i, z, y, core, :, pl.ds(off, w)], c_s.at[p], c_r.at[p, i], moved(mine[p][2], q // 2, q % 2))
        rbuf[i, z, y, core, :, off:off + w] = sbuf[p][db, 0, aa]

    def chunk_rows(i, dbs):
        for db in dbs:
            for p in range(np_):
                send_rows(p, db, i)

    def body(dbs):
        def run(i, carry):
            chunk_rows(i, dbs)
            return carry
        return run

    for p in range(np_):
        select(p, 0)
    lax.fori_loop(0, n, body((0,)), 0)
    for db in range(1, n):
        for p in range(np_):
            if db == 1:
                drain(tbuf[p].at[pl.ds(0, n - 1)], tb_r.at[p])
            drain(xbuf[p].at[0], xb_r.at[p, db - 1])
            select(p, db)
        chunk_rows(0, (db,))
    lax.fori_loop(1, n, body(tuple(range(1, n))), 0)

    cols = n * 2 * n * CAP
    for p in range(np_):
        (a, sa), (b, sb), (_, sc) = mine[p]
        slot = _iota((experts, cols), 1)
        ident = slot // (2 * n * CAP) * sb + lax.rem(slot // (2 * CAP), n) * sc + lax.rem(slot // CAP, 2) + a * sa
        spread = (ident == _iota((experts, cols), 0)).astype(BF16)
        keep = _iota((CAP, cols), 0) == lax.rem(_iota((CAP, cols), 1), CAP)
        for aa in range(n):
            tg = tbuf[p][b, aa]
            gate = tg[CAP:]
            g1 = gate.astype(BF16).astype(F32)
            g2 = (gate - g1).astype(BF16).astype(F32)
            g3 = gate - g1 - g2
            wide = jnp.dot(jnp.concatenate([tg[:CAP], g1, g2, g3], axis=0).astype(BF16), spread, preferred_element_type=F32)
            line = [jnp.sum(jnp.where(keep, wide[i * CAP:(i + 1) * CAP], 0.0), axis=0, keepdims=True) for i in range(4)]
            here = line[0] == _iota((tok, cols), 0).astype(F32)
            mixbuf[p][aa] = jnp.concatenate([jnp.where(here, line[i], 0.0) for i in (1, 2, 3)], axis=0).astype(BF16)

    for load in loads:
        load.wait()

    def expert(i, carry):
        for p in range(np_):
            drain(sbuf[p].at[:, pl.ds(0, 2 * n - 1), 0], c_r.at[p, i])
        rows = rbuf[i].reshape(n * n * 2 * CAP, width)
        g = jnp.dot(rows, wg[...], preferred_element_type=F32)
        u = jnp.dot(rows, wu[...], preferred_element_type=F32)
        h = (g * jax.nn.sigmoid(g) * u).astype(BF16)
        o = jnp.dot(h, wd[...], preferred_element_type=F32).astype(BF16)
        obuf[i] = o.reshape(n, n, 2, CAP, width)
        for db in list(range(1, n)) + [0]:
            for q in list(range(1, 2 * n)) + [0]:
                for p, (off, w) in enumerate(parts):
                    cc, axes = (1 - core, theirs[p]) if q % 2 else (core, mine[p])
                    (_, _), (b, _), (k, _) = axes
                    kk, bb = mod(k + q // 2), mod(b + db)
                    aa = mod(i + 2 * n - bb - kk)
                    z, y = canon(p, cc, aa, bb, kk)
                    if q:
                        put(obuf.at[i, z, y, cc, :, pl.ds(off, w)], cbuf[p].at[bb, aa, k * 2 + core],
                            rc_s.at[p], rc_r.at[p, db, i], moved(axes[2], q // 2, q % 2))
                    else:
                        cbuf[p][bb, aa, k * 2 + core] = obuf[i, z, y, cc, :, off:off + w]
        return carry

    lax.fori_loop(0, n, expert, 0)

    def forward(i):
        for db in list(range(1, n)) + [0]:
            for p in range(np_):
                _, (b, _), (k, _) = mine[p]
                bb = mod(b + db)
                aa = mod(i + 2 * n - bb - k)
                drain(cbuf[p].at[0, 0, pl.ds(0, 2 * n - 1)], rc_r.at[p, db, i])
                if db:
                    put(cbuf[p].at[bb, aa], bbuf[p].at[aa, b], rb_s.at[p], rb_r.at[p, i], moved(mine[p][1], db))
                else:
                    bbuf[p][aa, b] = cbuf[p][b, aa]

    def weigh(i):
        for p in range(np_):
            off, w = parts[p]
            (a, sa), (b, _), (k, _) = mine[p]
            aa = mod(i + 2 * n - b - k)
            drain(cbuf[p].at[0, pl.ds(0, n - 1)], rb_r.at[p, i])
            part = jnp.dot(mixbuf[p][aa], bbuf[p][aa].reshape(cols, w), preferred_element_type=F32)
            pbuf[p][i] = part[:tok] + part[tok:2 * tok] + part[2 * tok:]

            @pl.when(aa != a)
            def _():
                put(pbuf[p].at[i], abuf[p].at[a], ra_s.at[p], ra_r.at[p], me + (aa - a) * sa)

            @pl.when(aa == a)
            def _():
                abuf[p][a] = pbuf[p][i]

    for i in range(n):
        forward(i)
        if i:
            weigh(i - 1)
    weigh(n - 1)
    for p, (off, w) in enumerate(parts):
        drain(pbuf[p].at[pl.ds(0, n - 1)], ra_r.at[p])
        total = abuf[p][0]
        for i in range(1, n):
            total += abuf[p][i]
        y_ref[:, off:off + w] = total.astype(BF16)
    for p in range(np_):
        drain(tbuf[p].at[0, pl.ds(0, n - 1)], ta_s.at[p])
        drain(tbuf[p].at[pl.ds(0, n - 1)], tb_s.at[p])
        drain(xbuf[p].at[0, pl.ds(0, n - 1)], xa_s.at[p])
        drain(xbuf[p].at[pl.ds(0, n - 1)], xb_s.at[p])
        drain(sbuf[p].at[:, pl.ds(0, 2 * n - 1)], c_s.at[p])
        drain(cbuf[p].at[:, :, pl.ds(0, 2 * n - 1)], rc_s.at[p])
        drain(cbuf[p].at[pl.ds(0, n - 1)], rb_s.at[p])
        drain(pbuf[p].at[pl.ds(0, n - 1)], ra_s.at[p])


def build(mesh, n, parts):
    row_spec = P(('data', 'expert'), None)
    expert_spec = P('expert', None, None)
    vmem = pl.BlockSpec(memory_space=pltpu.VMEM)
    hbm = pl.BlockSpec(memory_space=pl.ANY)

    def device_step(tokens, w_router, routes, w_gate, w_up, w_down):
        tok, width = tokens.shape
        experts = w_router.shape[1]
        ff = w_gate.shape[2]
        dma = pltpu.SemaphoreType.DMA
        np_ = len(parts)
        cols = n * 2 * n * CAP
        return pl.pallas_call(
            functools.partial(moe_kernel, n, parts),
            out_shape=jax.ShapeDtypeStruct((tok, width), BF16),
            in_specs=[vmem, vmem, vmem, hbm, hbm, hbm], out_specs=vmem,
            scratch_shapes=[
                pltpu.VMEM((width, ff), BF16), pltpu.VMEM((width, ff), BF16), pltpu.VMEM((ff, width), BF16),
                pltpu.VMEM((n, n, n, 2, CAP, width), BF16), pltpu.VMEM((n, n, n, 2, CAP, width), BF16),
                pltpu.VMEM((2 * CAP, experts), F32),
                *[pltpu.VMEM((n, n, 2 * CAP, experts), F32) for _ in parts],
                *[pltpu.VMEM((n, n, tok, w), BF16) for _, w in parts],
                *[pltpu.VMEM((n, 2 * n, n, CAP, w), BF16) for _, w in parts],
                *[pltpu.VMEM((n, n, 2 * n, CAP, w), BF16) for _, w in parts],
                *[pltpu.VMEM((n, n, 2 * n, CAP, w), BF16) for _, w in parts],
                *[pltpu.VMEM((n, tok, w), F32) for _, w in parts],
                *[pltpu.VMEM((n, tok, w), F32) for _, w in parts],
                *[pltpu.VMEM((n, 3 * tok, cols), BF16) for _ in parts],
                dma((3,)), dma((np_,)), dma((np_,)), dma((np_,)), dma((np_,)),
                dma((np_,)), dma((np_, n - 1)), dma((np_,)), dma((np_, n - 1)), dma((np_,)), dma((np_, n)),
                dma((np_,)), dma((np_, n, n)), dma((np_,)), dma((np_, n)), dma((np_,)), dma((np_,)),
            ],
            compiler_params=pltpu.CompilerParams(collective_id=0, has_side_effects=True, vmem_limit_bytes=60 * 1024 * 1024),
            name='moe',
        )(tokens, w_router, routes.T, w_gate, w_up, w_down)

    return jax.shard_map(device_step, mesh=mesh, in_specs=(row_spec, P(None, None), row_spec, expert_spec, expert_spec, expert_spec), out_specs=row_spec, check_vma=False)


def solution(mesh):
    return build(mesh, 4, ((0, 768), (768, 640), (1408, 640)))
```

```python
import functools

import jax
import jax.numpy as jnp
from jax import lax
from jax.experimental import pallas as pl
from jax.experimental.pallas import tpu as pltpu
from jax.sharding import PartitionSpec as P

F32 = jnp.float32
BF16 = jnp.bfloat16
CAP = 8


def _iota(shape, dim):
    return lax.broadcasted_iota(jnp.int32, shape, dim)


def _places(r):
    return (2 - r) % 3, (1 - r) % 3, (-r) % 3


def routing_table(x, wr, routes_t):
    tok, experts = x.shape[0], wr.shape[1]
    top_k = routes_t.shape[0]
    logits = jnp.dot(x, wr, preferred_element_type=F32)
    eye = (_iota((top_k, top_k), 0) == _iota((top_k, top_k), 1)).astype(BF16)
    routes = lax.dot_general(routes_t.astype(F32).astype(BF16), eye, (((0,), (0,)), ((), ())), preferred_element_type=F32)
    lane = _iota((tok, experts), 1).astype(F32)
    hit = jnp.zeros((tok, experts), F32)
    for j in range(top_k):
        hit += (routes[:, j:j + 1] == lane).astype(F32)
    on = hit > 0.5
    top = jnp.max(jnp.where(on, logits, -jnp.inf), axis=1, keepdims=True)
    e = jnp.where(on, jnp.exp(jnp.where(on, logits, top) - top), 0.0)
    gate = e / jnp.sum(e, axis=1, keepdims=True)
    below = (_iota((tok, tok), 1) < _iota((tok, tok), 0)).astype(BF16)
    rank = jnp.dot(below, hit.astype(BF16), preferred_element_type=F32)
    rank = jnp.where(on, rank, -1.0)
    row = _iota((tok, experts), 0).astype(F32)
    toks, gates = [], []
    for r in range(CAP):
        at = rank == r
        toks.append(jnp.sum(jnp.where(at, row + 1.0, 0.0), axis=0, keepdims=True) - 1.0)
        gates.append(jnp.sum(jnp.where(at, gate, 0.0), axis=0, keepdims=True))
    return jnp.concatenate(toks + gates, axis=0)


def moe_kernel(n, parts, lefts, x_ref, wr_ref, rt_ref, wg_hbm, wu_hbm, wd_hbm, y_ref, wg, wu, wd, rbuf, obuf, tab_ref, *rest):
    np_ = len(parts)
    tbuf, xbuf, sbuf, cbuf, farp, fari, nearp, neari, pbuf, abuf, mixbuf = [rest[i * np_:(i + 1) * np_] for i in range(11)]
    (w_sem, ta_s, ta_r, tb_s, tb_r, xa_s, xa_r, xb_s, xb_r, c_s, c_r, rc_s, rc_r, rf_s, rf_r, rn_s, rn_r, ra_s, ra_r) = rest[11 * np_:]
    tok, width = x_ref.shape
    experts = tab_ref.shape[1]
    me = lax.axis_index('expert')
    strides = (2 * n * n, 2 * n, 2)
    pos = tuple(lax.rem(me // s, n) for s in strides)
    core = lax.rem(me, 2)
    mod = lambda v: lax.rem(v, n)

    def order(p, cc):
        r0, r1 = _places(p % 3), _places((p + 1) % 3)
        return [(pos[i] + cc * (pos[j] - pos[i]), strides[i] + cc * (strides[j] - strides[i])) for i, j in zip(r0, r1)]

    mine = [order(p, core) for p in range(np_)]
    theirs = [order(p, 1 - core) for p in range(np_)]

    def moved(axis, d, flip=0):
        where, stride = axis
        other = me + (mod(where + d) - where) * stride
        return other + (1 - 2 * core) if flip else other

    def put(src, dst, send, recv, device):
        pltpu.make_async_remote_copy(src_ref=src, dst_ref=dst, send_sem=send, recv_sem=recv,
                                     device_id={'expert': device}, device_id_type=pl.DeviceIdType.MESH).start()

    def drain(ref, sem):
        pltpu.make_async_copy(ref, ref, sem).wait()

    def canon(p, cc, a, b, k):
        r0, r1 = _places(p % 3), _places((p + 1) % 3)
        v = (a, b, k)
        return [v[r0.index(j)] + cc * (v[r1.index(j)] - v[r0.index(j)]) for j in (0, 1)]

    loads = [pltpu.make_async_copy(src, dst, w_sem.at[i]) for i, (src, dst) in enumerate(((wg_hbm.at[0], wg), (wu_hbm.at[0], wu), (wd_hbm.at[0], wd)))]
    for load in loads:
        load.start()

    barrier = pltpu.get_barrier_semaphore()
    peers = [moved((pos[j], strides[j]), d, flip) for j in range(3) for d in range(1, n) for flip in (0, 1)] + [me + 1 - 2 * core]
    for peer in peers:
        pl.semaphore_signal(barrier, inc=1, device_id={'expert': peer}, device_id_type=pl.DeviceIdType.MESH)
    pl.semaphore_wait(barrier, len(peers))

    for axis, send, recv in ((0, xa_s, xa_r), (1, xb_s, xb_r)):
        for d in range(1, n):
            for p, (off, w) in enumerate(parts):
                (a, _), (b, _), _ = mine[p]
                put(x_ref.at[:, pl.ds(off, w)], xbuf[p].at[b, a], send.at[p], recv.at[p, d - 1], moved(mine[p][axis], d))
    tab_ref[...] = routing_table(x_ref[...], wr_ref[...], rt_ref[...])
    for p, (off, w) in enumerate(parts):
        (a, _), (b, _), _ = mine[p]
        xbuf[p][b, a] = x_ref[:, off:off + w]
        tbuf[p][b, a] = tab_ref[...]
    for p in range(np_):
        (a, _), (b, _), _ = mine[p]
        for d in range(1, n):
            put(tab_ref, tbuf[p].at[b, a], ta_s.at[p], ta_r.at[p], moved(mine[p][0], d))
    for da in range(1, n):
        for p in range(np_):
            (a, _), (b, _), _ = mine[p]
            src = mod(a + n - da)
            drain(xbuf[p].at[0, 0], xa_r.at[p, da - 1])
            for d in range(1, n):
                put(xbuf[p].at[b, src], xbuf[p].at[b, src], xb_s.at[p], xb_r.at[p, d - 1], moved(mine[p][1], d))
    for p in range(np_):
        b = mine[p][1][0]
        drain(tbuf[p].at[0, pl.ds(0, n - 1)], ta_r.at[p])
        for d in range(1, n):
            put(tbuf[p].at[b], tbuf[p].at[b], tb_s.at[p], tb_r.at[p], moved(mine[p][1], d))

    def select(p, db):
        off, w = parts[p]
        (a, _), (b, _), (k, _) = mine[p]
        bb = mod(b + n - db)
        table = tbuf[p][bb][:, :CAP].reshape(n * CAP, experts)
        shift = (_iota((n * CAP, 1), 0) // CAP * tok).astype(F32)
        lane = _iota((n * CAP, experts), 1)
        token = _iota((n * CAP, n * tok), 1).astype(F32)
        picks = []
        for q in range(2 * n):
            col = jnp.sum(jnp.where(lane == moved(mine[p][2], q // 2, q % 2), table, 0.0), axis=1, keepdims=True)
            want = jnp.where(col >= 0.0, col + shift, -1.0)
            picks.append((want == token).astype(F32))
        pick = jnp.concatenate(picks, axis=0).astype(BF16)
        rows = jnp.dot(pick, xbuf[p][bb].reshape(n * tok, w), preferred_element_type=F32).astype(BF16)
        sbuf[p][db] = rows.reshape(2 * n, n, CAP, w)

    def send_rows(p, db, i):
        off, w = parts[p]
        (a, _), (b, _), (k, _) = mine[p]
        bb = mod(b + n - db)
        aa = mod(i + 2 * n - bb - k)
        z, y = canon(p, core, aa, bb, k)
        for q in range(1, 2 * n):
            put(sbuf[p].at[db, q, aa], rbuf.at[i, z, y, core, :, pl.ds(off, w)], c_s.at[p], c_r.at[p, i], moved(mine[p][2], q // 2, q % 2))
        rbuf[i, z, y, core, :, off:off + w] = sbuf[p][db, 0, aa]

    def chunk_rows(i, dbs):
        for db in dbs:
            for p in range(np_):
                send_rows(p, db, i)

    def body(dbs):
        def run(i, carry):
            chunk_rows(i, dbs)
            return carry
        return run

    for p in range(np_):
        select(p, 0)
    lax.fori_loop(0, n, body((0,)), 0)
    for db in range(1, n):
        for p in range(np_):
            if db == 1:
                drain(tbuf[p].at[pl.ds(0, n - 1)], tb_r.at[p])
            drain(xbuf[p].at[0], xb_r.at[p, db - 1])
            select(p, db)
        chunk_rows(0, (db,))
    lax.fori_loop(1, n, body(tuple(range(1, n))), 0)

    cols = 2 * n * CAP
    for p in range(np_):
        (a, sa), (b, sb), (_, sc) = mine[p]
        slot = _iota((experts, cols), 1)
        ident = slot // (2 * CAP) * sc + lax.rem(slot // CAP, 2) + a * sa + b * sb
        spread = (ident == _iota((experts, cols), 0)).astype(BF16)
        keep = _iota((CAP, cols), 0) == lax.rem(_iota((CAP, cols), 1), CAP)
        for bb in range(n):
            tg = tbuf[p][bb]
            gate = tg[:, CAP:]
            g1 = gate.astype(BF16).astype(F32)
            g2 = (gate - g1).astype(BF16).astype(F32)
            g3 = gate - g1 - g2
            terms = jnp.concatenate([tg[:, :CAP], g1, g2, g3], axis=1).reshape(n * 4 * CAP, experts).astype(BF16)
            wide = jnp.dot(terms, spread, preferred_element_type=F32)
            for aa in range(n):
                line = [jnp.sum(jnp.where(keep, wide[(aa * 4 + i) * CAP:(aa * 4 + i + 1) * CAP], 0.0), axis=0, keepdims=True) for i in range(4)]
                here = line[0] == _iota((tok, cols), 0).astype(F32)
                mixbuf[p][bb, aa] = jnp.concatenate([jnp.where(here, line[i], 0.0) for i in (1, 2, 3)], axis=0).astype(BF16)

    for load in loads:
        load.wait()

    ring = (2, 1, 3, 0) if n == 4 else tuple(range(1, n)) + (0,)

    def expert(i, carry):
        for p in range(np_):
            drain(sbuf[p].at[:, pl.ds(0, 2 * n - 1), 0], c_r.at[p, i])
        rows = rbuf[i].reshape(n * n * 2 * CAP, width)
        g = jnp.dot(rows, wg[...], preferred_element_type=F32)
        u = jnp.dot(rows, wu[...], preferred_element_type=F32)
        h = (g * jax.nn.sigmoid(g) * u).astype(BF16)
        o = jnp.dot(h, wd[...], preferred_element_type=F32).astype(BF16)
        obuf[i] = o.reshape(n, n, 2, CAP, width)
        for db in ring:
            for q in list(range(1, 2 * n)) + [0]:
                for p, (off, w) in enumerate(parts):
                    cc, axes = (1 - core, theirs[p]) if q % 2 else (core, mine[p])
                    (_, _), (b, _), (k, _) = axes
                    kk, bb = mod(k + q // 2), mod(b + db)
                    aa = mod(i + 2 * n - bb - kk)
                    z, y = canon(p, cc, aa, bb, kk)
                    if q:
                        put(obuf.at[i, z, y, cc, :, pl.ds(off, w)], cbuf[p].at[bb, aa, k * 2 + core],
                            rc_s.at[p], rc_r.at[p, db, i], moved(axes[2], q // 2, q % 2))
                    else:
                        cbuf[p][bb, aa, k * 2 + core] = obuf[i, z, y, cc, :, off:off + w]
        return carry

    lax.fori_loop(0, n, expert, 0)

    def line_sum(p, db, i):
        w = parts[p][1]
        _, (b, _), (k, _) = mine[p]
        bb = mod(b + db)
        aa = mod(i + 2 * n - bb - k)
        drain(cbuf[p].at[0, 0, pl.ds(0, 2 * n - 1)], rc_r.at[p, db, i])
        part = jnp.dot(mixbuf[p][bb, aa], cbuf[p][bb, aa].reshape(cols, w), preferred_element_type=F32)
        return part[:tok] + part[tok:2 * tok] + part[2 * tok:]

    def far(i):
        for p in range(np_):
            w, left = parts[p][1], lefts[p]
            farp[p][i] = line_sum(p, 2, i)
            put(farp[p].at[i, :, pl.ds(0, left)], fari[p].at[i, :, pl.ds(0, left)], rf_s.at[p], rf_r.at[p, i], moved(mine[p][1], 1))
            put(farp[p].at[i, :, pl.ds(left, w - left)], fari[p].at[i, :, pl.ds(left, w - left)], rf_s.at[p], rf_r.at[p, i], moved(mine[p][1], n - 1))

    def near(i):
        for p in range(np_):
            left = lefts[p]
            up, down = line_sum(p, 1, i), line_sum(p, n - 1, i)
            drain(fari[p].at[i], rf_r.at[p, i])
            nearp[p][i, 0, :, :left] = up[:, :left] + fari[p][i, :, :left]
            nearp[p][i, 0, :, left:] = up[:, left:]
            put(nearp[p].at[i, 0], neari[p].at[i, 0], rn_s.at[p], rn_r.at[p, i], moved(mine[p][1], 1))
            nearp[p][i, 1, :, :left] = down[:, :left]
            nearp[p][i, 1, :, left:] = down[:, left:] + fari[p][i, :, left:]
            put(nearp[p].at[i, 1], neari[p].at[i, 1], rn_s.at[p], rn_r.at[p, i], moved(mine[p][1], n - 1))

    def here(i):
        for p in range(np_):
            (a, sa), (b, _), (k, _) = mine[p]
            aa = mod(i + 2 * n - b - k)
            own = line_sum(p, 0, i)
            drain(neari[p].at[i], rn_r.at[p, i])
            pbuf[p][i] = own + neari[p][i, 0] + neari[p][i, 1]

            @pl.when(aa != a)
            def _():
                put(pbuf[p].at[i], abuf[p].at[a], ra_s.at[p], ra_r.at[p], me + (aa - a) * sa)

            @pl.when(aa == a)
            def _():
                abuf[p][a] = pbuf[p][i]

    for t in range(n + 2):
        if t < n:
            far(t)
        if 0 <= t - 1 < n:
            near(t - 1)
        if t >= 2:
            here(t - 2)
    for p, (off, w) in enumerate(parts):
        drain(pbuf[p].at[pl.ds(0, n - 1)], ra_r.at[p])
        total = abuf[p][0]
        for i in range(1, n):
            total += abuf[p][i]
        y_ref[:, off:off + w] = total.astype(BF16)
    for p in range(np_):
        drain(tbuf[p].at[0, pl.ds(0, n - 1)], ta_s.at[p])
        drain(tbuf[p].at[pl.ds(0, n - 1)], tb_s.at[p])
        drain(xbuf[p].at[0, pl.ds(0, n - 1)], xa_s.at[p])
        drain(xbuf[p].at[pl.ds(0, n - 1)], xb_s.at[p])
        drain(sbuf[p].at[:, pl.ds(0, 2 * n - 1)], c_s.at[p])
        drain(cbuf[p].at[:, :, pl.ds(0, 2 * n - 1)], rc_s.at[p])
        drain(farp[p], rf_s.at[p])
        drain(nearp[p], rn_s.at[p])
        drain(pbuf[p].at[pl.ds(0, n - 1)], ra_s.at[p])


def build(mesh, n, parts, lefts):
    row_spec = P(('data', 'expert'), None)
    expert_spec = P('expert', None, None)
    vmem = pl.BlockSpec(memory_space=pltpu.VMEM)
    hbm = pl.BlockSpec(memory_space=pl.ANY)

    def device_step(tokens, w_router, routes, w_gate, w_up, w_down):
        tok, width = tokens.shape
        experts = w_router.shape[1]
        ff = w_gate.shape[2]
        dma = pltpu.SemaphoreType.DMA
        np_ = len(parts)
        cols = 2 * n * CAP
        return pl.pallas_call(
            functools.partial(moe_kernel, n, parts, lefts),
            out_shape=jax.ShapeDtypeStruct((tok, width), BF16),
            in_specs=[vmem, vmem, vmem, hbm, hbm, hbm], out_specs=vmem,
            scratch_shapes=[
                pltpu.VMEM((width, ff), BF16), pltpu.VMEM((width, ff), BF16), pltpu.VMEM((ff, width), BF16),
                pltpu.VMEM((n, n, n, 2, CAP, width), BF16), pltpu.VMEM((n, n, n, 2, CAP, width), BF16),
                pltpu.VMEM((2 * CAP, experts), F32),
                *[pltpu.VMEM((n, n, 2 * CAP, experts), F32) for _ in parts],
                *[pltpu.VMEM((n, n, tok, w), BF16) for _, w in parts],
                *[pltpu.VMEM((n, 2 * n, n, CAP, w), BF16) for _, w in parts],
                *[pltpu.VMEM((n, n, 2 * n, CAP, w), BF16) for _, w in parts],
                *[pltpu.VMEM((n, tok, w), F32) for _, w in parts],
                *[pltpu.VMEM((n, tok, w), F32) for _, w in parts],
                *[pltpu.VMEM((n, 2, tok, w), F32) for _, w in parts],
                *[pltpu.VMEM((n, 2, tok, w), F32) for _, w in parts],
                *[pltpu.VMEM((n, tok, w), F32) for _, w in parts],
                *[pltpu.VMEM((n, tok, w), F32) for _, w in parts],
                *[pltpu.VMEM((n, n, 3 * tok, cols), BF16) for _ in parts],
                dma((3,)), dma((np_,)), dma((np_,)), dma((np_,)), dma((np_,)),
                dma((np_,)), dma((np_, n - 1)), dma((np_,)), dma((np_, n - 1)), dma((np_,)), dma((np_, n)),
                dma((np_,)), dma((np_, n, n)), dma((np_,)), dma((np_, n)), dma((np_,)), dma((np_, n)), dma((np_,)), dma((np_,)),
            ],
            compiler_params=pltpu.CompilerParams(collective_id=0, has_side_effects=True, vmem_limit_bytes=60 * 1024 * 1024),
            name='moe',
        )(tokens, w_router, routes.T, w_gate, w_up, w_down)

    return jax.shard_map(device_step, mesh=mesh, in_specs=(row_spec, P(None, None), row_spec, expert_spec, expert_spec, expert_spec), out_specs=row_spec, check_vma=False)


def solution(mesh):
    return build(mesh, 4, ((0, 768), (768, 640), (1408, 640)), (384, 384, 256))
```

```python
import functools

import jax
import jax.numpy as jnp
from jax import lax
from jax.experimental import pallas as pl
from jax.experimental.pallas import tpu as pltpu
from jax.sharding import PartitionSpec as P

F32 = jnp.float32
BF16 = jnp.bfloat16
CAP = 8


def _iota(shape, dim):
    return lax.broadcasted_iota(jnp.int32, shape, dim)


def _places(r):
    return (2 - r) % 3, (1 - r) % 3, (-r) % 3


def routing_table(x, wr, routes_t):
    tok, experts = x.shape[0], wr.shape[1]
    top_k = routes_t.shape[0]
    logits = jnp.dot(x, wr, preferred_element_type=F32)
    eye = (_iota((top_k, top_k), 0) == _iota((top_k, top_k), 1)).astype(BF16)
    routes = lax.dot_general(routes_t.astype(F32).astype(BF16), eye, (((0,), (0,)), ((), ())), preferred_element_type=F32)
    lane = _iota((tok, experts), 1).astype(F32)
    hit = jnp.zeros((tok, experts), F32)
    for j in range(top_k):
        hit += (routes[:, j:j + 1] == lane).astype(F32)
    on = hit > 0.5
    top = jnp.max(jnp.where(on, logits, -jnp.inf), axis=1, keepdims=True)
    e = jnp.where(on, jnp.exp(jnp.where(on, logits, top) - top), 0.0)
    gate = e / jnp.sum(e, axis=1, keepdims=True)
    below = (_iota((tok, tok), 1) < _iota((tok, tok), 0)).astype(BF16)
    rank = jnp.dot(below, hit.astype(BF16), preferred_element_type=F32)
    rank = jnp.where(on, rank, -1.0)
    row = _iota((tok, experts), 0).astype(F32)
    toks, gates = [], []
    for r in range(CAP):
        at = rank == r
        toks.append(jnp.sum(jnp.where(at, row + 1.0, 0.0), axis=0, keepdims=True) - 1.0)
        gates.append(jnp.sum(jnp.where(at, gate, 0.0), axis=0, keepdims=True))
    return jnp.concatenate(toks + gates, axis=0)


def moe_kernel(n, parts, lefts, x_hbm, wr_hbm, rt_hbm, wg_hbm, wu_hbm, wd_hbm, y_ref, x_ref, wr_ref, rt_ref, wg, wu, wd, rbuf, obuf, tab_ref, *rest):
    np_ = len(parts)
    tbuf, xbuf, sbuf, cbuf, farp, fari, nearp, neari, pbuf, abuf, mixbuf = [rest[i * np_:(i + 1) * np_] for i in range(11)]
    (w_sem, ta_s, ta_r, tb_s, tb_r, xa_s, xa_r, xb_s, xb_r, xd_s, xd_r, c_s, c_r, rc_s, rc_r, rf_s, rf_r, rn_s, rn_r, ra_s, ra_r) = rest[11 * np_:]
    tok, width = x_ref.shape
    experts = tab_ref.shape[1]
    me = lax.axis_index('expert')
    strides = (2 * n * n, 2 * n, 2)
    pos = tuple(lax.rem(me // s, n) for s in strides)
    core = lax.rem(me, 2)
    mod = lambda v: lax.rem(v, n)

    def order(p, cc):
        r0, r1 = _places(p % 3), _places((p + 1) % 3)
        return [(pos[i] + cc * (pos[j] - pos[i]), strides[i] + cc * (strides[j] - strides[i])) for i, j in zip(r0, r1)]

    mine = [order(p, core) for p in range(np_)]
    theirs = [order(p, 1 - core) for p in range(np_)]

    def moved(axis, d, flip=0):
        where, stride = axis
        other = me + (mod(where + d) - where) * stride
        return other + (1 - 2 * core) if flip else other

    def put(src, dst, send, recv, device):
        pltpu.make_async_remote_copy(src_ref=src, dst_ref=dst, send_sem=send, recv_sem=recv,
                                     device_id={'expert': device}, device_id_type=pl.DeviceIdType.MESH).start()

    def drain(ref, sem):
        pltpu.make_async_copy(ref, ref, sem).wait()

    def canon(p, cc, a, b, k):
        r0, r1 = _places(p % 3), _places((p + 1) % 3)
        v = (a, b, k)
        return [v[r0.index(j)] + cc * (v[r1.index(j)] - v[r0.index(j)]) for j in (0, 1)]

    loads = [pltpu.make_async_copy(src, dst, w_sem.at[i]) for i, (src, dst) in enumerate(((x_hbm, x_ref), (wr_hbm, wr_ref), (rt_hbm, rt_ref), (wg_hbm.at[0], wg), (wu_hbm.at[0], wu), (wd_hbm.at[0], wd)))]
    for load in loads:
        load.start()

    barrier = pltpu.get_barrier_semaphore()
    peers = [moved((pos[j], strides[j]), d, flip) for j in range(3) for d in range(1, n) for flip in (0, 1)] + [me + 1 - 2 * core]
    for peer in peers:
        pl.semaphore_signal(barrier, inc=1, device_id={'expert': peer}, device_id_type=pl.DeviceIdType.MESH)
    for load in loads[:3]:
        load.wait()
    pl.semaphore_wait(barrier, len(peers))

    near_first, far_first = (1, 3, 2), (2, 1, 3)

    for d in far_first:
        for p, (off, w) in enumerate(parts):
            (a, _), (b, _), _ = mine[p]
            put(x_ref.at[:, pl.ds(off, w)], xbuf[p].at[b, a], xa_s.at[p], xa_r.at[p, d - 1], moved(mine[p][0], d))
    for side in (0, 1):
        for p, (off, w) in enumerate(parts):
            (a, _), (b, _), _ = mine[p]
            put(x_ref.at[:, pl.ds(off, w)], xbuf[p].at[b, a], xb_s.at[p], xb_r.at[p, side, 0], moved(mine[p][1], 1 + 2 * side))
    tab_ref[...] = routing_table(x_ref[...], wr_ref[...], rt_ref[...])
    for p, (off, w) in enumerate(parts):
        (a, _), (b, _), _ = mine[p]
        xbuf[p][b, a] = x_ref[:, off:off + w]
        tbuf[p][b, a] = tab_ref[...]
    for d in far_first:
        for p in range(np_):
            (a, _), (b, _), _ = mine[p]
            put(tab_ref, tbuf[p].at[b, a], ta_s.at[p], ta_r.at[p], moved(mine[p][0], d))

    def along_b(da):
        for p in range(np_):
            (a, _), (b, _), _ = mine[p]
            src = mod(a + n - da)
            drain(xbuf[p].at[0, 0], xa_r.at[p, da - 1])
            for side in (0, 1):
                put(xbuf[p].at[b, src], xbuf[p].at[b, src], xb_s.at[p], xb_r.at[p, side, da], moved(mine[p][1], 1 + 2 * side))

    def onward(da):
        for side in (0, 1):
            for p, (off, w) in enumerate(parts):
                (a, _), (b, _), _ = mine[p]
                src, bb = mod(a + n - da), mod(b + n - 1 - 2 * side)
                drain(xbuf[p].at[0, 0], xb_r.at[p, side, da])
                half = pl.ds(lefts[p], w - lefts[p]) if side else pl.ds(0, lefts[p])
                put(xbuf[p].at[bb, src, :, half], xbuf[p].at[bb, src, :, half], xd_s.at[p], xd_r.at[p], moved(mine[p][1], 1 + 2 * side))

    along_b(1)
    along_b(3)
    onward(0)
    along_b(2)
    for p in range(np_):
        b = mine[p][1][0]
        drain(tbuf[p].at[0, pl.ds(0, n - 1)], ta_r.at[p])
        for d in far_first:
            put(tbuf[p].at[b], tbuf[p].at[b], tb_s.at[p], tb_r.at[p], moved(mine[p][1], d))

    q_order = (4, 5, 2, 3, 6, 7, 1)

    def select(p, db):
        off, w = parts[p]
        (a, _), (b, _), (k, _) = mine[p]
        bb = mod(b + n - db)
        table = tbuf[p][bb][:, :CAP].reshape(n * CAP, experts)
        shift = (_iota((n * CAP, 1), 0) // CAP * tok).astype(F32)
        lane = _iota((n * CAP, experts), 1)
        token = _iota((n * CAP, n * tok), 1).astype(F32)
        picks = []
        for q in range(2 * n):
            col = jnp.sum(jnp.where(lane == moved(mine[p][2], q // 2, q % 2), table, 0.0), axis=1, keepdims=True)
            want = jnp.where(col >= 0.0, col + shift, -1.0)
            picks.append((want == token).astype(F32))
        pick = jnp.concatenate(picks, axis=0).astype(BF16)
        rows = jnp.dot(pick, xbuf[p][bb].reshape(n * tok, w), preferred_element_type=F32).astype(BF16)
        sbuf[p][db] = rows.reshape(2 * n, n, CAP, w)

    def send_rows(p, db, i):
        off, w = parts[p]
        (a, _), (b, _), (k, _) = mine[p]
        bb = mod(b + n - db)
        aa = mod(i + 2 * n - bb - k)
        z, y = canon(p, core, aa, bb, k)
        for q in q_order:
            put(sbuf[p].at[db, q, aa], rbuf.at[i, z, y, core, :, pl.ds(off, w)], c_s.at[p], c_r.at[p, i], moved(mine[p][2], q // 2, q % 2))
        rbuf[i, z, y, core, :, off:off + w] = sbuf[p][db, 0, aa]

    def chunk_rows(i, dbs):
        for db in dbs:
            for p in range(np_):
                send_rows(p, db, i)

    def body(dbs):
        def run(i, carry):
            chunk_rows(i, dbs)
            return carry
        return run

    for p in range(np_):
        select(p, 0)
    lax.fori_loop(0, n, body((0,)), 0)
    for da in near_first:
        onward(da)
    for p in range(np_):
        drain(tbuf[p].at[pl.ds(0, n - 1)], tb_r.at[p])
    for db in (1, 3):
        for p in range(np_):
            select(p, db)
        chunk_rows(0, (db,))
    chunk_rows(1, (1, 3))
    for p in range(np_):
        drain(xbuf[p].at[0], xd_r.at[p])
        select(p, 2)
    chunk_rows(0, (2,))
    chunk_rows(1, (2,))
    lax.fori_loop(2, n, body((1, 3, 2)), 0)

    cols = 2 * n * CAP
    for p in range(np_):
        (a, sa), (b, sb), (_, sc) = mine[p]
        slot = _iota((experts, cols), 1)
        ident = slot // (2 * CAP) * sc + lax.rem(slot // CAP, 2) + a * sa + b * sb
        spread = (ident == _iota((experts, cols), 0)).astype(BF16)
        keep = _iota((CAP, cols), 0) == lax.rem(_iota((CAP, cols), 1), CAP)
        for bb in range(n):
            tg = tbuf[p][bb]
            gate = tg[:, CAP:]
            g1 = gate.astype(BF16).astype(F32)
            g2 = (gate - g1).astype(BF16).astype(F32)
            g3 = gate - g1 - g2
            terms = jnp.concatenate([tg[:, :CAP], g1, g2, g3], axis=1).reshape(n * 4 * CAP, experts).astype(BF16)
            wide = jnp.dot(terms, spread, preferred_element_type=F32)
            for aa in range(n):
                line = [jnp.sum(jnp.where(keep, wide[(aa * 4 + i) * CAP:(aa * 4 + i + 1) * CAP], 0.0), axis=0, keepdims=True) for i in range(4)]
                here = line[0] == _iota((tok, cols), 0).astype(F32)
                mixbuf[p][bb, aa] = jnp.concatenate([jnp.where(here, line[i], 0.0) for i in (1, 2, 3)], axis=0).astype(BF16)

    for load in loads[3:]:
        load.wait()

    ring = (2, 1, 3, 0) if n == 4 else tuple(range(1, n)) + (0,)

    def expert(i, carry):
        for p in range(np_):
            drain(sbuf[p].at[:, pl.ds(0, 2 * n - 1), 0], c_r.at[p, i])
        rows = rbuf[i].reshape(n * n * 2 * CAP, width)
        g = jnp.dot(rows, wg[...], preferred_element_type=F32)
        u = jnp.dot(rows, wu[...], preferred_element_type=F32)
        h = (g * jax.nn.sigmoid(g) * u).astype(BF16)
        o = jnp.dot(h, wd[...], preferred_element_type=F32).astype(BF16)
        obuf[i] = o.reshape(n, n, 2, CAP, width)
        for db in ring:
            for q in q_order + (0,):
                for p, (off, w) in enumerate(parts):
                    cc, axes = (1 - core, theirs[p]) if q % 2 else (core, mine[p])
                    (_, _), (b, _), (k, _) = axes
                    kk, bb = mod(k + q // 2), mod(b + db)
                    aa = mod(i + 2 * n - bb - kk)
                    z, y = canon(p, cc, aa, bb, kk)
                    if q:
                        put(obuf.at[i, z, y, cc, :, pl.ds(off, w)], cbuf[p].at[bb, aa, k * 2 + core],
                            rc_s.at[p], rc_r.at[p, db, i], moved(axes[2], q // 2, q % 2))
                    else:
                        cbuf[p][bb, aa, k * 2 + core] = obuf[i, z, y, cc, :, off:off + w]
        return carry

    lax.fori_loop(0, n, expert, 0)

    def line_sum(p, db, i):
        w = parts[p][1]
        _, (b, _), (k, _) = mine[p]
        bb = mod(b + db)
        aa = mod(i + 2 * n - bb - k)
        drain(cbuf[p].at[0, 0, pl.ds(0, 2 * n - 1)], rc_r.at[p, db, i])
        part = jnp.dot(mixbuf[p][bb, aa], cbuf[p][bb, aa].reshape(cols, w), preferred_element_type=F32)
        return part[:tok] + part[tok:2 * tok] + part[2 * tok:]

    def far(i):
        for p in range(np_):
            w, left = parts[p][1], lefts[p]
            farp[p][i] = line_sum(p, 2, i)
            put(farp[p].at[i, :, pl.ds(0, left)], fari[p].at[i, :, pl.ds(0, left)], rf_s.at[p], rf_r.at[p, i], moved(mine[p][1], 1))
            put(farp[p].at[i, :, pl.ds(left, w - left)], fari[p].at[i, :, pl.ds(left, w - left)], rf_s.at[p], rf_r.at[p, i], moved(mine[p][1], n - 1))

    def near(i):
        for p in range(np_):
            left = lefts[p]
            up, down = line_sum(p, 1, i), line_sum(p, n - 1, i)
            drain(fari[p].at[i], rf_r.at[p, i])
            nearp[p][i, 0, :, :left] = up[:, :left] + fari[p][i, :, :left]
            nearp[p][i, 0, :, left:] = up[:, left:]
            put(nearp[p].at[i, 0], neari[p].at[i, 0], rn_s.at[p], rn_r.at[p, i], moved(mine[p][1], 1))
            nearp[p][i, 1, :, :left] = down[:, :left]
            nearp[p][i, 1, :, left:] = down[:, left:] + fari[p][i, :, left:]
            put(nearp[p].at[i, 1], neari[p].at[i, 1], rn_s.at[p], rn_r.at[p, i], moved(mine[p][1], n - 1))

    def here(i):
        for p in range(np_):
            (a, sa), (b, _), (k, _) = mine[p]
            aa = mod(i + 2 * n - b - k)
            own = line_sum(p, 0, i)
            drain(neari[p].at[i], rn_r.at[p, i])
            pbuf[p][i] = own + neari[p][i, 0] + neari[p][i, 1]

            @pl.when(aa != a)
            def _():
                put(pbuf[p].at[i], abuf[p].at[a], ra_s.at[p], ra_r.at[p], me + (aa - a) * sa)

            @pl.when(aa == a)
            def _():
                abuf[p][a] = pbuf[p][i]

    for t in range(n + 2):
        if t < n:
            far(t)
        if 0 <= t - 1 < n:
            near(t - 1)
        if t >= 2:
            here(t - 2)
    for p, (off, w) in enumerate(parts):
        drain(pbuf[p].at[pl.ds(0, n - 1)], ra_r.at[p])
        total = abuf[p][0]
        for i in range(1, n):
            total += abuf[p][i]
        y_ref[:, off:off + w] = total.astype(BF16)
    for p in range(np_):
        drain(tbuf[p].at[0, pl.ds(0, n - 1)], ta_s.at[p])
        drain(tbuf[p].at[pl.ds(0, n - 1)], tb_s.at[p])
        drain(xbuf[p].at[0, pl.ds(0, n - 1)], xa_s.at[p])
        drain(xbuf[p].at[pl.ds(0, 2)], xb_s.at[p])
        drain(xbuf[p].at[0], xd_s.at[p])
        drain(sbuf[p].at[:, pl.ds(0, 2 * n - 1)], c_s.at[p])
        drain(cbuf[p].at[:, :, pl.ds(0, 2 * n - 1)], rc_s.at[p])
        drain(farp[p], rf_s.at[p])
        drain(nearp[p], rn_s.at[p])
        drain(pbuf[p].at[pl.ds(0, n - 1)], ra_s.at[p])


def build(mesh, n, parts, lefts):
    row_spec = P(('data', 'expert'), None)
    expert_spec = P('expert', None, None)
    vmem = pl.BlockSpec(memory_space=pltpu.VMEM)
    hbm = pl.BlockSpec(memory_space=pl.ANY)

    def device_step(tokens, w_router, routes, w_gate, w_up, w_down):
        tok, width = tokens.shape
        experts = w_router.shape[1]
        ff = w_gate.shape[2]
        dma = pltpu.SemaphoreType.DMA
        np_ = len(parts)
        cols = 2 * n * CAP
        return pl.pallas_call(
            functools.partial(moe_kernel, n, parts, lefts),
            out_shape=jax.ShapeDtypeStruct((tok, width), BF16),
            in_specs=[hbm] * 6, out_specs=vmem,
            scratch_shapes=[
                pltpu.VMEM((tok, width), BF16), pltpu.VMEM((width, experts), BF16), pltpu.VMEM((routes.shape[1], tok), jnp.int32),
                pltpu.VMEM((width, ff), BF16), pltpu.VMEM((width, ff), BF16), pltpu.VMEM((ff, width), BF16),
                pltpu.VMEM((n, n, n, 2, CAP, width), BF16), pltpu.VMEM((n, n, n, 2, CAP, width), BF16),
                pltpu.VMEM((2 * CAP, experts), F32),
                *[pltpu.VMEM((n, n, 2 * CAP, experts), F32) for _ in parts],
                *[pltpu.VMEM((n, n, tok, w), BF16) for _, w in parts],
                *[pltpu.VMEM((n, 2 * n, n, CAP, w), BF16) for _, w in parts],
                *[pltpu.VMEM((n, n, 2 * n, CAP, w), BF16) for _, w in parts],
                *[pltpu.VMEM((n, tok, w), F32) for _, w in parts],
                *[pltpu.VMEM((n, tok, w), F32) for _, w in parts],
                *[pltpu.VMEM((n, 2, tok, w), F32) for _, w in parts],
                *[pltpu.VMEM((n, 2, tok, w), F32) for _, w in parts],
                *[pltpu.VMEM((n, tok, w), F32) for _, w in parts],
                *[pltpu.VMEM((n, tok, w), F32) for _, w in parts],
                *[pltpu.VMEM((n, n, 3 * tok, cols), BF16) for _ in parts],
                dma((6,)), dma((np_,)), dma((np_,)), dma((np_,)), dma((np_,)),
                dma((np_,)), dma((np_, n - 1)), dma((np_,)), dma((np_, 2, n)), dma((np_,)), dma((np_,)), dma((np_,)), dma((np_, n)),
                dma((np_,)), dma((np_, n, n)), dma((np_,)), dma((np_, n)), dma((np_,)), dma((np_, n)), dma((np_,)), dma((np_,)),
            ],
            compiler_params=pltpu.CompilerParams(collective_id=0, has_side_effects=True, vmem_limit_bytes=60 * 1024 * 1024),
            name='moe',
        )(tokens, w_router, routes.T, w_gate, w_up, w_down)

    return jax.shard_map(device_step, mesh=mesh, in_specs=(row_spec, P(None, None), row_spec, expert_spec, expert_spec, expert_spec), out_specs=row_spec, check_vma=False)


def solution(mesh):
    return build(mesh, 4, ((0, 768), (768, 640), (1408, 640)), (384, 384, 256))
```

```python
import functools

import jax
import jax.numpy as jnp
from jax import lax
from jax.experimental import pallas as pl
from jax.experimental.pallas import tpu as pltpu
from jax.sharding import PartitionSpec as P

F32 = jnp.float32
BF16 = jnp.bfloat16
CAP = 8


def _iota(shape, dim):
    return lax.broadcasted_iota(jnp.int32, shape, dim)


def _places(r):
    return (2 - r) % 3, (1 - r) % 3, (-r) % 3


def routing_table(x, wr, routes_t):
    tok, experts = x.shape[0], wr.shape[1]
    top_k = routes_t.shape[0]
    logits = jnp.dot(x, wr, preferred_element_type=F32)
    eye = (_iota((top_k, top_k), 0) == _iota((top_k, top_k), 1)).astype(BF16)
    routes = lax.dot_general(routes_t.astype(F32).astype(BF16), eye, (((0,), (0,)), ((), ())), preferred_element_type=F32)
    lane = _iota((tok, experts), 1).astype(F32)
    hit = jnp.zeros((tok, experts), F32)
    for j in range(top_k):
        hit += (routes[:, j:j + 1] == lane).astype(F32)
    on = hit > 0.5
    top = jnp.max(jnp.where(on, logits, -jnp.inf), axis=1, keepdims=True)
    e = jnp.where(on, jnp.exp(jnp.where(on, logits, top) - top), 0.0)
    gate = e / jnp.sum(e, axis=1, keepdims=True)
    below = (_iota((tok, tok), 1) < _iota((tok, tok), 0)).astype(BF16)
    rank = jnp.dot(below, hit.astype(BF16), preferred_element_type=F32)
    rank = jnp.where(on, rank, -1.0)
    row = _iota((tok, experts), 0).astype(F32)
    toks, gates = [], []
    for r in range(CAP):
        at = rank == r
        toks.append(jnp.sum(jnp.where(at, row + 1.0, 0.0), axis=0, keepdims=True) - 1.0)
        gates.append(jnp.sum(jnp.where(at, gate, 0.0), axis=0, keepdims=True))
    return jnp.concatenate(toks + gates, axis=0)


def moe_kernel(n, parts, lefts, x_hbm, wr_hbm, rt_hbm, wg_hbm, wu_hbm, wd_hbm, y_ref, x_ref, wr_ref, rt_ref, wg, wu, wd, rbuf, obuf, tab_ref, *rest):
    np_ = len(parts)
    tbuf, xbuf, sbuf, cbuf, farp, fari, nearp, neari, pbuf, abuf, mixbuf = [rest[i * np_:(i + 1) * np_] for i in range(11)]
    (w_sem, ta_s, ta_r, tb_s, tb_r, xa_s, xa_r, xb_s, xb_r, c_s, c_r, rc_s, rc_r, rf_s, rf_r, rn_s, rn_r, ra_s, ra_r) = rest[11 * np_:]
    tok, width = x_ref.shape
    experts = tab_ref.shape[1]
    me = lax.axis_index('expert')
    strides = (2 * n * n, 2 * n, 2)
    pos = tuple(lax.rem(me // s, n) for s in strides)
    core = lax.rem(me, 2)
    mod = lambda v: lax.rem(v, n)

    def order(p, cc):
        r0, r1 = _places(p % 3), _places((p + 1) % 3)
        return [(pos[i] + cc * (pos[j] - pos[i]), strides[i] + cc * (strides[j] - strides[i])) for i, j in zip(r0, r1)]

    mine = [order(p, core) for p in range(np_)]
    theirs = [order(p, 1 - core) for p in range(np_)]

    def moved(axis, d, flip=0):
        where, stride = axis
        other = me + (mod(where + d) - where) * stride
        return other + (1 - 2 * core) if flip else other

    def put(src, dst, send, recv, device):
        pltpu.make_async_remote_copy(src_ref=src, dst_ref=dst, send_sem=send, recv_sem=recv,
                                     device_id={'expert': device}, device_id_type=pl.DeviceIdType.MESH).start()

    def drain(ref, sem):
        pltpu.make_async_copy(ref, ref, sem).wait()

    def canon(p, cc, a, b, k):
        r0, r1 = _places(p % 3), _places((p + 1) % 3)
        v = (a, b, k)
        return [v[r0.index(j)] + cc * (v[r1.index(j)] - v[r0.index(j)]) for j in (0, 1)]

    loads = [pltpu.make_async_copy(src, dst, w_sem.at[i]) for i, (src, dst) in enumerate(((x_hbm, x_ref), (wr_hbm, wr_ref), (rt_hbm, rt_ref), (wg_hbm.at[0], wg), (wu_hbm.at[0], wu), (wd_hbm.at[0], wd)))]
    for load in loads:
        load.start()

    barrier = pltpu.get_barrier_semaphore()
    peers = [moved((pos[j], strides[j]), d, flip) for j in range(3) for d in range(1, n) for flip in (0, 1)] + [me + 1 - 2 * core]
    for peer in peers:
        pl.semaphore_signal(barrier, inc=1, device_id={'expert': peer}, device_id_type=pl.DeviceIdType.MESH)
    for load in loads[:3]:
        load.wait()
    pl.semaphore_wait(barrier, len(peers))

    near_first, far_first = (1, 3, 2), (2, 1, 3)

    for axis, send, recv in ((0, xa_s, xa_r), (1, xb_s, xb_r)):
        for d in far_first:
            for p, (off, w) in enumerate(parts):
                (a, _), (b, _), _ = mine[p]
                put(x_ref.at[:, pl.ds(off, w)], xbuf[p].at[b, a], send.at[p], recv.at[p, d - 1], moved(mine[p][axis], d))
    tab_ref[...] = routing_table(x_ref[...], wr_ref[...], rt_ref[...])
    for p, (off, w) in enumerate(parts):
        (a, _), (b, _), _ = mine[p]
        xbuf[p][b, a] = x_ref[:, off:off + w]
        tbuf[p][b, a] = tab_ref[...]
    for d in far_first:
        for p in range(np_):
            (a, _), (b, _), _ = mine[p]
            put(tab_ref, tbuf[p].at[b, a], ta_s.at[p], ta_r.at[p], moved(mine[p][0], d))
    for da in near_first:
        for p in range(np_):
            (a, _), (b, _), _ = mine[p]
            src = mod(a + n - da)
            drain(xbuf[p].at[0, 0], xa_r.at[p, da - 1])
            for d in far_first:
                put(xbuf[p].at[b, src], xbuf[p].at[b, src], xb_s.at[p], xb_r.at[p, d - 1], moved(mine[p][1], d))
    for p in range(np_):
        b = mine[p][1][0]
        drain(tbuf[p].at[0, pl.ds(0, n - 1)], ta_r.at[p])
        for d in far_first:
            put(tbuf[p].at[b], tbuf[p].at[b], tb_s.at[p], tb_r.at[p], moved(mine[p][1], d))

    q_order = (4, 5, 2, 3, 6, 7, 1)

    def select(p, db):
        off, w = parts[p]
        (a, _), (b, _), (k, _) = mine[p]
        bb = mod(b + n - db)
        table = tbuf[p][bb][:, :CAP].reshape(n * CAP, experts)
        shift = (_iota((n * CAP, 1), 0) // CAP * tok).astype(F32)
        lane = _iota((n * CAP, experts), 1)
        token = _iota((n * CAP, n * tok), 1).astype(F32)
        picks = []
        for q in range(2 * n):
            col = jnp.sum(jnp.where(lane == moved(mine[p][2], q // 2, q % 2), table, 0.0), axis=1, keepdims=True)
            want = jnp.where(col >= 0.0, col + shift, -1.0)
            picks.append((want == token).astype(F32))
        pick = jnp.concatenate(picks, axis=0).astype(BF16)
        rows = jnp.dot(pick, xbuf[p][bb].reshape(n * tok, w), preferred_element_type=F32).astype(BF16)
        sbuf[p][db] = rows.reshape(2 * n, n, CAP, w)

    def send_rows(p, db, i):
        off, w = parts[p]
        (a, _), (b, _), (k, _) = mine[p]
        bb = mod(b + n - db)
        aa = mod(i + 2 * n - bb - k)
        z, y = canon(p, core, aa, bb, k)
        for q in q_order:
            put(sbuf[p].at[db, q, aa], rbuf.at[i, z, y, core, :, pl.ds(off, w)], c_s.at[p], c_r.at[p, i], moved(mine[p][2], q // 2, q % 2))
        rbuf[i, z, y, core, :, off:off + w] = sbuf[p][db, 0, aa]

    def chunk_rows(i, dbs):
        for db in dbs:
            for p in range(np_):
                send_rows(p, db, i)

    def body(dbs):
        def run(i, carry):
            chunk_rows(i, dbs)
            return carry
        return run

    for p in range(np_):
        select(p, 0)
    lax.fori_loop(0, n, body((0,)), 0)
    for p in range(np_):
        drain(tbuf[p].at[pl.ds(0, n - 1)], tb_r.at[p])
    for db in near_first:
        for p in range(np_):
            drain(xbuf[p].at[0], xb_r.at[p, db - 1])
            select(p, db)
        chunk_rows(0, (db,))
    lax.fori_loop(1, n, body(near_first), 0)

    cols = 2 * n * CAP
    for p in range(np_):
        (a, sa), (b, sb), (_, sc) = mine[p]
        slot = _iota((experts, cols), 1)
        ident = slot // (2 * CAP) * sc + lax.rem(slot // CAP, 2) + a * sa + b * sb
        spread = (ident == _iota((experts, cols), 0)).astype(BF16)
        keep = _iota((CAP, cols), 0) == lax.rem(_iota((CAP, cols), 1), CAP)
        for bb in range(n):
            tg = tbuf[p][bb]
            gate = tg[:, CAP:]
            g1 = gate.astype(BF16).astype(F32)
            g2 = (gate - g1).astype(BF16).astype(F32)
            g3 = gate - g1 - g2
            terms = jnp.concatenate([tg[:, :CAP], g1, g2, g3], axis=1).reshape(n * 4 * CAP, experts).astype(BF16)
            wide = jnp.dot(terms, spread, preferred_element_type=F32)
            for aa in range(n):
                line = [jnp.sum(jnp.where(keep, wide[(aa * 4 + i) * CAP:(aa * 4 + i + 1) * CAP], 0.0), axis=0, keepdims=True) for i in range(4)]
                here = line[0] == _iota((tok, cols), 0).astype(F32)
                mixbuf[p][bb, aa] = jnp.concatenate([jnp.where(here, line[i], 0.0) for i in (1, 2, 3)], axis=0).astype(BF16)

    for load in loads[3:]:
        load.wait()

    ring = (2, 1, 3, 0) if n == 4 else tuple(range(1, n)) + (0,)

    def expert(i, carry):
        for p in range(np_):
            drain(sbuf[p].at[:, pl.ds(0, 2 * n - 1), 0], c_r.at[p, i])
        rows = rbuf[i].reshape(n * n * 2 * CAP, width)
        g = jnp.dot(rows, wg[...], preferred_element_type=F32)
        u = jnp.dot(rows, wu[...], preferred_element_type=F32)
        h = (g * jax.nn.sigmoid(g) * u).astype(BF16)
        o = jnp.dot(h, wd[...], preferred_element_type=F32).astype(BF16)
        obuf[i] = o.reshape(n, n, 2, CAP, width)
        for db in ring:
            for q in q_order + (0,):
                for p, (off, w) in enumerate(parts):
                    cc, axes = (1 - core, theirs[p]) if q % 2 else (core, mine[p])
                    (_, _), (b, _), (k, _) = axes
                    kk, bb = mod(k + q // 2), mod(b + db)
                    aa = mod(i + 2 * n - bb - kk)
                    z, y = canon(p, cc, aa, bb, kk)
                    if q:
                        put(obuf.at[i, z, y, cc, :, pl.ds(off, w)], cbuf[p].at[bb, aa, k * 2 + core],
                            rc_s.at[p], rc_r.at[p, db, i], moved(axes[2], q // 2, q % 2))
                    else:
                        cbuf[p][bb, aa, k * 2 + core] = obuf[i, z, y, cc, :, off:off + w]
        return carry

    lax.fori_loop(0, n, expert, 0)

    def line_sum(p, db, i):
        w = parts[p][1]
        _, (b, _), (k, _) = mine[p]
        bb = mod(b + db)
        aa = mod(i + 2 * n - bb - k)
        drain(cbuf[p].at[0, 0, pl.ds(0, 2 * n - 1)], rc_r.at[p, db, i])
        part = jnp.dot(mixbuf[p][bb, aa], cbuf[p][bb, aa].reshape(cols, w), preferred_element_type=F32)
        return part[:tok] + part[tok:2 * tok] + part[2 * tok:]

    def far(i):
        for p in range(np_):
            w, left = parts[p][1], lefts[i % 2][p]
            farp[p][i] = line_sum(p, 2, i)
            put(farp[p].at[i, :, pl.ds(0, left)], fari[p].at[i, :, pl.ds(0, left)], rf_s.at[p], rf_r.at[p, i], moved(mine[p][1], 1))
            put(farp[p].at[i, :, pl.ds(left, w - left)], fari[p].at[i, :, pl.ds(left, w - left)], rf_s.at[p], rf_r.at[p, i], moved(mine[p][1], n - 1))

    def near(i):
        for p in range(np_):
            left = lefts[i % 2][p]
            up, down = line_sum(p, 1, i), line_sum(p, n - 1, i)
            drain(fari[p].at[i], rf_r.at[p, i])
            nearp[p][i, 0, :, :left] = up[:, :left] + fari[p][i, :, :left]
            nearp[p][i, 0, :, left:] = up[:, left:]
            put(nearp[p].at[i, 0], neari[p].at[i, 0], rn_s.at[p], rn_r.at[p, i], moved(mine[p][1], 1))
            nearp[p][i, 1, :, :left] = down[:, :left]
            nearp[p][i, 1, :, left:] = down[:, left:] + fari[p][i, :, left:]
            put(nearp[p].at[i, 1], neari[p].at[i, 1], rn_s.at[p], rn_r.at[p, i], moved(mine[p][1], n - 1))

    def here(i):
        for p in range(np_):
            (a, sa), (b, _), (k, _) = mine[p]
            aa = mod(i + 2 * n - b - k)
            own = line_sum(p, 0, i)
            drain(neari[p].at[i], rn_r.at[p, i])
            pbuf[p][i] = own + neari[p][i, 0] + neari[p][i, 1]

            @pl.when(aa != a)
            def _():
                put(pbuf[p].at[i], abuf[p].at[a], ra_s.at[p], ra_r.at[p], me + (aa - a) * sa)

            @pl.when(aa == a)
            def _():
                abuf[p][a] = pbuf[p][i]

    for t in range(n + 2):
        if t < n:
            far(t)
        if 0 <= t - 1 < n:
            near(t - 1)
        if t >= 2:
            here(t - 2)
    for p, (off, w) in enumerate(parts):
        drain(pbuf[p].at[pl.ds(0, n - 1)], ra_r.at[p])
        total = abuf[p][0]
        for i in range(1, n):
            total += abuf[p][i]
        y_ref[:, off:off + w] = total.astype(BF16)
    for p in range(np_):
        drain(tbuf[p].at[0, pl.ds(0, n - 1)], ta_s.at[p])
        drain(tbuf[p].at[pl.ds(0, n - 1)], tb_s.at[p])
        drain(xbuf[p].at[0, pl.ds(0, n - 1)], xa_s.at[p])
        drain(xbuf[p].at[pl.ds(0, n - 1)], xb_s.at[p])
        drain(sbuf[p].at[:, pl.ds(0, 2 * n - 1)], c_s.at[p])
        drain(cbuf[p].at[:, :, pl.ds(0, 2 * n - 1)], rc_s.at[p])
        drain(farp[p], rf_s.at[p])
        drain(nearp[p], rn_s.at[p])
        drain(pbuf[p].at[pl.ds(0, n - 1)], ra_s.at[p])


def build(mesh, n, parts, lefts):
    row_spec = P(('data', 'expert'), None)
    expert_spec = P('expert', None, None)
    vmem = pl.BlockSpec(memory_space=pltpu.VMEM)
    hbm = pl.BlockSpec(memory_space=pltpu.HBM)

    def device_step(tokens, w_router, routes, w_gate, w_up, w_down):
        tok, width = tokens.shape
        experts = w_router.shape[1]
        ff = w_gate.shape[2]
        dma = pltpu.SemaphoreType.DMA
        np_ = len(parts)
        cols = 2 * n * CAP
        return pl.pallas_call(
            functools.partial(moe_kernel, n, parts, lefts),
            out_shape=pltpu.VMEM((tok, width), BF16),
            in_specs=[hbm] * 6, out_specs=vmem,
            scratch_shapes=[
                pltpu.VMEM((tok, width), BF16), pltpu.VMEM((width, experts), BF16), pltpu.VMEM((routes.shape[1], tok), jnp.int32),
                pltpu.VMEM((width, ff), BF16), pltpu.VMEM((width, ff), BF16), pltpu.VMEM((ff, width), BF16),
                pltpu.VMEM((n, n, n, 2, CAP, width), BF16), pltpu.VMEM((n, n, n, 2, CAP, width), BF16),
                pltpu.VMEM((2 * CAP, experts), F32),
                *[pltpu.VMEM((n, n, 2 * CAP, experts), F32) for _ in parts],
                *[pltpu.VMEM((n, n, tok, w), BF16) for _, w in parts],
                *[pltpu.VMEM((n, 2 * n, n, CAP, w), BF16) for _, w in parts],
                *[pltpu.VMEM((n, n, 2 * n, CAP, w), BF16) for _, w in parts],
                *[pltpu.VMEM((n, tok, w), F32) for _, w in parts],
                *[pltpu.VMEM((n, tok, w), F32) for _, w in parts],
                *[pltpu.VMEM((n, 2, tok, w), F32) for _, w in parts],
                *[pltpu.VMEM((n, 2, tok, w), F32) for _, w in parts],
                *[pltpu.VMEM((n, tok, w), F32) for _, w in parts],
                *[pltpu.VMEM((n, tok, w), F32) for _, w in parts],
                *[pltpu.VMEM((n, n, 3 * tok, cols), BF16) for _ in parts],
                dma((6,)), dma((np_,)), dma((np_,)), dma((np_,)), dma((np_,)),
                dma((np_,)), dma((np_, n - 1)), dma((np_,)), dma((np_, n - 1)), dma((np_,)), dma((np_, n)),
                dma((np_,)), dma((np_, n, n)), dma((np_,)), dma((np_, n)), dma((np_,)), dma((np_, n)), dma((np_,)), dma((np_,)),
            ],
            compiler_params=pltpu.CompilerParams(collective_id=0, has_side_effects=True, vmem_limit_bytes=57 * 1024 * 1024),
            name='moe',
        )(tokens, w_router, routes.T, w_gate, w_up, w_down)

    return jax.shard_map(device_step, mesh=mesh, in_specs=(row_spec, P(None, None), row_spec, expert_spec, expert_spec, expert_spec), out_specs=row_spec, check_vma=False)


def solution(mesh):
    return build(mesh, 4, ((0, 768), (768, 640), (1408, 640)), ((384, 384, 256), (384, 256, 384)))
```

```python
import functools

import jax
import jax.numpy as jnp
from jax import lax
from jax.experimental import pallas as pl
from jax.experimental.pallas import tpu as pltpu
from jax.sharding import PartitionSpec as P

F32 = jnp.float32
BF16 = jnp.bfloat16
CAP = 8
PLAN = 'y f0 x3 f1 f2 n0 f3 n1 n2 n3 h0 h1 h2 h3'


def _iota(shape, dim):
    return lax.broadcasted_iota(jnp.int32, shape, dim)


def _places(r):
    return (2 - r) % 3, (1 - r) % 3, (-r) % 3


def routing_table(x, wr, routes_t):
    tok, experts = x.shape[0], wr.shape[1]
    top_k = routes_t.shape[0]
    logits = jnp.dot(x, wr, preferred_element_type=F32)
    eye = (_iota((top_k, top_k), 0) == _iota((top_k, top_k), 1)).astype(BF16)
    routes = lax.dot_general(routes_t.astype(F32).astype(BF16), eye, (((0,), (0,)), ((), ())), preferred_element_type=F32)
    lane = _iota((tok, experts), 1).astype(F32)
    hit = jnp.zeros((tok, experts), F32)
    for j in range(top_k):
        hit += (routes[:, j:j + 1] == lane).astype(F32)
    on = hit > 0.5
    top = jnp.max(jnp.where(on, logits, -jnp.inf), axis=1, keepdims=True)
    e = jnp.where(on, jnp.exp(jnp.where(on, logits, top) - top), 0.0)
    gate = e / jnp.sum(e, axis=1, keepdims=True)
    below = (_iota((tok, tok), 1) < _iota((tok, tok), 0)).astype(BF16)
    rank = jnp.dot(below, hit.astype(BF16), preferred_element_type=F32)
    rank = jnp.where(on, rank, -1.0)
    row = _iota((tok, experts), 0).astype(F32)
    toks, gates = [], []
    for r in range(CAP):
        at = rank == r
        toks.append(jnp.sum(jnp.where(at, row + 1.0, 0.0), axis=0, keepdims=True) - 1.0)
        gates.append(jnp.sum(jnp.where(at, gate, 0.0), axis=0, keepdims=True))
    return jnp.concatenate(toks + gates, axis=0)


def moe_kernel(n, parts, lefts, x_hbm, wr_hbm, rt_hbm, wg_hbm, wu_hbm, wd_hbm, y_ref, x_ref, wr_ref, rt_ref, wg, wu, wd, rbuf, obuf, tab_ref, *rest):
    np_ = len(parts)
    tbuf, xbuf, sbuf, cbuf, farp, fari, nearp, neari, pbuf, abuf, mixbuf = [rest[i * np_:(i + 1) * np_] for i in range(11)]
    (w_sem, ta_s, ta_r, tb_s, tb_r, xa_s, xa_r, xb_s, xb_r, c_s, c_r, rc_s, rc_r, rf_s, rf_r, rn_s, rn_r, ra_s, ra_r) = rest[11 * np_:]
    tok, width = x_ref.shape
    experts = tab_ref.shape[1]
    me = lax.axis_index('expert')
    strides = (2 * n * n, 2 * n, 2)
    pos = tuple(lax.rem(me // s, n) for s in strides)
    core = lax.rem(me, 2)
    mod = lambda v: lax.rem(v, n)

    def order(p, cc):
        r0, r1 = _places(p % 3), _places((p + 1) % 3)
        return [(pos[i] + cc * (pos[j] - pos[i]), strides[i] + cc * (strides[j] - strides[i])) for i, j in zip(r0, r1)]

    mine = [order(p, core) for p in range(np_)]
    theirs = [order(p, 1 - core) for p in range(np_)]

    def moved(axis, d, flip=0):
        where, stride = axis
        other = me + (mod(where + d) - where) * stride
        return other + (1 - 2 * core) if flip else other

    def put(src, dst, send, recv, device):
        pltpu.make_async_remote_copy(src_ref=src, dst_ref=dst, send_sem=send, recv_sem=recv,
                                     device_id={'expert': device}, device_id_type=pl.DeviceIdType.MESH).start()

    def drain(ref, sem):
        pltpu.make_async_copy(ref, ref, sem).wait()

    def canon(p, cc, a, b, k):
        r0, r1 = _places(p % 3), _places((p + 1) % 3)
        v = (a, b, k)
        return [v[r0.index(j)] + cc * (v[r1.index(j)] - v[r0.index(j)]) for j in (0, 1)]

    loads = [pltpu.make_async_copy(src, dst, w_sem.at[i]) for i, (src, dst) in enumerate(((x_hbm, x_ref), (wr_hbm, wr_ref), (rt_hbm, rt_ref), (wg_hbm.at[0], wg), (wu_hbm.at[0], wu), (wd_hbm.at[0], wd)))]
    for load in loads:
        load.start()

    barrier = pltpu.get_barrier_semaphore()
    peers = [moved((pos[j], strides[j]), d, flip) for j in range(3) for d in range(1, n) for flip in (0, 1)] + [me + 1 - 2 * core]
    for peer in peers:
        pl.semaphore_signal(barrier, inc=1, device_id={'expert': peer}, device_id_type=pl.DeviceIdType.MESH)
    for load in loads[:3]:
        load.wait()
    tab_ref[...] = routing_table(x_ref[...], wr_ref[...], rt_ref[...])
    for p, (off, w) in enumerate(parts):
        (a, _), (b, _), _ = mine[p]
        xbuf[p][b, a] = x_ref[:, off:off + w]
        tbuf[p][b, a] = tab_ref[...]
    pl.semaphore_wait(barrier, len(peers))

    near_first, far_first = (1, 3, 2), (2, 1, 3)

    for d in far_first:
        for p in range(np_):
            (a, _), (b, _), _ = mine[p]
            put(tab_ref, tbuf[p].at[b, a], ta_s.at[p], ta_r.at[p], moved(mine[p][0], d))
    for axis, send, recv in ((0, xa_s, xa_r), (1, xb_s, xb_r)):
        for d in far_first:
            for p, (off, w) in enumerate(parts):
                (a, _), (b, _), _ = mine[p]
                put(x_ref.at[:, pl.ds(off, w)], xbuf[p].at[b, a], send.at[p], recv.at[p, d - 1], moved(mine[p][axis], d))
    for p in range(np_):
        b = mine[p][1][0]
        drain(tbuf[p].at[0, pl.ds(0, n - 1)], ta_r.at[p])
        for d in far_first:
            put(tbuf[p].at[b], tbuf[p].at[b], tb_s.at[p], tb_r.at[p], moved(mine[p][1], d))
    for da in near_first:
        for p in range(np_):
            (a, _), (b, _), _ = mine[p]
            src = mod(a + n - da)
            drain(xbuf[p].at[0, 0], xa_r.at[p, da - 1])
            for d in far_first:
                put(xbuf[p].at[b, src], xbuf[p].at[b, src], xb_s.at[p], xb_r.at[p, d - 1], moved(mine[p][1], d))

    q_order = (4, 5, 2, 3, 6, 7, 1)

    def select(p, db):
        off, w = parts[p]
        (a, _), (b, _), (k, _) = mine[p]
        bb = mod(b + n - db)
        table = tbuf[p][bb][:, :CAP].reshape(n * CAP, experts)
        shift = (_iota((n * CAP, 1), 0) // CAP * tok).astype(F32)
        lane = _iota((n * CAP, experts), 1)
        token = _iota((n * CAP, n * tok), 1).astype(F32)
        picks = []
        for q in range(2 * n):
            col = jnp.sum(jnp.where(lane == moved(mine[p][2], q // 2, q % 2), table, 0.0), axis=1, keepdims=True)
            want = jnp.where(col >= 0.0, col + shift, -1.0)
            picks.append((want == token).astype(F32))
        pick = jnp.concatenate(picks, axis=0).astype(BF16)
        rows = jnp.dot(pick, xbuf[p][bb].reshape(n * tok, w), preferred_element_type=F32).astype(BF16)
        sbuf[p][db] = rows.reshape(2 * n, n, CAP, w)

    def send_rows(p, db, i):
        off, w = parts[p]
        (a, _), (b, _), (k, _) = mine[p]
        bb = mod(b + n - db)
        aa = mod(i + 2 * n - bb - k)
        z, y = canon(p, core, aa, bb, k)
        for q in q_order:
            put(sbuf[p].at[db, q, aa], rbuf.at[i, z, y, core, :, pl.ds(off, w)], c_s.at[p], c_r.at[p, i], moved(mine[p][2], q // 2, q % 2))
        rbuf[i, z, y, core, :, off:off + w] = sbuf[p][db, 0, aa]

    def chunk_rows(i, dbs):
        for db in dbs:
            for p in range(np_):
                send_rows(p, db, i)

    def body(dbs):
        def run(i, carry):
            chunk_rows(i, dbs)
            return carry
        return run

    for p in range(np_):
        select(p, 0)
    lax.fori_loop(0, n, body((0,)), 0)
    for p in range(np_):
        drain(tbuf[p].at[pl.ds(0, n - 1)], tb_r.at[p])
    for db in near_first:
        for p in range(np_):
            drain(xbuf[p].at[0], xb_r.at[p, db - 1])
            select(p, db)
        chunk_rows(0, (db,))
    lax.fori_loop(1, n, body(near_first), 0)

    cols = 2 * n * CAP
    for p in range(np_):
        (a, sa), (b, sb), (_, sc) = mine[p]
        slot = _iota((experts, cols), 1)
        ident = slot // (2 * CAP) * sc + lax.rem(slot // CAP, 2) + a * sa + b * sb
        spread = (ident == _iota((experts, cols), 0)).astype(BF16)
        keep = _iota((CAP, cols), 0) == lax.rem(_iota((CAP, cols), 1), CAP)
        for bb in range(n):
            tg = tbuf[p][bb]
            gate = tg[:, CAP:]
            g1 = gate.astype(BF16).astype(F32)
            g2 = (gate - g1).astype(BF16).astype(F32)
            g3 = gate - g1 - g2
            terms = jnp.concatenate([tg[:, :CAP], g1, g2, g3], axis=1).reshape(n * 4 * CAP, experts).astype(BF16)
            wide = jnp.dot(terms, spread, preferred_element_type=F32)
            for aa in range(n):
                line = [jnp.sum(jnp.where(keep, wide[(aa * 4 + i) * CAP:(aa * 4 + i + 1) * CAP], 0.0), axis=0, keepdims=True) for i in range(4)]
                here = line[0] == _iota((tok, cols), 0).astype(F32)
                mixbuf[p][bb, aa] = jnp.concatenate([jnp.where(here, line[i], 0.0) for i in (1, 2, 3)], axis=0).astype(BF16)

    for load in loads[3:]:
        load.wait()

    ring = (2, 1, 3, 0) if n == 4 else tuple(range(1, n)) + (0,)

    def expert(i, carry):
        for p in range(np_):
            drain(sbuf[p].at[:, pl.ds(0, 2 * n - 1), 0], c_r.at[p, i])
        rows = rbuf[i].reshape(n * n * 2 * CAP, width)
        g = jnp.dot(rows, wg[...], preferred_element_type=F32)
        u = jnp.dot(rows, wu[...], preferred_element_type=F32)
        h = (g * jax.nn.sigmoid(g) * u).astype(BF16)
        o = jnp.dot(h, wd[...], preferred_element_type=F32).astype(BF16)
        obuf[i] = o.reshape(n, n, 2, CAP, width)
        for db in ring:
            for q in q_order + (0,):
                for p, (off, w) in enumerate(parts):
                    cc, axes = (1 - core, theirs[p]) if q % 2 else (core, mine[p])
                    (_, _), (b, _), (k, _) = axes
                    kk, bb = mod(k + q // 2), mod(b + db)
                    aa = mod(i + 2 * n - bb - kk)
                    z, y = canon(p, cc, aa, bb, kk)
                    if q:
                        put(obuf.at[i, z, y, cc, :, pl.ds(off, w)], cbuf[p].at[bb, aa, k * 2 + core],
                            rc_s.at[p], rc_r.at[p, db, i], moved(axes[2], q // 2, q % 2))
                    else:
                        cbuf[p][bb, aa, k * 2 + core] = obuf[i, z, y, cc, :, off:off + w]
        return carry

    def line_sum(p, db, i):
        w = parts[p][1]
        _, (b, _), (k, _) = mine[p]
        bb = mod(b + db)
        aa = mod(i + 2 * n - bb - k)
        drain(cbuf[p].at[0, 0, pl.ds(0, 2 * n - 1)], rc_r.at[p, db, i])
        part = jnp.dot(mixbuf[p][bb, aa], cbuf[p][bb, aa].reshape(cols, w), preferred_element_type=F32)
        return part[:tok] + part[tok:2 * tok] + part[2 * tok:]

    def far(i):
        for p in range(np_):
            w, left = parts[p][1], lefts[i % 2][p]
            farp[p][i] = line_sum(p, 2, i)
            put(farp[p].at[i, :, pl.ds(0, left)], fari[p].at[i, :, pl.ds(0, left)], rf_s.at[p], rf_r.at[p, i], moved(mine[p][1], 1))
            put(farp[p].at[i, :, pl.ds(left, w - left)], fari[p].at[i, :, pl.ds(left, w - left)], rf_s.at[p], rf_r.at[p, i], moved(mine[p][1], n - 1))

    def near(i):
        for p in range(np_):
            left = lefts[i % 2][p]
            up, down = line_sum(p, 1, i), line_sum(p, n - 1, i)
            drain(fari[p].at[i], rf_r.at[p, i])
            nearp[p][i, 0, :, :left] = up[:, :left] + fari[p][i, :, :left]
            nearp[p][i, 0, :, left:] = up[:, left:]
            put(nearp[p].at[i, 0], neari[p].at[i, 0], rn_s.at[p], rn_r.at[p, i], moved(mine[p][1], 1))
            nearp[p][i, 1, :, :left] = down[:, :left]
            nearp[p][i, 1, :, left:] = down[:, left:] + fari[p][i, :, left:]
            put(nearp[p].at[i, 1], neari[p].at[i, 1], rn_s.at[p], rn_r.at[p, i], moved(mine[p][1], n - 1))

    def here(i):
        for p in range(np_):
            (a, sa), (b, _), (k, _) = mine[p]
            aa = mod(i + 2 * n - b - k)
            own = line_sum(p, 0, i)
            drain(neari[p].at[i], rn_r.at[p, i])
            pbuf[p][i] = own + neari[p][i, 0] + neari[p][i, 1]

            @pl.when(aa != a)
            def _():
                put(pbuf[p].at[i], abuf[p].at[a], ra_s.at[p], ra_r.at[p], me + (aa - a) * sa)

            @pl.when(aa == a)
            def _():
                abuf[p][a] = pbuf[p][i]

    steps = {'x': lambda i: expert(i, 0), 'f': far, 'n': near, 'h': here}
    todo = PLAN.split()
    if todo[0] == 'x':
        lax.fori_loop(0, n, expert, 0)
        todo = todo[1:]
    elif todo[0] == 'y':
        lax.fori_loop(0, n - 1, expert, 0)
        todo = todo[1:]
    for step in todo:
        steps[step[0]](int(step[1]))
    for p, (off, w) in enumerate(parts):
        drain(pbuf[p].at[pl.ds(0, n - 1)], ra_r.at[p])
        total = abuf[p][0]
        for i in range(1, n):
            total += abuf[p][i]
        y_ref[:, off:off + w] = total.astype(BF16)
    for p in range(np_):
        drain(tbuf[p].at[0, pl.ds(0, n - 1)], ta_s.at[p])
        drain(tbuf[p].at[pl.ds(0, n - 1)], tb_s.at[p])
        drain(xbuf[p].at[0, pl.ds(0, n - 1)], xa_s.at[p])
        drain(xbuf[p].at[pl.ds(0, n - 1)], xb_s.at[p])
        drain(sbuf[p].at[:, pl.ds(0, 2 * n - 1)], c_s.at[p])
        drain(cbuf[p].at[:, :, pl.ds(0, 2 * n - 1)], rc_s.at[p])
        drain(farp[p], rf_s.at[p])
        drain(nearp[p], rn_s.at[p])
        drain(pbuf[p].at[pl.ds(0, n - 1)], ra_s.at[p])


def build(mesh, n, parts, lefts):
    row_spec = P(('data', 'expert'), None)
    expert_spec = P('expert', None, None)
    vmem = pl.BlockSpec(memory_space=pltpu.VMEM)
    hbm = pl.BlockSpec(memory_space=pltpu.HBM)

    def device_step(tokens, w_router, routes, w_gate, w_up, w_down):
        tok, width = tokens.shape
        experts = w_router.shape[1]
        ff = w_gate.shape[2]
        dma = pltpu.SemaphoreType.DMA
        np_ = len(parts)
        cols = 2 * n * CAP
        return pl.pallas_call(
            functools.partial(moe_kernel, n, parts, lefts),
            out_shape=pltpu.VMEM((tok, width), BF16),
            in_specs=[hbm] * 6, out_specs=vmem,
            scratch_shapes=[
                pltpu.VMEM((tok, width), BF16), pltpu.VMEM((width, experts), BF16), pltpu.VMEM((routes.shape[1], tok), jnp.int32),
                pltpu.VMEM((width, ff), BF16), pltpu.VMEM((width, ff), BF16), pltpu.VMEM((ff, width), BF16),
                pltpu.VMEM((n, n, n, 2, CAP, width), BF16), pltpu.VMEM((n, n, n, 2, CAP, width), BF16),
                pltpu.VMEM((2 * CAP, experts), F32),
                *[pltpu.VMEM((n, n, 2 * CAP, experts), F32) for _ in parts],
                *[pltpu.VMEM((n, n, tok, w), BF16) for _, w in parts],
                *[pltpu.VMEM((n, 2 * n, n, CAP, w), BF16) for _, w in parts],
                *[pltpu.VMEM((n, n, 2 * n, CAP, w), BF16) for _, w in parts],
                *[pltpu.VMEM((n, tok, w), F32) for _, w in parts],
                *[pltpu.VMEM((n, tok, w), F32) for _, w in parts],
                *[pltpu.VMEM((n, 2, tok, w), F32) for _, w in parts],
                *[pltpu.VMEM((n, 2, tok, w), F32) for _, w in parts],
                *[pltpu.VMEM((n, tok, w), F32) for _, w in parts],
                *[pltpu.VMEM((n, tok, w), F32) for _, w in parts],
                *[pltpu.VMEM((n, n, 3 * tok, cols), BF16) for _ in parts],
                dma((6,)), dma((np_,)), dma((np_,)), dma((np_,)), dma((np_,)),
                dma((np_,)), dma((np_, n - 1)), dma((np_,)), dma((np_, n - 1)), dma((np_,)), dma((np_, n)),
                dma((np_,)), dma((np_, n, n)), dma((np_,)), dma((np_, n)), dma((np_,)), dma((np_, n)), dma((np_,)), dma((np_,)),
            ],
            compiler_params=pltpu.CompilerParams(collective_id=0, has_side_effects=True, vmem_limit_bytes=57 * 1024 * 1024),
            name='moe',
        )(tokens, w_router, routes.T, w_gate, w_up, w_down)

    return jax.shard_map(device_step, mesh=mesh, in_specs=(row_spec, P(None, None), row_spec, expert_spec, expert_spec, expert_spec), out_specs=row_spec, check_vma=False)


def solution(mesh):
    return build(mesh, 4, ((0, 768), (768, 640), (1408, 640)), ((384, 384, 256), (384, 256, 384)))
```

```python
import functools

import jax
import jax.numpy as jnp
from jax import lax
from jax.experimental import pallas as pl
from jax.experimental.pallas import tpu as pltpu
from jax.sharding import PartitionSpec as P

F32 = jnp.float32
BF16 = jnp.bfloat16
CAP = 8
RETURN_STEPS = ('f0', 'x3', 'f1', 'f2', 'n0', 'f3', 'n1', 'n2', 'n3', 'h0', 'h1', 'h2', 'h3')


def _iota(shape, dim):
    return lax.broadcasted_iota(jnp.int32, shape, dim)


def _places(r):
    return (2 - r) % 3, (1 - r) % 3, (-r) % 3


def routing_table(x, wr, routes_t):
    tok, experts = x.shape[0], wr.shape[1]
    top_k = routes_t.shape[0]
    logits = jnp.dot(x, wr, preferred_element_type=F32)
    eye = (_iota((top_k, top_k), 0) == _iota((top_k, top_k), 1)).astype(BF16)
    routes = lax.dot_general(routes_t.astype(F32).astype(BF16), eye, (((0,), (0,)), ((), ())), preferred_element_type=F32)
    lane = _iota((tok, experts), 1).astype(F32)
    hit = jnp.zeros((tok, experts), F32)
    for j in range(top_k):
        hit += (routes[:, j:j + 1] == lane).astype(F32)
    on = hit > 0.5
    top = jnp.max(jnp.where(on, logits, -jnp.inf), axis=1, keepdims=True)
    e = jnp.where(on, jnp.exp(jnp.where(on, logits, top) - top), 0.0)
    gate = e / jnp.sum(e, axis=1, keepdims=True)
    below = (_iota((tok, tok), 1) < _iota((tok, tok), 0)).astype(BF16)
    rank = jnp.dot(below, hit.astype(BF16), preferred_element_type=F32)
    rank = jnp.where(on, rank, -1.0)
    row = _iota((tok, experts), 0).astype(F32)
    toks, gates = [], []
    for r in range(CAP):
        at = rank == r
        toks.append(jnp.sum(jnp.where(at, row + 1.0, 0.0), axis=0, keepdims=True) - 1.0)
        gates.append(jnp.sum(jnp.where(at, gate, 0.0), axis=0, keepdims=True))
    return jnp.concatenate(toks + gates, axis=0)


def moe_kernel(n, parts, lefts, x_hbm, wr_hbm, rt_hbm, wg_hbm, wu_hbm, wd_hbm, y_ref, x_ref, wr_ref, rt_ref, wg, wu, wd, rbuf, obuf, tab_ref, *rest):
    np_ = len(parts)
    tbuf, xbuf, sbuf, cbuf, farp, fari, nearp, neari, pbuf, abuf, mixbuf, ownbuf = [rest[i * np_:(i + 1) * np_] for i in range(12)]
    (w_sem, ta_s, ta_r, tb_s, tb_r, xa_s, xa_r, xb_s, xb_r, xd_s, xd_r, c_s, c_r, rc_s, rc_r, rf_s, rf_r, rn_s, rn_r, ra_s, ra_r) = rest[12 * np_:]
    tok, width = x_ref.shape
    experts = tab_ref.shape[1]
    me = lax.axis_index('expert')
    strides = (2 * n * n, 2 * n, 2)
    pos = tuple(lax.rem(me // s, n) for s in strides)
    core = lax.rem(me, 2)
    mod = lambda v: lax.rem(v, n)

    def order(p, cc):
        r0, r1 = _places(p % 3), _places((p + 1) % 3)
        return [(pos[i] + cc * (pos[j] - pos[i]), strides[i] + cc * (strides[j] - strides[i])) for i, j in zip(r0, r1)]

    mine = [order(p, core) for p in range(np_)]
    theirs = [order(p, 1 - core) for p in range(np_)]

    def moved(axis, d, flip=0):
        where, stride = axis
        other = me + (mod(where + d) - where) * stride
        return other + (1 - 2 * core) if flip else other

    def put(src, dst, send, recv, device):
        pltpu.make_async_remote_copy(src_ref=src, dst_ref=dst, send_sem=send, recv_sem=recv,
                                     device_id={'expert': device}, device_id_type=pl.DeviceIdType.MESH).start()

    def drain(ref, sem):
        pltpu.make_async_copy(ref, ref, sem).wait()

    def canon(p, cc, a, b, k):
        r0, r1 = _places(p % 3), _places((p + 1) % 3)
        v = (a, b, k)
        return [v[r0.index(j)] + cc * (v[r1.index(j)] - v[r0.index(j)]) for j in (0, 1)]

    loads = [pltpu.make_async_copy(src, dst, w_sem.at[i]) for i, (src, dst) in enumerate(((x_hbm, x_ref), (wr_hbm, wr_ref), (rt_hbm, rt_ref), (wg_hbm.at[0], wg), (wu_hbm.at[0], wu), (wd_hbm.at[0], wd)))]
    for load in loads:
        load.start()

    barrier = pltpu.get_barrier_semaphore()
    peers = [moved((pos[j], strides[j]), d, flip) for j in range(3) for d in range(1, n) for flip in (0, 1)] + [me + 1 - 2 * core]
    for peer in peers:
        pl.semaphore_signal(barrier, inc=1, device_id={'expert': peer}, device_id_type=pl.DeviceIdType.MESH)
    for load in loads[:3]:
        load.wait()
    tab_ref[...] = routing_table(x_ref[...], wr_ref[...], rt_ref[...])
    for p, (off, w) in enumerate(parts):
        (a, _), (b, _), _ = mine[p]
        xbuf[p][b, a] = x_ref[:, off:off + w]
        tbuf[p][b, a] = tab_ref[...]
    pl.semaphore_wait(barrier, len(peers))

    near_first, far_first = (1, 3, 2), (2, 1, 3)

    q_order = (4, 5, 2, 3, 6, 7, 1)

    def select(p, db):
        off, w = parts[p]
        (a, _), (b, _), (k, _) = mine[p]
        bb = mod(b + n - db)
        table = tbuf[p][bb][:, :CAP].reshape(n * CAP, experts)
        shift = (_iota((n * CAP, 1), 0) // CAP * tok).astype(F32)
        lane = _iota((n * CAP, experts), 1)
        token = _iota((n * CAP, n * tok), 1).astype(F32)
        picks = []
        for q in range(2 * n):
            col = jnp.sum(jnp.where(lane == moved(mine[p][2], q // 2, q % 2), table, 0.0), axis=1, keepdims=True)
            want = jnp.where(col >= 0.0, col + shift, -1.0)
            picks.append((want == token).astype(F32))
        pick = jnp.concatenate(picks, axis=0).astype(BF16)
        rows = jnp.dot(pick, xbuf[p][bb].reshape(n * tok, w), preferred_element_type=F32).astype(BF16)
        sbuf[p][db] = rows.reshape(2 * n, n, CAP, w)

    def send_rows(p, db, i):
        off, w = parts[p]
        (a, _), (b, _), (k, _) = mine[p]
        bb = mod(b + n - db)
        aa = mod(i + 2 * n - bb - k)
        z, y = canon(p, core, aa, bb, k)

        def go():
            for q in q_order:
                put(sbuf[p].at[db, q, aa], rbuf.at[i, z, y, core, :, pl.ds(off, w)], c_s.at[p], c_r.at[p, i], moved(mine[p][2], q // 2, q % 2))
            rbuf[i, z, y, core, :, off:off + w] = sbuf[p][db, 0, aa]

        if db:
            go()
        else:
            pl.when(aa != a)(go)

    def own_rows():
        for p, (off, w) in enumerate(parts):
            (a, _), (b, _), (k, _) = mine[p]
            i = mod(a + b + k)
            table = tab_ref[:CAP]
            lane = _iota((CAP, experts), 1)
            token = _iota((CAP, tok), 1).astype(F32)
            picks = []
            for q in range(2 * n):
                col = jnp.sum(jnp.where(lane == moved(mine[p][2], q // 2, q % 2), table, 0.0), axis=1, keepdims=True)
                picks.append((col == token).astype(F32))
            pick = jnp.concatenate(picks, axis=0).astype(BF16)
            rows = jnp.dot(pick, x_ref[:, off:off + w], preferred_element_type=F32).astype(BF16)
            ownbuf[p][...] = rows.reshape(2 * n, CAP, w)
            z, y = canon(p, core, a, b, k)
            for q in q_order:
                put(ownbuf[p].at[q], rbuf.at[i, z, y, core, :, pl.ds(off, w)], c_s.at[p], c_r.at[p, i], moved(mine[p][2], q // 2, q % 2))
            rbuf[i, z, y, core, :, off:off + w] = ownbuf[p][0]

    def chunk_rows(i, dbs):
        for db in dbs:
            for p in range(np_):
                send_rows(p, db, i)

    def body(dbs):
        def run(i, carry):
            chunk_rows(i, dbs)
            return carry
        return run


    for d in far_first:
        for p in range(np_):
            (a, _), (b, _), _ = mine[p]
            put(tab_ref, tbuf[p].at[b, a], ta_s.at[p], ta_r.at[p], moved(mine[p][0], d))
    def own_a(d):
        for p, (off, w) in enumerate(parts):
            (a, _), (b, _), _ = mine[p]
            put(x_ref.at[:, pl.ds(off, w)], xbuf[p].at[b, a], xa_s.at[p], xa_r.at[p, d - 1], moved(mine[p][0], d))

    def own_b(side):
        for p, (off, w) in enumerate(parts):
            (a, _), (b, _), _ = mine[p]
            put(x_ref.at[:, pl.ds(off, w)], xbuf[p].at[b, a], xb_s.at[p], xb_r.at[p, side, 0], moved(mine[p][1], 1 + 2 * side))
    own_a(1)
    own_a(3)
    own_b(0)
    own_b(1)
    own_a(2)
    own_rows()
    for p in range(np_):
        b = mine[p][1][0]
        drain(tbuf[p].at[0, pl.ds(0, n - 1)], ta_r.at[p])
        for d in far_first:
            put(tbuf[p].at[b], tbuf[p].at[b], tb_s.at[p], tb_r.at[p], moved(mine[p][1], d))

    def along_b(da):
        for p in range(np_):
            (a, _), (b, _), _ = mine[p]
            src = mod(a + n - da)
            drain(xbuf[p].at[0, 0], xa_r.at[p, da - 1])
            for side in (0, 1):
                put(xbuf[p].at[b, src], xbuf[p].at[b, src], xb_s.at[p], xb_r.at[p, side, da], moved(mine[p][1], 1 + 2 * side))

    def onward(da):
        for side in (0, 1):
            for p, (off, w) in enumerate(parts):
                (a, _), (b, _), _ = mine[p]
                src, bb = mod(a + n - da), mod(b + n - 1 - 2 * side)
                left = lefts[da % 2][p]
                drain(xbuf[p].at[0, 0], xb_r.at[p, side, da])
                half = pl.ds(left, w - left) if side else pl.ds(0, left)
                put(xbuf[p].at[bb, src, :, half], xbuf[p].at[bb, src, :, half], xd_s.at[p], xd_r.at[p], moved(mine[p][1], 1 + 2 * side))

    along_b(1)
    along_b(3)
    onward(0)
    along_b(2)

    for p in range(np_):
        select(p, 0)
    lax.fori_loop(0, n - 1, body((0,)), 0)
    for da in near_first:
        onward(da)
    chunk_rows(n - 1, (0,))
    for p in range(np_):
        drain(tbuf[p].at[pl.ds(0, n - 1)], tb_r.at[p])
    for db in (1, 3):
        for p in range(np_):
            select(p, db)
        chunk_rows(0, (db,))
    chunk_rows(1, (1, 3))
    for p in range(np_):
        drain(xbuf[p].at[0], xd_r.at[p])
        select(p, 2)
    chunk_rows(0, (2,))
    chunk_rows(1, (2,))
    lax.fori_loop(2, n, body((1, 3, 2)), 0)

    cols = 2 * n * CAP
    for p in range(np_):
        (a, sa), (b, sb), (_, sc) = mine[p]
        slot = _iota((experts, cols), 1)
        ident = slot // (2 * CAP) * sc + lax.rem(slot // CAP, 2) + a * sa + b * sb
        spread = (ident == _iota((experts, cols), 0)).astype(BF16)
        keep = _iota((CAP, cols), 0) == lax.rem(_iota((CAP, cols), 1), CAP)
        for bb in range(n):
            tg = tbuf[p][bb]
            gate = tg[:, CAP:]
            g1 = gate.astype(BF16).astype(F32)
            g2 = (gate - g1).astype(BF16).astype(F32)
            g3 = gate - g1 - g2
            terms = jnp.concatenate([tg[:, :CAP], g1, g2, g3], axis=1).reshape(n * 4 * CAP, experts).astype(BF16)
            wide = jnp.dot(terms, spread, preferred_element_type=F32)
            for aa in range(n):
                line = [jnp.sum(jnp.where(keep, wide[(aa * 4 + i) * CAP:(aa * 4 + i + 1) * CAP], 0.0), axis=0, keepdims=True) for i in range(4)]
                here = line[0] == _iota((tok, cols), 0).astype(F32)
                mixbuf[p][bb, aa] = jnp.concatenate([jnp.where(here, line[i], 0.0) for i in (1, 2, 3)], axis=0).astype(BF16)

    for load in loads[3:]:
        load.wait()

    ring = (2, 1, 3, 0) if n == 4 else tuple(range(1, n)) + (0,)

    def expert(i, carry):
        for p in range(np_):
            drain(sbuf[p].at[:, pl.ds(0, 2 * n - 1), 0], c_r.at[p, i])
        rows = rbuf[i].reshape(n * n * 2 * CAP, width)
        g = jnp.dot(rows, wg[...], preferred_element_type=F32)
        u = jnp.dot(rows, wu[...], preferred_element_type=F32)
        h = (g * jax.nn.sigmoid(g) * u).astype(BF16)
        o = jnp.dot(h, wd[...], preferred_element_type=F32).astype(BF16)
        obuf[i] = o.reshape(n, n, 2, CAP, width)
        for db in ring:
            for q in q_order + (0,):
                for p, (off, w) in enumerate(parts):
                    cc, axes = (1 - core, theirs[p]) if q % 2 else (core, mine[p])
                    (_, _), (b, _), (k, _) = axes
                    kk, bb = mod(k + q // 2), mod(b + db)
                    aa = mod(i + 2 * n - bb - kk)
                    z, y = canon(p, cc, aa, bb, kk)
                    if q:
                        put(obuf.at[i, z, y, cc, :, pl.ds(off, w)], cbuf[p].at[bb, aa, k * 2 + core],
                            rc_s.at[p], rc_r.at[p, db, i], moved(axes[2], q // 2, q % 2))
                    else:
                        cbuf[p][bb, aa, k * 2 + core] = obuf[i, z, y, cc, :, off:off + w]
        return carry

    def line_sum(p, db, i):
        w = parts[p][1]
        _, (b, _), (k, _) = mine[p]
        bb = mod(b + db)
        aa = mod(i + 2 * n - bb - k)
        drain(cbuf[p].at[0, 0, pl.ds(0, 2 * n - 1)], rc_r.at[p, db, i])
        part = jnp.dot(mixbuf[p][bb, aa], cbuf[p][bb, aa].reshape(cols, w), preferred_element_type=F32)
        return part[:tok] + part[tok:2 * tok] + part[2 * tok:]

    def far(i):
        for p in range(np_):
            w, left = parts[p][1], lefts[i % 2][p]
            farp[p][i] = line_sum(p, 2, i)
            put(farp[p].at[i, :, pl.ds(0, left)], fari[p].at[i, :, pl.ds(0, left)], rf_s.at[p], rf_r.at[p, i], moved(mine[p][1], 1))
            put(farp[p].at[i, :, pl.ds(left, w - left)], fari[p].at[i, :, pl.ds(left, w - left)], rf_s.at[p], rf_r.at[p, i], moved(mine[p][1], n - 1))

    def near(i):
        for p in range(np_):
            left = lefts[i % 2][p]
            up, down = line_sum(p, 1, i), line_sum(p, n - 1, i)
            drain(fari[p].at[i], rf_r.at[p, i])
            nearp[p][i, 0, :, :left] = up[:, :left] + fari[p][i, :, :left]
            nearp[p][i, 0, :, left:] = up[:, left:]
            put(nearp[p].at[i, 0], neari[p].at[i, 0], rn_s.at[p], rn_r.at[p, i], moved(mine[p][1], 1))
            nearp[p][i, 1, :, :left] = down[:, :left]
            nearp[p][i, 1, :, left:] = down[:, left:] + fari[p][i, :, left:]
            put(nearp[p].at[i, 1], neari[p].at[i, 1], rn_s.at[p], rn_r.at[p, i], moved(mine[p][1], n - 1))

    def here(i):
        for p in range(np_):
            (a, sa), (b, _), (k, _) = mine[p]
            aa = mod(i + 2 * n - b - k)
            own = line_sum(p, 0, i)
            drain(neari[p].at[i], rn_r.at[p, i])
            pbuf[p][i] = own + neari[p][i, 0] + neari[p][i, 1]

            @pl.when(aa != a)
            def _():
                put(pbuf[p].at[i], abuf[p].at[a], ra_s.at[p], ra_r.at[p], me + (aa - a) * sa)

            @pl.when(aa == a)
            def _():
                abuf[p][a] = pbuf[p][i]

    steps = {'x': lambda i: expert(i, 0), 'f': far, 'n': near, 'h': here}
    lax.fori_loop(0, n - 1, expert, 0)
    for step in RETURN_STEPS:
        steps[step[0]](int(step[1]))
    for p, (off, w) in enumerate(parts):
        drain(pbuf[p].at[pl.ds(0, n - 1)], ra_r.at[p])
        total = abuf[p][0]
        for i in range(1, n):
            total += abuf[p][i]
        y_ref[:, off:off + w] = total.astype(BF16)
    for p in range(np_):
        drain(tbuf[p].at[0, pl.ds(0, n - 1)], ta_s.at[p])
        drain(tbuf[p].at[pl.ds(0, n - 1)], tb_s.at[p])
        drain(xbuf[p].at[0, pl.ds(0, n - 1)], xa_s.at[p])
        drain(xbuf[p].at[pl.ds(0, 2)], xb_s.at[p])
        drain(xbuf[p].at[0], xd_s.at[p])
        drain(sbuf[p].at[:, pl.ds(0, 2 * n - 1)], c_s.at[p])
        drain(cbuf[p].at[:, :, pl.ds(0, 2 * n - 1)], rc_s.at[p])
        drain(farp[p], rf_s.at[p])
        drain(nearp[p], rn_s.at[p])
        drain(pbuf[p].at[pl.ds(0, n - 1)], ra_s.at[p])


def build(mesh, n, parts, lefts):
    row_spec = P(('data', 'expert'), None)
    expert_spec = P('expert', None, None)
    vmem = pl.BlockSpec(memory_space=pltpu.VMEM)
    hbm = pl.BlockSpec(memory_space=pltpu.HBM)

    def device_step(tokens, w_router, routes, w_gate, w_up, w_down):
        tok, width = tokens.shape
        experts = w_router.shape[1]
        ff = w_gate.shape[2]
        dma = pltpu.SemaphoreType.DMA
        np_ = len(parts)
        cols = 2 * n * CAP
        return pl.pallas_call(
            functools.partial(moe_kernel, n, parts, lefts),
            out_shape=pltpu.VMEM((tok, width), BF16),
            in_specs=[hbm] * 6, out_specs=vmem,
            scratch_shapes=[
                pltpu.VMEM((tok, width), BF16), pltpu.VMEM((width, experts), BF16), pltpu.VMEM((routes.shape[1], tok), jnp.int32),
                pltpu.VMEM((width, ff), BF16), pltpu.VMEM((width, ff), BF16), pltpu.VMEM((ff, width), BF16),
                pltpu.VMEM((n, n, n, 2, CAP, width), BF16), pltpu.VMEM((n, n, n, 2, CAP, width), BF16),
                pltpu.VMEM((2 * CAP, experts), F32),
                *[pltpu.VMEM((n, n, 2 * CAP, experts), F32) for _ in parts],
                *[pltpu.VMEM((n, n, tok, w), BF16) for _, w in parts],
                *[pltpu.VMEM((n, 2 * n, n, CAP, w), BF16) for _, w in parts],
                *[pltpu.VMEM((n, n, 2 * n, CAP, w), BF16) for _, w in parts],
                *[pltpu.VMEM((n, tok, w), F32) for _, w in parts],
                *[pltpu.VMEM((n, tok, w), F32) for _, w in parts],
                *[pltpu.VMEM((n, 2, tok, w), F32) for _, w in parts],
                *[pltpu.VMEM((n, 2, tok, w), F32) for _, w in parts],
                *[pltpu.VMEM((n, tok, w), F32) for _, w in parts],
                *[pltpu.VMEM((n, tok, w), F32) for _, w in parts],
                *[pltpu.VMEM((n, n, 3 * tok, cols), BF16) for _ in parts],
                *[pltpu.VMEM((2 * n, CAP, w), BF16) for _, w in parts],
                dma((6,)), dma((np_,)), dma((np_,)), dma((np_,)), dma((np_,)),
                dma((np_,)), dma((np_, n - 1)), dma((np_,)), dma((np_, 2, n)), dma((np_,)), dma((np_,)), dma((np_,)), dma((np_, n)),
                dma((np_,)), dma((np_, n, n)), dma((np_,)), dma((np_, n)), dma((np_,)), dma((np_, n)), dma((np_,)), dma((np_,)),
            ],
            compiler_params=pltpu.CompilerParams(collective_id=0, has_side_effects=True, vmem_limit_bytes=57 * 1024 * 1024),
            name='moe',
        )(tokens, w_router, routes.T, w_gate, w_up, w_down)

    return jax.shard_map(device_step, mesh=mesh, in_specs=(row_spec, P(None, None), row_spec, expert_spec, expert_spec, expert_spec), out_specs=row_spec, check_vma=False)


def solution(mesh):
    return build(mesh, 4, ((0, 768), (768, 640), (1408, 640)), ((384, 384, 256), (384, 256, 384)))
```

```python
import functools

import jax
import jax.numpy as jnp
from jax import lax
from jax.experimental import pallas as pl
from jax.experimental.pallas import tpu as pltpu
from jax.sharding import PartitionSpec as P

F32 = jnp.float32
BF16 = jnp.bfloat16
CAP = 8
RETURN_STEPS = ('f0', 'x3', 'f1', 'f2', 'n0', 'f3', 'n1', 'n2', 'n3', 'h0', 'h1', 'h2', 'h3')


def _iota(shape, dim):
    return lax.broadcasted_iota(jnp.int32, shape, dim)


def _places(r):
    return (2 - r) % 3, (1 - r) % 3, (-r) % 3


def routing_table(x, wr, routes_t):
    tok, experts = x.shape[0], wr.shape[1]
    top_k = routes_t.shape[0]
    logits = jnp.dot(x, wr, preferred_element_type=F32).T
    ident = _iota((experts, tok), 0)
    chosen = [ident == routes_t[j:j + 1] for j in range(top_k)]
    hit = jnp.zeros((experts, tok), F32)
    for c in chosen:
        hit += c.astype(F32)
    on = hit > 0.5
    top = jnp.max(jnp.where(on, logits, -jnp.inf), axis=0, keepdims=True)
    e = jnp.where(on, jnp.exp(jnp.where(on, logits, top) - top), 0.0)
    gate = e / jnp.sum(e, axis=0, keepdims=True)
    above = (_iota((tok, tok), 0) < _iota((tok, tok), 1)).astype(BF16)
    slot = jnp.dot(hit.astype(BF16), above, preferred_element_type=F32)
    pick = lambda c, v: jnp.sum(jnp.where(c, v, 0.0), axis=0, keepdims=True)
    codes = [routes_t[j:j + 1].astype(F32) * CAP + pick(chosen[j], slot) for j in range(top_k)]
    return jnp.concatenate(codes + [pick(c, gate) for c in chosen], axis=0)


def split3(v):
    v1 = v.astype(BF16).astype(F32)
    v2 = (v - v1).astype(BF16).astype(F32)
    return v1, v2, v - v1 - v2


def one_hot(codes, want):
    out = jnp.zeros((want.shape[0], codes.shape[1]), F32)
    for j in range(codes.shape[0]):
        out += (codes[j:j + 1] == want).astype(F32)
    return out


def moe_kernel(n, parts, lefts, x_hbm, wr_hbm, rt_hbm, wg_hbm, wu_hbm, wd_hbm, y_ref, x_ref, wr_ref, rt_ref, wg, wu, wd, rbuf, obuf, tab_ref, *rest):
    top_k = rt_ref.shape[0]
    np_ = len(parts)
    tbuf, xbuf, sbuf, cbuf, farp, fari, nearp, neari, pbuf, abuf, mixbuf, ownbuf, tline = [rest[i * np_:(i + 1) * np_] for i in range(13)]
    (w_sem, ta_s, ta_r, tb_s, tb_r, xa_s, xa_r, xb_s, xb_r, xd_s, xd_r, c_s, c_r, rc_s, rc_r, rf_s, rf_r, rn_s, rn_r, ra_s, ra_r) = rest[13 * np_:]
    tok, width = x_ref.shape
    experts = wr_ref.shape[1]
    me = lax.axis_index('expert')
    strides = (2 * n * n, 2 * n, 2)
    pos = tuple(lax.rem(me // s, n) for s in strides)
    core = lax.rem(me, 2)
    mod = lambda v: lax.rem(v, n)

    def order(p, cc):
        r0, r1 = _places(p % 3), _places((p + 1) % 3)
        return [(pos[i] + cc * (pos[j] - pos[i]), strides[i] + cc * (strides[j] - strides[i])) for i, j in zip(r0, r1)]

    mine = [order(p, core) for p in range(np_)]
    theirs = [order(p, 1 - core) for p in range(np_)]

    def moved(axis, d, flip=0):
        where, stride = axis
        other = me + (mod(where + d) - where) * stride
        return other + (1 - 2 * core) if flip else other

    def put(src, dst, send, recv, device):
        pltpu.make_async_remote_copy(src_ref=src, dst_ref=dst, send_sem=send, recv_sem=recv,
                                     device_id={'expert': device}, device_id_type=pl.DeviceIdType.MESH).start()

    def drain(ref, sem):
        pltpu.make_async_copy(ref, ref, sem).wait()

    def canon(p, cc, a, b, k):
        r0, r1 = _places(p % 3), _places((p + 1) % 3)
        v = (a, b, k)
        return [v[r0.index(j)] + cc * (v[r1.index(j)] - v[r0.index(j)]) for j in (0, 1)]

    loads = [pltpu.make_async_copy(src, dst, w_sem.at[i]) for i, (src, dst) in enumerate(((x_hbm, x_ref), (wr_hbm, wr_ref), (rt_hbm, rt_ref), (wg_hbm.at[0], wg), (wu_hbm.at[0], wu), (wd_hbm.at[0], wd)))]
    for load in loads:
        load.start()

    barrier = pltpu.get_barrier_semaphore()
    peers = [moved((pos[j], strides[j]), d, flip) for j in range(3) for d in range(1, n) for flip in (0, 1)] + [me + 1 - 2 * core]
    for peer in peers:
        pl.semaphore_signal(barrier, inc=1, device_id={'expert': peer}, device_id_type=pl.DeviceIdType.MESH)
    for load in loads[:3]:
        load.wait()
    tab_ref[...] = routing_table(x_ref[...], wr_ref[...], rt_ref[...])
    terms = jnp.concatenate(split3(tab_ref[...]), axis=0).astype(BF16)
    for p, (off, w) in enumerate(parts):
        (a, _), (b, _), _ = mine[p]
        xbuf[p][b, a] = x_ref[:, off:off + w]
        place = (_iota((tok, n * tok), 1) == _iota((tok, n * tok), 0) + a * tok).astype(BF16)
        wide = jnp.dot(terms, place, preferred_element_type=F32)
        tline[p][a] = wide[:2 * top_k] + wide[2 * top_k:4 * top_k] + wide[4 * top_k:]
    pl.semaphore_wait(barrier, len(peers))

    near_first, far_first = (1, 3, 2), (2, 1, 3)

    q_order = (4, 5, 2, 3, 6, 7, 1)

    def select(p, db):
        off, w = parts[p]
        (a, _), (b, _), (k, _) = mine[p]
        bb = mod(b + n - db)
        row = _iota((n * CAP, 1), 0)
        want = jnp.concatenate([(moved(mine[p][2], q // 2, q % 2) * CAP + lax.rem(row, CAP)).astype(F32) for q in range(2 * n)], axis=0)
        shape = (2 * n * n * CAP, n * tok)
        same = lax.rem(_iota(shape, 0) // CAP, n) == _iota(shape, 1) // tok
        pick = jnp.where(same, one_hot(tbuf[p][bb, :top_k], want), 0.0).astype(BF16)
        rows = jnp.dot(pick, xbuf[p][bb].reshape(n * tok, w), preferred_element_type=F32).astype(BF16)
        sbuf[p][db] = rows.reshape(2 * n, n, CAP, w)

    def send_rows(p, db, i):
        off, w = parts[p]
        (a, _), (b, _), (k, _) = mine[p]
        bb = mod(b + n - db)
        aa = mod(i + 2 * n - bb - k)
        z, y = canon(p, core, aa, bb, k)

        def go():
            for q in q_order:
                put(sbuf[p].at[db, q, aa], rbuf.at[i, z, y, core, :, pl.ds(off, w)], c_s.at[p], c_r.at[p, i], moved(mine[p][2], q // 2, q % 2))
            rbuf[i, z, y, core, :, off:off + w] = sbuf[p][db, 0, aa]

        if db:
            go()
        else:
            pl.when(aa != a)(go)

    def own_rows():
        for p, (off, w) in enumerate(parts):
            (a, _), (b, _), (k, _) = mine[p]
            i = mod(a + b + k)
            row = _iota((CAP, 1), 0)
            want = jnp.concatenate([(moved(mine[p][2], q // 2, q % 2) * CAP + row).astype(F32) for q in range(2 * n)], axis=0)
            pick = one_hot(tab_ref[:top_k], want).astype(BF16)
            rows = jnp.dot(pick, x_ref[:, off:off + w], preferred_element_type=F32).astype(BF16)
            ownbuf[p][...] = rows.reshape(2 * n, CAP, w)
            z, y = canon(p, core, a, b, k)
            for q in q_order:
                put(ownbuf[p].at[q], rbuf.at[i, z, y, core, :, pl.ds(off, w)], c_s.at[p], c_r.at[p, i], moved(mine[p][2], q // 2, q % 2))
            rbuf[i, z, y, core, :, off:off + w] = ownbuf[p][0]

    def chunk_rows(i, dbs):
        for db in dbs:
            for p in range(np_):
                send_rows(p, db, i)

    def body(dbs):
        def run(i, carry):
            chunk_rows(i, dbs)
            return carry
        return run


    for d in far_first:
        for p in range(np_):
            (a, _), (b, _), _ = mine[p]
            put(tline[p].at[a], tline[p].at[a], ta_s.at[p], ta_r.at[p], moved(mine[p][0], d))
    def own_a(d):
        for p, (off, w) in enumerate(parts):
            (a, _), (b, _), _ = mine[p]
            put(x_ref.at[:, pl.ds(off, w)], xbuf[p].at[b, a], xa_s.at[p], xa_r.at[p, d - 1], moved(mine[p][0], d))

    def own_b(side):
        for p, (off, w) in enumerate(parts):
            (a, _), (b, _), _ = mine[p]
            put(x_ref.at[:, pl.ds(off, w)], xbuf[p].at[b, a], xb_s.at[p], xb_r.at[p, side, 0], moved(mine[p][1], 1 + 2 * side))
    own_a(1)
    own_a(3)
    own_b(0)
    own_b(1)
    own_a(2)
    own_rows()
    for p in range(np_):
        b = mine[p][1][0]
        drain(tline[p].at[pl.ds(0, n - 1)], ta_r.at[p])
        line = tline[p][0]
        for i in range(1, n):
            line += tline[p][i]
        tbuf[p][b] = line
        for d in far_first:
            put(tbuf[p].at[b], tbuf[p].at[b], tb_s.at[p], tb_r.at[p], moved(mine[p][1], d))

    def along_b(da):
        for p in range(np_):
            (a, _), (b, _), _ = mine[p]
            src = mod(a + n - da)
            drain(xbuf[p].at[0, 0], xa_r.at[p, da - 1])
            for side in (0, 1):
                put(xbuf[p].at[b, src], xbuf[p].at[b, src], xb_s.at[p], xb_r.at[p, side, da], moved(mine[p][1], 1 + 2 * side))

    def onward(da):
        for side in (0, 1):
            for p, (off, w) in enumerate(parts):
                (a, _), (b, _), _ = mine[p]
                src, bb = mod(a + n - da), mod(b + n - 1 - 2 * side)
                left = lefts[da % 2][p]
                drain(xbuf[p].at[0, 0], xb_r.at[p, side, da])
                half = pl.ds(left, w - left) if side else pl.ds(0, left)
                put(xbuf[p].at[bb, src, :, half], xbuf[p].at[bb, src, :, half], xd_s.at[p], xd_r.at[p], moved(mine[p][1], 1 + 2 * side))

    along_b(1)
    along_b(3)
    onward(0)
    along_b(2)

    for p in range(np_):
        select(p, 0)
    lax.fori_loop(0, n - 1, body((0,)), 0)
    for da in near_first:
        onward(da)
    chunk_rows(n - 1, (0,))
    for p in range(np_):
        drain(tbuf[p].at[pl.ds(0, n - 1)], tb_r.at[p])
    for db in (1, 3):
        for p in range(np_):
            select(p, db)
        chunk_rows(0, (db,))
    chunk_rows(1, (1, 3))
    for p in range(np_):
        drain(xbuf[p].at[0], xd_r.at[p])
        select(p, 2)
    chunk_rows(0, (2,))
    chunk_rows(1, (2,))
    lax.fori_loop(2, n, body((1, 3, 2)), 0)

    cols = 2 * n * CAP
    for p in range(np_):
        (a, sa), (b, sb), (_, sc) = mine[p]
        slot = _iota((cols, 1), 0)
        ident = slot // (2 * CAP) * sc + lax.rem(slot // CAP, 2) + a * sa + b * sb
        want = (ident * CAP + lax.rem(slot, CAP)).astype(F32)
        for bb in range(n):
            tb = tbuf[p][bb]
            gates = split3(tb[top_k:])
            mix = [jnp.zeros((cols, n * tok), F32) for _ in gates]
            for j in range(top_k):
                at = tb[j:j + 1] == want
                mix = [m + jnp.where(at, g[j:j + 1], 0.0) for m, g in zip(mix, gates)]
            mix = [m.T for m in mix]
            for aa in range(n):
                mixbuf[p][bb, aa] = jnp.concatenate([m[aa * tok:(aa + 1) * tok] for m in mix], axis=0).astype(BF16)

    for load in loads[3:]:
        load.wait()

    ring = (2, 1, 3, 0) if n == 4 else tuple(range(1, n)) + (0,)

    def expert(i, carry):
        for p in range(np_):
            drain(sbuf[p].at[:, pl.ds(0, 2 * n - 1), 0], c_r.at[p, i])
        rows = rbuf[i].reshape(n * n * 2 * CAP, width)
        g = jnp.dot(rows, wg[...], preferred_element_type=F32)
        u = jnp.dot(rows, wu[...], preferred_element_type=F32)
        h = (g * jax.nn.sigmoid(g) * u).astype(BF16)
        o = jnp.dot(h, wd[...], preferred_element_type=F32).astype(BF16)
        obuf[i] = o.reshape(n, n, 2, CAP, width)
        for db in ring:
            for q in q_order + (0,):
                for p, (off, w) in enumerate(parts):
                    cc, axes = (1 - core, theirs[p]) if q % 2 else (core, mine[p])
                    (_, _), (b, _), (k, _) = axes
                    kk, bb = mod(k + q // 2), mod(b + db)
                    aa = mod(i + 2 * n - bb - kk)
                    z, y = canon(p, cc, aa, bb, kk)
                    if q:
                        put(obuf.at[i, z, y, cc, :, pl.ds(off, w)], cbuf[p].at[bb, aa, k * 2 + core],
                            rc_s.at[p], rc_r.at[p, db, i], moved(axes[2], q // 2, q % 2))
                    else:
                        cbuf[p][bb, aa, k * 2 + core] = obuf[i, z, y, cc, :, off:off + w]
        return carry

    def line_sum(p, db, i):
        w = parts[p][1]
        _, (b, _), (k, _) = mine[p]
        bb = mod(b + db)
        aa = mod(i + 2 * n - bb - k)
        drain(cbuf[p].at[0, 0, pl.ds(0, 2 * n - 1)], rc_r.at[p, db, i])
        part = jnp.dot(mixbuf[p][bb, aa], cbuf[p][bb, aa].reshape(cols, w), preferred_element_type=F32)
        return part[:tok] + part[tok:2 * tok] + part[2 * tok:]

    def far(i):
        for p in range(np_):
            w, left = parts[p][1], lefts[i % 2][p]
            farp[p][i] = line_sum(p, 2, i)
            put(farp[p].at[i, :, pl.ds(0, left)], fari[p].at[i, :, pl.ds(0, left)], rf_s.at[p], rf_r.at[p, i], moved(mine[p][1], 1))
            put(farp[p].at[i, :, pl.ds(left, w - left)], fari[p].at[i, :, pl.ds(left, w - left)], rf_s.at[p], rf_r.at[p, i], moved(mine[p][1], n - 1))

    def near(i):
        for p in range(np_):
            left = lefts[i % 2][p]
            up, down = line_sum(p, 1, i), line_sum(p, n - 1, i)
            drain(fari[p].at[i], rf_r.at[p, i])
            nearp[p][i, 0, :, :left] = up[:, :left] + fari[p][i, :, :left]
            nearp[p][i, 0, :, left:] = up[:, left:]
            put(nearp[p].at[i, 0], neari[p].at[i, 0], rn_s.at[p], rn_r.at[p, i], moved(mine[p][1], 1))
            nearp[p][i, 1, :, :left] = down[:, :left]
            nearp[p][i, 1, :, left:] = down[:, left:] + fari[p][i, :, left:]
            put(nearp[p].at[i, 1], neari[p].at[i, 1], rn_s.at[p], rn_r.at[p, i], moved(mine[p][1], n - 1))

    def here(i):
        for p in range(np_):
            (a, sa), (b, _), (k, _) = mine[p]
            aa = mod(i + 2 * n - b - k)
            own = line_sum(p, 0, i)
            drain(neari[p].at[i], rn_r.at[p, i])
            pbuf[p][i] = own + neari[p][i, 0] + neari[p][i, 1]

            @pl.when(aa != a)
            def _():
                put(pbuf[p].at[i], abuf[p].at[a], ra_s.at[p], ra_r.at[p], me + (aa - a) * sa)

            @pl.when(aa == a)
            def _():
                abuf[p][a] = pbuf[p][i]

    steps = {'x': lambda i: expert(i, 0), 'f': far, 'n': near, 'h': here}
    lax.fori_loop(0, n - 1, expert, 0)
    for step in RETURN_STEPS:
        steps[step[0]](int(step[1]))
    for p, (off, w) in enumerate(parts):
        drain(pbuf[p].at[pl.ds(0, n - 1)], ra_r.at[p])
        total = abuf[p][0]
        for i in range(1, n):
            total += abuf[p][i]
        y_ref[:, off:off + w] = total.astype(BF16)
    for p in range(np_):
        drain(tline[p].at[pl.ds(0, n - 1)], ta_s.at[p])
        drain(tbuf[p].at[pl.ds(0, n - 1)], tb_s.at[p])
        drain(xbuf[p].at[0, pl.ds(0, n - 1)], xa_s.at[p])
        drain(xbuf[p].at[pl.ds(0, 2)], xb_s.at[p])
        drain(xbuf[p].at[0], xd_s.at[p])
        drain(sbuf[p].at[:, pl.ds(0, 2 * n - 1)], c_s.at[p])
        drain(cbuf[p].at[:, :, pl.ds(0, 2 * n - 1)], rc_s.at[p])
        drain(farp[p], rf_s.at[p])
        drain(nearp[p], rn_s.at[p])
        drain(pbuf[p].at[pl.ds(0, n - 1)], ra_s.at[p])


def build(mesh, n, parts, lefts):
    row_spec = P(('data', 'expert'), None)
    expert_spec = P('expert', None, None)
    vmem = pl.BlockSpec(memory_space=pltpu.VMEM)
    hbm = pl.BlockSpec(memory_space=pltpu.HBM)

    def device_step(tokens, w_router, routes, w_gate, w_up, w_down):
        tok, width = tokens.shape
        experts = w_router.shape[1]
        ff = w_gate.shape[2]
        dma = pltpu.SemaphoreType.DMA
        np_ = len(parts)
        cols = 2 * n * CAP
        return pl.pallas_call(
            functools.partial(moe_kernel, n, parts, lefts),
            out_shape=pltpu.VMEM((tok, width), BF16),
            in_specs=[hbm] * 6, out_specs=vmem,
            scratch_shapes=[
                pltpu.VMEM((tok, width), BF16), pltpu.VMEM((width, experts), BF16), pltpu.VMEM((routes.shape[1], tok), jnp.int32),
                pltpu.VMEM((width, ff), BF16), pltpu.VMEM((width, ff), BF16), pltpu.VMEM((ff, width), BF16),
                pltpu.VMEM((n, n, n, 2, CAP, width), BF16), pltpu.VMEM((n, n, n, 2, CAP, width), BF16),
                pltpu.VMEM((2 * routes.shape[1], tok), F32),
                *[pltpu.VMEM((n, 2 * routes.shape[1], n * tok), F32) for _ in parts],
                *[pltpu.VMEM((n, n, tok, w), BF16) for _, w in parts],
                *[pltpu.VMEM((n, 2 * n, n, CAP, w), BF16) for _, w in parts],
                *[pltpu.VMEM((n, n, 2 * n, CAP, w), BF16) for _, w in parts],
                *[pltpu.VMEM((n, tok, w), F32) for _, w in parts],
                *[pltpu.VMEM((n, tok, w), F32) for _, w in parts],
                *[pltpu.VMEM((n, 2, tok, w), F32) for _, w in parts],
                *[pltpu.VMEM((n, 2, tok, w), F32) for _, w in parts],
                *[pltpu.VMEM((n, tok, w), F32) for _, w in parts],
                *[pltpu.VMEM((n, tok, w), F32) for _, w in parts],
                *[pltpu.VMEM((n, n, 3 * tok, cols), BF16) for _ in parts],
                *[pltpu.VMEM((2 * n, CAP, w), BF16) for _, w in parts],
                *[pltpu.VMEM((n, 2 * routes.shape[1], n * tok), F32) for _ in parts],
                dma((6,)), dma((np_,)), dma((np_,)), dma((np_,)), dma((np_,)),
                dma((np_,)), dma((np_, n - 1)), dma((np_,)), dma((np_, 2, n)), dma((np_,)), dma((np_,)), dma((np_,)), dma((np_, n)),
                dma((np_,)), dma((np_, n, n)), dma((np_,)), dma((np_, n)), dma((np_,)), dma((np_, n)), dma((np_,)), dma((np_,)),
            ],
            compiler_params=pltpu.CompilerParams(collective_id=0, has_side_effects=True, vmem_limit_bytes=57 * 1024 * 1024),
            name='moe',
        )(tokens, w_router, routes.T, w_gate, w_up, w_down)

    return jax.shard_map(device_step, mesh=mesh, in_specs=(row_spec, P(None, None), row_spec, expert_spec, expert_spec, expert_spec), out_specs=row_spec, check_vma=False)


def solution(mesh):
    return build(mesh, 4, ((0, 768), (768, 640), (1408, 640)), ((384, 384, 256), (384, 256, 384)))
```

```python
import functools

import jax
import jax.numpy as jnp
from jax import lax
from jax.experimental import pallas as pl
from jax.experimental.pallas import tpu as pltpu
from jax.sharding import PartitionSpec as P

F32 = jnp.float32
BF16 = jnp.bfloat16
CAP = 8
RETURN_STEPS = ('f0', 'x3', 'f1', 'f2', 'n0', 'f3', 'n1', 'n2', 'n3', 'h0', 'h1', 'h2', 'h3')


def _iota(shape, dim):
    return lax.broadcasted_iota(jnp.int32, shape, dim)


def _places(r):
    return (2 - r) % 3, (1 - r) % 3, (-r) % 3


def routing_table(x, wr, routes_t):
    tok, experts = x.shape[0], wr.shape[1]
    top_k = routes_t.shape[0]
    logits = jnp.dot(x, wr, preferred_element_type=F32).T
    ident = _iota((experts, tok), 0)
    chosen = [ident == routes_t[j:j + 1] for j in range(top_k)]
    hit = jnp.zeros((experts, tok), F32)
    for c in chosen:
        hit += c.astype(F32)
    on = hit > 0.5
    top = jnp.max(jnp.where(on, logits, -jnp.inf), axis=0, keepdims=True)
    e = jnp.where(on, jnp.exp(jnp.where(on, logits, top) - top), 0.0)
    gate = e / jnp.sum(e, axis=0, keepdims=True)
    above = (_iota((tok, tok), 0) < _iota((tok, tok), 1)).astype(BF16)
    slot = jnp.dot(hit.astype(BF16), above, preferred_element_type=F32)
    pick = lambda c, v: jnp.sum(jnp.where(c, v, 0.0), axis=0, keepdims=True)
    codes = [routes_t[j:j + 1].astype(F32) * CAP + pick(chosen[j], slot) for j in range(top_k)]
    return jnp.concatenate(codes + [pick(c, gate) for c in chosen], axis=0)


def split3(v):
    v1 = v.astype(BF16).astype(F32)
    v2 = (v - v1).astype(BF16).astype(F32)
    return v1, v2, v - v1 - v2


def one_hot(codes, want):
    out = jnp.zeros((want.shape[0], codes.shape[1]), F32)
    for j in range(codes.shape[0]):
        out += (codes[j:j + 1] == want).astype(F32)
    return out


def moe_kernel(n, parts, lefts, x_hbm, wr_hbm, rt_hbm, wg_hbm, wu_hbm, wd_hbm, y_ref, x_ref, wr_ref, rt_ref, wg, wu, wd, rbuf, obuf, tab_ref, *rest):
    top_k = rt_ref.shape[0]
    np_ = len(parts)
    tbuf, xbuf, sbuf, cbuf, farp, fari, nearp, neari, pbuf, abuf, mixbuf, ownbuf, tline = [rest[i * np_:(i + 1) * np_] for i in range(13)]
    (w_sem, ta_s, ta_r, tb_s, tb_r, xa_s, xa_r, xb_s, xb_r, xd_s, xd_r, c_s, c_r, rc_s, rc_r, rf_s, rf_r, rn_s, rn_r, ra_s, ra_r) = rest[13 * np_:]
    tok, width = x_ref.shape
    experts = wr_ref.shape[1]
    me = lax.axis_index('expert')
    strides = (2 * n * n, 2 * n, 2)
    pos = tuple(lax.rem(me // s, n) for s in strides)
    core = lax.rem(me, 2)
    mod = lambda v: lax.rem(v, n)

    def order(p, cc):
        r0, r1 = _places(p % 3), _places((p + 1) % 3)
        return [(pos[i] + cc * (pos[j] - pos[i]), strides[i] + cc * (strides[j] - strides[i])) for i, j in zip(r0, r1)]

    mine = [order(p, core) for p in range(np_)]
    theirs = [order(p, 1 - core) for p in range(np_)]

    def moved(axis, d, flip=0):
        where, stride = axis
        other = me + (mod(where + d) - where) * stride
        return other + (1 - 2 * core) if flip else other

    def put(src, dst, send, recv, device):
        pltpu.make_async_remote_copy(src_ref=src, dst_ref=dst, send_sem=send, recv_sem=recv,
                                     device_id={'expert': device}, device_id_type=pl.DeviceIdType.MESH).start()

    def drain(ref, sem):
        pltpu.make_async_copy(ref, ref, sem).wait()

    def canon(p, cc, a, b, k):
        r0, r1 = _places(p % 3), _places((p + 1) % 3)
        v = (a, b, k)
        return [v[r0.index(j)] + cc * (v[r1.index(j)] - v[r0.index(j)]) for j in (0, 1)]

    loads = [pltpu.make_async_copy(src, dst, w_sem.at[i]) for i, (src, dst) in enumerate(((x_hbm, x_ref), (wr_hbm, wr_ref), (rt_hbm, rt_ref), (wg_hbm.at[0], wg), (wu_hbm.at[0], wu), (wd_hbm.at[0], wd)))]
    for load in loads:
        load.start()

    barrier = pltpu.get_barrier_semaphore()
    peers = [moved((pos[j], strides[j]), d, flip) for j in range(3) for d in range(1, n) for flip in (0, 1)] + [me + 1 - 2 * core]
    for peer in peers:
        pl.semaphore_signal(barrier, inc=1, device_id={'expert': peer}, device_id_type=pl.DeviceIdType.MESH)
    for load in loads[:3]:
        load.wait()
    tab_ref[...] = routing_table(x_ref[...], wr_ref[...], rt_ref[...])
    terms = jnp.concatenate(split3(tab_ref[...]), axis=0).astype(BF16)
    for p, (off, w) in enumerate(parts):
        (a, _), (b, _), _ = mine[p]
        xbuf[p][b, a] = x_ref[:, off:off + w]
        place = (_iota((tok, n * tok), 1) == _iota((tok, n * tok), 0) + a * tok).astype(BF16)
        wide = jnp.dot(terms, place, preferred_element_type=F32)
        tline[p][a] = wide[:2 * top_k] + wide[2 * top_k:4 * top_k] + wide[4 * top_k:]
    pl.semaphore_wait(barrier, len(peers))

    near_first, far_first = (1, 3, 2), (2, 1, 3)

    q_order = (1, 4, 5, 2, 3, 6, 7)

    def select(p, db):
        off, w = parts[p]
        (a, _), (b, _), (k, _) = mine[p]
        bb = mod(b + n - db)
        row = _iota((n * CAP, 1), 0)
        want = jnp.concatenate([(moved(mine[p][2], q // 2, q % 2) * CAP + lax.rem(row, CAP)).astype(F32) for q in range(2 * n)], axis=0)
        shape = (2 * n * n * CAP, n * tok)
        same = lax.rem(_iota(shape, 0) // CAP, n) == _iota(shape, 1) // tok
        pick = jnp.where(same, one_hot(tbuf[p][bb, :top_k], want), 0.0).astype(BF16)
        rows = jnp.dot(pick, xbuf[p][bb].reshape(n * tok, w), preferred_element_type=F32).astype(BF16)
        sbuf[p][db] = rows.reshape(2 * n, n, CAP, w)

    def send_rows(p, db, i):
        off, w = parts[p]
        (a, _), (b, _), (k, _) = mine[p]
        bb = mod(b + n - db)
        aa = mod(i + 2 * n - bb - k)
        z, y = canon(p, core, aa, bb, k)

        def go():
            for q in q_order:
                put(sbuf[p].at[db, q, aa], rbuf.at[i, z, y, core, :, pl.ds(off, w)], c_s.at[p], c_r.at[p, i], moved(mine[p][2], q // 2, q % 2))
            rbuf[i, z, y, core, :, off:off + w] = sbuf[p][db, 0, aa]

        if db:
            go()
        else:
            pl.when(aa != a)(go)

    def own_rows():
        for p, (off, w) in enumerate(parts):
            (a, _), (b, _), (k, _) = mine[p]
            i = mod(a + b + k)
            row = _iota((CAP, 1), 0)
            want = jnp.concatenate([(moved(mine[p][2], q // 2, q % 2) * CAP + row).astype(F32) for q in range(2 * n)], axis=0)
            pick = one_hot(tab_ref[:top_k], want).astype(BF16)
            rows = jnp.dot(pick, x_ref[:, off:off + w], preferred_element_type=F32).astype(BF16)
            ownbuf[p][...] = rows.reshape(2 * n, CAP, w)
            z, y = canon(p, core, a, b, k)
            for q in q_order:
                put(ownbuf[p].at[q], rbuf.at[i, z, y, core, :, pl.ds(off, w)], c_s.at[p], c_r.at[p, i], moved(mine[p][2], q // 2, q % 2))
            rbuf[i, z, y, core, :, off:off + w] = ownbuf[p][0]

    def chunk_rows(i, dbs):
        for db in dbs:
            for p in range(np_):
                send_rows(p, db, i)

    def body(dbs):
        def run(i, carry):
            chunk_rows(i, dbs)
            return carry
        return run


    for d in far_first:
        for p in range(np_):
            (a, _), (b, _), _ = mine[p]
            put(tline[p].at[a], tline[p].at[a], ta_s.at[p], ta_r.at[p], moved(mine[p][0], d))
    def own_a(d):
        for p, (off, w) in enumerate(parts):
            (a, _), (b, _), _ = mine[p]
            put(x_ref.at[:, pl.ds(off, w)], xbuf[p].at[b, a], xa_s.at[p], xa_r.at[p, d - 1], moved(mine[p][0], d))

    def own_b(side):
        for p, (off, w) in enumerate(parts):
            (a, _), (b, _), _ = mine[p]
            put(x_ref.at[:, pl.ds(off, w)], xbuf[p].at[b, a], xb_s.at[p], xb_r.at[p, side, 0], moved(mine[p][1], 1 + 2 * side))
    own_a(1)
    own_a(3)
    own_b(0)
    own_b(1)
    own_a(2)
    own_rows()
    for p in range(np_):
        b = mine[p][1][0]
        drain(tline[p].at[pl.ds(0, n - 1)], ta_r.at[p])
        line = tline[p][0]
        for i in range(1, n):
            line += tline[p][i]
        tbuf[p][b] = line
        for d in far_first:
            put(tbuf[p].at[b], tbuf[p].at[b], tb_s.at[p], tb_r.at[p], moved(mine[p][1], d))

    def along_b(da):
        for p in range(np_):
            (a, _), (b, _), _ = mine[p]
            src = mod(a + n - da)
            drain(xbuf[p].at[0, 0], xa_r.at[p, da - 1])
            for side in (0, 1):
                put(xbuf[p].at[b, src], xbuf[p].at[b, src], xb_s.at[p], xb_r.at[p, side, da], moved(mine[p][1], 1 + 2 * side))

    def onward(da):
        for side in (0, 1):
            for p, (off, w) in enumerate(parts):
                (a, _), (b, _), _ = mine[p]
                src, bb = mod(a + n - da), mod(b + n - 1 - 2 * side)
                left = lefts[da % 2][p]
                drain(xbuf[p].at[0, 0], xb_r.at[p, side, da])
                half = pl.ds(left, w - left) if side else pl.ds(0, left)
                put(xbuf[p].at[bb, src, :, half], xbuf[p].at[bb, src, :, half], xd_s.at[p], xd_r.at[p], moved(mine[p][1], 1 + 2 * side))

    along_b(1)
    along_b(3)
    onward(0)
    along_b(2)

    for p in range(np_):
        select(p, 0)
    lax.fori_loop(0, n - 1, body((0,)), 0)
    for da in near_first:
        onward(da)
    chunk_rows(n - 1, (0,))
    for p in range(np_):
        drain(tbuf[p].at[pl.ds(0, n - 1)], tb_r.at[p])
    for db in (1, 3):
        for p in range(np_):
            select(p, db)
    lax.fori_loop(0, 2, body((1, 3)), 0)
    for p in range(np_):
        drain(xbuf[p].at[0], xd_r.at[p])
        select(p, 2)
    chunk_rows(0, (2,))
    chunk_rows(1, (2,))
    lax.fori_loop(2, n, body((1, 3, 2)), 0)

    cols = 2 * n * CAP
    for p in range(np_):
        (a, sa), (b, sb), (_, sc) = mine[p]
        slot = _iota((cols, 1), 0)
        ident = slot // (2 * CAP) * sc + lax.rem(slot // CAP, 2) + a * sa + b * sb
        want = (ident * CAP + lax.rem(slot, CAP)).astype(F32)
        for bb in range(n):
            tb = tbuf[p][bb]
            gates = split3(tb[top_k:])
            mix = [jnp.zeros((cols, n * tok), F32) for _ in gates]
            for j in range(top_k):
                at = tb[j:j + 1] == want
                mix = [m + jnp.where(at, g[j:j + 1], 0.0) for m, g in zip(mix, gates)]
            mix = [m.T for m in mix]
            for aa in range(n):
                mixbuf[p][bb, aa] = jnp.concatenate([m[aa * tok:(aa + 1) * tok] for m in mix], axis=0).astype(BF16)

    for load in loads[3:]:
        load.wait()

    ring = (2, 1, 3, 0) if n == 4 else tuple(range(1, n)) + (0,)

    def expert(i, carry):
        for p in range(np_):
            drain(sbuf[p].at[:, pl.ds(0, 2 * n - 1), 0], c_r.at[p, i])
        rows = rbuf[i].reshape(n * n * 2 * CAP, width)
        g = jnp.dot(rows, wg[...], preferred_element_type=F32)
        u = jnp.dot(rows, wu[...], preferred_element_type=F32)
        h = (g * jax.nn.sigmoid(g) * u).astype(BF16)
        o = jnp.dot(h, wd[...], preferred_element_type=F32).astype(BF16)
        obuf[i] = o.reshape(n, n, 2, CAP, width)
        for db in ring:
            for q in q_order + (0,):
                for p, (off, w) in enumerate(parts):
                    cc, axes = (1 - core, theirs[p]) if q % 2 else (core, mine[p])
                    (_, _), (b, _), (k, _) = axes
                    kk, bb = mod(k + q // 2), mod(b + db)
                    aa = mod(i + 2 * n - bb - kk)
                    z, y = canon(p, cc, aa, bb, kk)
                    if q:
                        put(obuf.at[i, z, y, cc, :, pl.ds(off, w)], cbuf[p].at[bb, aa, k * 2 + core],
                            rc_s.at[p], rc_r.at[p, db, i], moved(axes[2], q // 2, q % 2))
                    else:
                        cbuf[p][bb, aa, k * 2 + core] = obuf[i, z, y, cc, :, off:off + w]
        return carry

    def line_sum(p, db, i):
        w = parts[p][1]
        _, (b, _), (k, _) = mine[p]
        bb = mod(b + db)
        aa = mod(i + 2 * n - bb - k)
        drain(cbuf[p].at[0, 0, pl.ds(0, 2 * n - 1)], rc_r.at[p, db, i])
        part = jnp.dot(mixbuf[p][bb, aa], cbuf[p][bb, aa].reshape(cols, w), preferred_element_type=F32)
        return part[:tok] + part[tok:2 * tok] + part[2 * tok:]

    def far(i):
        for p in range(np_):
            w, left = parts[p][1], lefts[i % 2][p]
            farp[p][i] = line_sum(p, 2, i)
            put(farp[p].at[i, :, pl.ds(0, left)], fari[p].at[i, :, pl.ds(0, left)], rf_s.at[p], rf_r.at[p, i], moved(mine[p][1], 1))
            put(farp[p].at[i, :, pl.ds(left, w - left)], fari[p].at[i, :, pl.ds(left, w - left)], rf_s.at[p], rf_r.at[p, i], moved(mine[p][1], n - 1))

    def near(i):
        for p in range(np_):
            left = lefts[i % 2][p]
            up, down = line_sum(p, 1, i), line_sum(p, n - 1, i)
            drain(fari[p].at[i], rf_r.at[p, i])
            nearp[p][i, 0, :, :left] = up[:, :left] + fari[p][i, :, :left]
            nearp[p][i, 0, :, left:] = up[:, left:]
            put(nearp[p].at[i, 0], neari[p].at[i, 0], rn_s.at[p], rn_r.at[p, i], moved(mine[p][1], 1))
            nearp[p][i, 1, :, :left] = down[:, :left]
            nearp[p][i, 1, :, left:] = down[:, left:] + fari[p][i, :, left:]
            put(nearp[p].at[i, 1], neari[p].at[i, 1], rn_s.at[p], rn_r.at[p, i], moved(mine[p][1], n - 1))

    def here(i):
        for p in range(np_):
            pbuf[p][i] = line_sum(p, 0, i)
        for p in range(np_):
            (a, sa), (b, _), (k, _) = mine[p]
            aa = mod(i + 2 * n - b - k)
            drain(neari[p].at[i], rn_r.at[p, i])
            pbuf[p][i] += neari[p][i, 0] + neari[p][i, 1]

            @pl.when(aa != a)
            def _():
                put(pbuf[p].at[i], abuf[p].at[a], ra_s.at[p], ra_r.at[p], me + (aa - a) * sa)

            @pl.when(aa == a)
            def _():
                abuf[p][a] = pbuf[p][i]

    steps = {'x': lambda i: expert(i, 0), 'f': far, 'n': near, 'h': here}
    lax.fori_loop(0, n - 1, expert, 0)
    for step in RETURN_STEPS:
        steps[step[0]](int(step[1]))
    for p, (off, w) in enumerate(parts):
        drain(pbuf[p].at[pl.ds(0, n - 1)], ra_r.at[p])
        total = abuf[p][0]
        for i in range(1, n):
            total += abuf[p][i]
        y_ref[:, off:off + w] = total.astype(BF16)
    for p in range(np_):
        drain(tline[p].at[pl.ds(0, n - 1)], ta_s.at[p])
        drain(tbuf[p].at[pl.ds(0, n - 1)], tb_s.at[p])
        drain(xbuf[p].at[0, pl.ds(0, n - 1)], xa_s.at[p])
        drain(xbuf[p].at[pl.ds(0, 2)], xb_s.at[p])
        drain(xbuf[p].at[0], xd_s.at[p])
        drain(sbuf[p].at[:, pl.ds(0, 2 * n - 1)], c_s.at[p])
        drain(cbuf[p].at[:, :, pl.ds(0, 2 * n - 1)], rc_s.at[p])
        drain(farp[p], rf_s.at[p])
        drain(nearp[p], rn_s.at[p])
        drain(pbuf[p].at[pl.ds(0, n - 1)], ra_s.at[p])


def build(mesh, n, parts, lefts):
    row_spec = P(('data', 'expert'), None)
    expert_spec = P('expert', None, None)
    vmem = pl.BlockSpec(memory_space=pltpu.VMEM)
    hbm = pl.BlockSpec(memory_space=pltpu.HBM)

    def device_step(tokens, w_router, routes, w_gate, w_up, w_down):
        tok, width = tokens.shape
        experts = w_router.shape[1]
        ff = w_gate.shape[2]
        dma = pltpu.SemaphoreType.DMA
        np_ = len(parts)
        cols = 2 * n * CAP
        return pl.pallas_call(
            functools.partial(moe_kernel, n, parts, lefts),
            out_shape=pltpu.VMEM((tok, width), BF16),
            in_specs=[hbm] * 6, out_specs=vmem,
            scratch_shapes=[
                pltpu.VMEM((tok, width), BF16), pltpu.VMEM((width, experts), BF16), pltpu.VMEM((routes.shape[1], tok), jnp.int32),
                pltpu.VMEM((width, ff), BF16), pltpu.VMEM((width, ff), BF16), pltpu.VMEM((ff, width), BF16),
                pltpu.VMEM((n, n, n, 2, CAP, width), BF16), pltpu.VMEM((n, n, n, 2, CAP, width), BF16),
                pltpu.VMEM((2 * routes.shape[1], tok), F32),
                *[pltpu.VMEM((n, 2 * routes.shape[1], n * tok), F32) for _ in parts],
                *[pltpu.VMEM((n, n, tok, w), BF16) for _, w in parts],
                *[pltpu.VMEM((n, 2 * n, n, CAP, w), BF16) for _, w in parts],
                *[pltpu.VMEM((n, n, 2 * n, CAP, w), BF16) for _, w in parts],
                *[pltpu.VMEM((n, tok, w), F32) for _, w in parts],
                *[pltpu.VMEM((n, tok, w), F32) for _, w in parts],
                *[pltpu.VMEM((n, 2, tok, w), F32) for _, w in parts],
                *[pltpu.VMEM((n, 2, tok, w), F32) for _, w in parts],
                *[pltpu.VMEM((n, tok, w), F32) for _, w in parts],
                *[pltpu.VMEM((n, tok, w), F32) for _, w in parts],
                *[pltpu.VMEM((n, n, 3 * tok, cols), BF16) for _ in parts],
                *[pltpu.VMEM((2 * n, CAP, w), BF16) for _, w in parts],
                *[pltpu.VMEM((n, 2 * routes.shape[1], n * tok), F32) for _ in parts],
                dma((6,)), dma((np_,)), dma((np_,)), dma((np_,)), dma((np_,)),
                dma((np_,)), dma((np_, n - 1)), dma((np_,)), dma((np_, 2, n)), dma((np_,)), dma((np_,)), dma((np_,)), dma((np_, n)),
                dma((np_,)), dma((np_, n, n)), dma((np_,)), dma((np_, n)), dma((np_,)), dma((np_, n)), dma((np_,)), dma((np_,)),
            ],
            compiler_params=pltpu.CompilerParams(collective_id=0, has_side_effects=True, vmem_limit_bytes=57 * 1024 * 1024),
            name='moe',
        )(tokens, w_router, routes.T, w_gate, w_up, w_down)

    return jax.shard_map(device_step, mesh=mesh, in_specs=(row_spec, P(None, None), row_spec, expert_spec, expert_spec, expert_spec), out_specs=row_spec, check_vma=False)


def solution(mesh):
    return build(mesh, 4, ((0, 768), (768, 640), (1408, 640)), ((384, 384, 256), (384, 256, 384)))
```

```python
import functools

import jax
import jax.numpy as jnp
from jax import lax
from jax.experimental import pallas as pl
from jax.experimental.pallas import tpu as pltpu
from jax.sharding import PartitionSpec as P

F32 = jnp.float32
BF16 = jnp.bfloat16
CAP = 8
RETURN_STEPS = ('f0', 'x3', 'f1', 'f2', 'n0', 'f3', 'n1', 'n2', 'n3', 'h0', 'h1', 'h2', 'h3')


def _iota(shape, dim):
    return lax.broadcasted_iota(jnp.int32, shape, dim)


def _places(r):
    return (2 - r) % 3, (1 - r) % 3, (-r) % 3


def routing_table(x, wr, routes_t):
    tok, experts = x.shape[0], wr.shape[1]
    top_k = routes_t.shape[0]
    logits = jnp.dot(x, wr, preferred_element_type=F32).T
    ident = _iota((experts, tok), 0)
    chosen = [ident == routes_t[j:j + 1] for j in range(top_k)]
    hit = jnp.zeros((experts, tok), F32)
    for c in chosen:
        hit += c.astype(F32)
    on = hit > 0.5
    top = jnp.max(jnp.where(on, logits, -jnp.inf), axis=0, keepdims=True)
    e = jnp.where(on, jnp.exp(jnp.where(on, logits, top) - top), 0.0)
    gate = e / jnp.sum(e, axis=0, keepdims=True)
    above = (_iota((tok, tok), 0) < _iota((tok, tok), 1)).astype(BF16)
    slot = jnp.dot(hit.astype(BF16), above, preferred_element_type=F32)
    pick = lambda c, v: jnp.sum(jnp.where(c, v, 0.0), axis=0, keepdims=True)
    codes = [routes_t[j:j + 1].astype(F32) * CAP + pick(chosen[j], slot) for j in range(top_k)]
    return jnp.concatenate(codes + [pick(c, gate) for c in chosen], axis=0)


def split3(v):
    v1 = v.astype(BF16).astype(F32)
    v2 = (v - v1).astype(BF16).astype(F32)
    return v1, v2, v - v1 - v2


def one_hot(codes, want):
    out = jnp.zeros((want.shape[0], codes.shape[1]), F32)
    for j in range(codes.shape[0]):
        out += (codes[j:j + 1] == want).astype(F32)
    return out


def moe_kernel(n, parts, lefts, x_hbm, wr_hbm, rt_hbm, wg_hbm, wu_hbm, wd_hbm, y_ref, x_ref, wr_ref, rt_ref, wg, wu, wd, rbuf, obuf, tab_ref, *rest):
    top_k = rt_ref.shape[0]
    np_ = len(parts)
    tbuf, xbuf, sbuf, cbuf, farp, fari, nearp, neari, pbuf, abuf, mixbuf, ownbuf, tline = [rest[i * np_:(i + 1) * np_] for i in range(13)]
    (w_sem, ta_s, ta_r, tb_s, tb_r, xa_s, xa_r, xb_s, xb_r, xd_s, xd_r, c_s, c_r, rc_s, rc_r, rf_s, rf_r, rn_s, rn_r, ra_s, ra_r) = rest[13 * np_:]
    tok, width = x_ref.shape
    experts = wr_ref.shape[1]
    me = lax.axis_index('expert')
    strides = (2 * n * n, 2 * n, 2)
    pos = tuple(lax.rem(me // s, n) for s in strides)
    core = lax.rem(me, 2)
    mod = lambda v: lax.rem(v, n)

    def order(p, cc):
        r0, r1 = _places(p % 3), _places((p + 1) % 3)
        return [(pos[i] + cc * (pos[j] - pos[i]), strides[i] + cc * (strides[j] - strides[i])) for i, j in zip(r0, r1)]

    mine = [order(p, core) for p in range(np_)]
    theirs = [order(p, 1 - core) for p in range(np_)]

    def moved(axis, d, flip=0):
        where, stride = axis
        other = me + (mod(where + d) - where) * stride
        return other + (1 - 2 * core) if flip else other

    def put(src, dst, send, recv, device):
        pltpu.make_async_remote_copy(src_ref=src, dst_ref=dst, send_sem=send, recv_sem=recv,
                                     device_id={'expert': device}, device_id_type=pl.DeviceIdType.MESH).start()

    def drain(ref, sem):
        pltpu.make_async_copy(ref, ref, sem).wait()

    def canon(p, cc, a, b, k):
        r0, r1 = _places(p % 3), _places((p + 1) % 3)
        v = (a, b, k)
        return [v[r0.index(j)] + cc * (v[r1.index(j)] - v[r0.index(j)]) for j in (0, 1)]

    loads = [pltpu.make_async_copy(src, dst, w_sem.at[i]) for i, (src, dst) in enumerate(((x_hbm, x_ref), (wr_hbm, wr_ref), (rt_hbm, rt_ref), (wg_hbm.at[0], wg), (wu_hbm.at[0], wu), (wd_hbm.at[0], wd)))]
    for load in loads:
        load.start()

    barrier = pltpu.get_barrier_semaphore()
    peers = [moved((pos[j], strides[j]), d, flip) for j in range(3) for d in range(1, n) for flip in (0, 1)] + [me + 1 - 2 * core]
    for peer in peers:
        pl.semaphore_signal(barrier, inc=1, device_id={'expert': peer}, device_id_type=pl.DeviceIdType.MESH)
    for load in loads[:3]:
        load.wait()
    tab_ref[...] = routing_table(x_ref[...], wr_ref[...], rt_ref[...])
    terms = jnp.concatenate(split3(tab_ref[...]), axis=0).astype(BF16)
    for p, (off, w) in enumerate(parts):
        (a, _), (b, _), _ = mine[p]
        xbuf[p][b, a] = x_ref[:, off:off + w]
        place = (_iota((tok, n * tok), 1) == _iota((tok, n * tok), 0) + a * tok).astype(BF16)
        wide = jnp.dot(terms, place, preferred_element_type=F32)
        tline[p][a] = wide[:2 * top_k] + wide[2 * top_k:4 * top_k] + wide[4 * top_k:]
    pl.semaphore_wait(barrier, len(peers))

    near_first, far_first = (1, 3, 2), (2, 1, 3)

    q_order = (1, 4, 5, 2, 3, 6, 7)

    def select(p, db):
        off, w = parts[p]
        (a, _), (b, _), (k, _) = mine[p]
        bb = mod(b + n - db)
        row = _iota((n * CAP, 1), 0)
        want = jnp.concatenate([(moved(mine[p][2], q // 2, q % 2) * CAP + lax.rem(row, CAP)).astype(F32) for q in range(2 * n)], axis=0)
        shape = (2 * n * n * CAP, n * tok)
        same = lax.rem(_iota(shape, 0) // CAP, n) == _iota(shape, 1) // tok
        pick = jnp.where(same, one_hot(tbuf[p][bb, :top_k], want), 0.0).astype(BF16)
        rows = jnp.dot(pick, xbuf[p][bb].reshape(n * tok, w), preferred_element_type=F32).astype(BF16)
        sbuf[p][db] = rows.reshape(2 * n, n, CAP, w)

    def send_rows(p, db, i):
        off, w = parts[p]
        (a, _), (b, _), (k, _) = mine[p]
        bb = mod(b + n - db)
        aa = mod(i + 2 * n - bb - k)
        z, y = canon(p, core, aa, bb, k)

        def go():
            for q in q_order:
                put(sbuf[p].at[db, q, aa], rbuf.at[i, z, y, core, :, pl.ds(off, w)], c_s.at[p], c_r.at[p, i], moved(mine[p][2], q // 2, q % 2))
            rbuf[i, z, y, core, :, off:off + w] = sbuf[p][db, 0, aa]

        if db:
            go()
        else:
            pl.when(aa != a)(go)

    def own_rows():
        for p, (off, w) in enumerate(parts):
            (a, _), (b, _), (k, _) = mine[p]
            i = mod(a + b + k)
            row = _iota((CAP, 1), 0)
            want = jnp.concatenate([(moved(mine[p][2], q // 2, q % 2) * CAP + row).astype(F32) for q in range(2 * n)], axis=0)
            pick = one_hot(tab_ref[:top_k], want).astype(BF16)
            rows = jnp.dot(pick, x_ref[:, off:off + w], preferred_element_type=F32).astype(BF16)
            ownbuf[p][...] = rows.reshape(2 * n, CAP, w)
            z, y = canon(p, core, a, b, k)
            for q in q_order:
                put(ownbuf[p].at[q], rbuf.at[i, z, y, core, :, pl.ds(off, w)], c_s.at[p], c_r.at[p, i], moved(mine[p][2], q // 2, q % 2))
            rbuf[i, z, y, core, :, off:off + w] = ownbuf[p][0]

    def chunk_rows(i, dbs):
        for db in dbs:
            for p in range(np_):
                send_rows(p, db, i)

    def body(dbs):
        def run(i, carry):
            chunk_rows(i, dbs)
            return carry
        return run


    for d in far_first:
        for p in range(np_):
            (a, _), (b, _), _ = mine[p]
            put(tline[p].at[a], tline[p].at[a], ta_s.at[p], ta_r.at[p], moved(mine[p][0], d))
    def own_a(d):
        for p, (off, w) in enumerate(parts):
            (a, _), (b, _), _ = mine[p]
            put(x_ref.at[:, pl.ds(off, w)], xbuf[p].at[b, a], xa_s.at[p], xa_r.at[p, d - 1], moved(mine[p][0], d))

    def own_b(side):
        for p, (off, w) in enumerate(parts):
            (a, _), (b, _), _ = mine[p]
            put(x_ref.at[:, pl.ds(off, w)], xbuf[p].at[b, a], xb_s.at[p], xb_r.at[p, side, 0], moved(mine[p][1], 1 + 2 * side))
    own_a(1)
    own_a(3)
    own_b(0)
    own_b(1)
    own_a(2)
    own_rows()
    for p in range(np_):
        b = mine[p][1][0]
        drain(tline[p].at[pl.ds(0, n - 1)], ta_r.at[p])
        line = tline[p][0]
        for i in range(1, n):
            line += tline[p][i]
        tbuf[p][b] = line
        for d in far_first:
            put(tbuf[p].at[b], tbuf[p].at[b], tb_s.at[p], tb_r.at[p], moved(mine[p][1], d))

    def along_b(da):
        for p in range(np_):
            (a, _), (b, _), _ = mine[p]
            src = mod(a + n - da)
            drain(xbuf[p].at[0, 0], xa_r.at[p, da - 1])
            for side in (0, 1):
                put(xbuf[p].at[b, src], xbuf[p].at[b, src], xb_s.at[p], xb_r.at[p, side, da], moved(mine[p][1], 1 + 2 * side))

    def onward(da):
        for side in (0, 1):
            for p, (off, w) in enumerate(parts):
                (a, _), (b, _), _ = mine[p]
                src, bb = mod(a + n - da), mod(b + n - 1 - 2 * side)
                left = lefts[da % 2][p]
                drain(xbuf[p].at[0, 0], xb_r.at[p, side, da])
                half = pl.ds(left, w - left) if side else pl.ds(0, left)
                put(xbuf[p].at[bb, src, :, half], xbuf[p].at[bb, src, :, half], xd_s.at[p], xd_r.at[p], moved(mine[p][1], 1 + 2 * side))

    along_b(1)
    along_b(3)
    onward(0)
    along_b(2)

    for p in range(np_):
        select(p, 0)
    lax.fori_loop(0, n - 1, body((0,)), 0)
    for da in near_first:
        onward(da)
    chunk_rows(n - 1, (0,))
    for p in range(np_):
        drain(tbuf[p].at[pl.ds(0, n - 1)], tb_r.at[p])
    for db in (1, 3):
        for p in range(np_):
            select(p, db)
    lax.fori_loop(0, 2, body((1, 3)), 0)
    for p in range(np_):
        drain(xbuf[p].at[0], xd_r.at[p])
        select(p, 2)
        send_rows(p, 2, 0)
    chunk_rows(1, (2,))
    lax.fori_loop(2, n, body((1, 3, 2)), 0)

    cols = 2 * n * CAP
    for p in range(np_):
        (a, sa), (b, sb), (_, sc) = mine[p]
        slot = _iota((cols, 1), 0)
        ident = slot // (2 * CAP) * sc + lax.rem(slot // CAP, 2) + a * sa + b * sb
        want = (ident * CAP + lax.rem(slot, CAP)).astype(F32)
        for bb in range(n):
            tb = tbuf[p][bb]
            gates = split3(tb[top_k:])
            mix = [jnp.zeros((cols, n * tok), F32) for _ in gates]
            for j in range(top_k):
                at = tb[j:j + 1] == want
                mix = [m + jnp.where(at, g[j:j + 1], 0.0) for m, g in zip(mix, gates)]
            mix = [m.T for m in mix]
            for aa in range(n):
                mixbuf[p][bb, aa] = jnp.concatenate([m[aa * tok:(aa + 1) * tok] for m in mix], axis=0).astype(BF16)

    for load in loads[3:]:
        load.wait()

    ring = (2, 1, 3, 0) if n == 4 else tuple(range(1, n)) + (0,)

    def expert(i, carry):
        for p in range(np_):
            drain(sbuf[p].at[:, pl.ds(0, 2 * n - 1), 0], c_r.at[p, i])
        rows = rbuf[i].reshape(n * n * 2 * CAP, width)
        g = jnp.dot(rows, wg[...], preferred_element_type=F32)
        u = jnp.dot(rows, wu[...], preferred_element_type=F32)
        h = (g * jax.nn.sigmoid(g) * u).astype(BF16)
        o = jnp.dot(h, wd[...], preferred_element_type=F32).astype(BF16)
        obuf[i] = o.reshape(n, n, 2, CAP, width)
        for db in ring:
            for q in q_order + (0,):
                for p, (off, w) in enumerate(parts):
                    cc, axes = (1 - core, theirs[p]) if q % 2 else (core, mine[p])
                    (_, _), (b, _), (k, _) = axes
                    kk, bb = mod(k + q // 2), mod(b + db)
                    aa = mod(i + 2 * n - bb - kk)
                    z, y = canon(p, cc, aa, bb, kk)
                    if q:
                        put(obuf.at[i, z, y, cc, :, pl.ds(off, w)], cbuf[p].at[bb, aa, k * 2 + core],
                            rc_s.at[p], rc_r.at[p, db, i], moved(axes[2], q // 2, q % 2))
                    else:
                        cbuf[p][bb, aa, k * 2 + core] = obuf[i, z, y, cc, :, off:off + w]
        return carry

    def line_sum(p, db, i):
        w = parts[p][1]
        _, (b, _), (k, _) = mine[p]
        bb = mod(b + db)
        aa = mod(i + 2 * n - bb - k)
        drain(cbuf[p].at[0, 0, pl.ds(0, 2 * n - 1)], rc_r.at[p, db, i])
        part = jnp.dot(mixbuf[p][bb, aa], cbuf[p][bb, aa].reshape(cols, w), preferred_element_type=F32)
        return part[:tok] + part[tok:2 * tok] + part[2 * tok:]

    def far(i):
        for p in range(np_):
            w, left = parts[p][1], lefts[i % 2][p]
            farp[p][i] = line_sum(p, 2, i)
            put(farp[p].at[i, :, pl.ds(0, left)], fari[p].at[i, :, pl.ds(0, left)], rf_s.at[p], rf_r.at[p, i], moved(mine[p][1], 1))
            put(farp[p].at[i, :, pl.ds(left, w - left)], fari[p].at[i, :, pl.ds(left, w - left)], rf_s.at[p], rf_r.at[p, i], moved(mine[p][1], n - 1))

    def near(i):
        for p in range(np_):
            left = lefts[i % 2][p]
            up, down = line_sum(p, 1, i), line_sum(p, n - 1, i)
            drain(fari[p].at[i], rf_r.at[p, i])
            nearp[p][i, 0, :, :left] = up[:, :left] + fari[p][i, :, :left]
            nearp[p][i, 0, :, left:] = up[:, left:]
            put(nearp[p].at[i, 0], neari[p].at[i, 0], rn_s.at[p], rn_r.at[p, i], moved(mine[p][1], 1))
            nearp[p][i, 1, :, :left] = down[:, :left]
            nearp[p][i, 1, :, left:] = down[:, left:] + fari[p][i, :, left:]
            put(nearp[p].at[i, 1], neari[p].at[i, 1], rn_s.at[p], rn_r.at[p, i], moved(mine[p][1], n - 1))

    def here(i):
        for p in range(np_):
            pbuf[p][i] = line_sum(p, 0, i)
        for p in range(np_):
            (a, sa), (b, _), (k, _) = mine[p]
            aa = mod(i + 2 * n - b - k)
            drain(neari[p].at[i], rn_r.at[p, i])
            pbuf[p][i] += neari[p][i, 0] + neari[p][i, 1]

            @pl.when(aa != a)
            def _():
                put(pbuf[p].at[i], abuf[p].at[a], ra_s.at[p], ra_r.at[p], me + (aa - a) * sa)

            @pl.when(aa == a)
            def _():
                abuf[p][a] = pbuf[p][i]

    steps = {'x': lambda i: expert(i, 0), 'f': far, 'n': near, 'h': here}
    lax.fori_loop(0, n - 1, expert, 0)
    for step in RETURN_STEPS:
        steps[step[0]](int(step[1]))
    for p, (off, w) in enumerate(parts):
        drain(pbuf[p].at[pl.ds(0, n - 1)], ra_r.at[p])
        total = abuf[p][0]
        for i in range(1, n):
            total += abuf[p][i]
        y_ref[:, off:off + w] = total.astype(BF16)
    for p in range(np_):
        drain(tline[p].at[pl.ds(0, n - 1)], ta_s.at[p])
        drain(tbuf[p].at[pl.ds(0, n - 1)], tb_s.at[p])
        drain(xbuf[p].at[0, pl.ds(0, n - 1)], xa_s.at[p])
        drain(xbuf[p].at[pl.ds(0, 2)], xb_s.at[p])
        drain(xbuf[p].at[0], xd_s.at[p])
        drain(sbuf[p].at[:, pl.ds(0, 2 * n - 1)], c_s.at[p])
        drain(cbuf[p].at[:, :, pl.ds(0, 2 * n - 1)], rc_s.at[p])
        drain(farp[p], rf_s.at[p])
        drain(nearp[p], rn_s.at[p])
        drain(pbuf[p].at[pl.ds(0, n - 1)], ra_s.at[p])


def build(mesh, n, parts, lefts):
    row_spec = P(('data', 'expert'), None)
    expert_spec = P('expert', None, None)
    vmem = pl.BlockSpec(memory_space=pltpu.VMEM)
    hbm = pl.BlockSpec(memory_space=pltpu.HBM)

    def device_step(tokens, w_router, routes, w_gate, w_up, w_down):
        tok, width = tokens.shape
        experts = w_router.shape[1]
        ff = w_gate.shape[2]
        dma = pltpu.SemaphoreType.DMA
        np_ = len(parts)
        cols = 2 * n * CAP
        return pl.pallas_call(
            functools.partial(moe_kernel, n, parts, lefts),
            out_shape=pltpu.VMEM((tok, width), BF16),
            in_specs=[hbm] * 6, out_specs=vmem,
            scratch_shapes=[
                pltpu.VMEM((tok, width), BF16), pltpu.VMEM((width, experts), BF16), pltpu.VMEM((routes.shape[1], tok), jnp.int32),
                pltpu.VMEM((width, ff), BF16), pltpu.VMEM((width, ff), BF16), pltpu.VMEM((ff, width), BF16),
                pltpu.VMEM((n, n, n, 2, CAP, width), BF16), pltpu.VMEM((n, n, n, 2, CAP, width), BF16),
                pltpu.VMEM((2 * routes.shape[1], tok), F32),
                *[pltpu.VMEM((n, 2 * routes.shape[1], n * tok), F32) for _ in parts],
                *[pltpu.VMEM((n, n, tok, w), BF16) for _, w in parts],
                *[pltpu.VMEM((n, 2 * n, n, CAP, w), BF16) for _, w in parts],
                *[pltpu.VMEM((n, n, 2 * n, CAP, w), BF16) for _, w in parts],
                *[pltpu.VMEM((n, tok, w), F32) for _, w in parts],
                *[pltpu.VMEM((n, tok, w), F32) for _, w in parts],
                *[pltpu.VMEM((n, 2, tok, w), F32) for _, w in parts],
                *[pltpu.VMEM((n, 2, tok, w), F32) for _, w in parts],
                *[pltpu.VMEM((n, tok, w), F32) for _, w in parts],
                *[pltpu.VMEM((n, tok, w), F32) for _, w in parts],
                *[pltpu.VMEM((n, n, 3 * tok, cols), BF16) for _ in parts],
                *[pltpu.VMEM((2 * n, CAP, w), BF16) for _, w in parts],
                *[pltpu.VMEM((n, 2 * routes.shape[1], n * tok), F32) for _ in parts],
                dma((6,)), dma((np_,)), dma((np_,)), dma((np_,)), dma((np_,)),
                dma((np_,)), dma((np_, n - 1)), dma((np_,)), dma((np_, 2, n)), dma((np_,)), dma((np_,)), dma((np_,)), dma((np_, n)),
                dma((np_,)), dma((np_, n, n)), dma((np_,)), dma((np_, n)), dma((np_,)), dma((np_, n)), dma((np_,)), dma((np_,)),
            ],
            compiler_params=pltpu.CompilerParams(collective_id=0, has_side_effects=True, vmem_limit_bytes=57 * 1024 * 1024),
            name='moe',
        )(tokens, w_router, routes.T, w_gate, w_up, w_down)

    return jax.shard_map(device_step, mesh=mesh, in_specs=(row_spec, P(None, None), row_spec, expert_spec, expert_spec, expert_spec), out_specs=row_spec, check_vma=False)


def solution(mesh):
    return build(mesh, 4, ((0, 768), (768, 640), (1408, 640)), ((384, 384, 256), (384, 256, 384)))
```
